512 devices in a mesh: seq: 128 (over z, x, y_lo, core), head: 4 (over y_hi).
Axes of the slice: x: 4, y: 8 (y_hi: 4, y_lo: 2; y = y_hi * 2 + y_lo), z: 8, core: 2. Of those that a mesh axis runs over, the one named last changes fastest.
Arguments:
- query: bfloat16 [2, 16384, 4096], P(None, 'seq', 'head'), may hold values from -5 to 5
- keys: bfloat16 [2, 16384, 1024], P(None, 'seq', 'head'), may hold values from -5 to 5
- values: bfloat16 [2, 16384, 1024], P(None, 'seq', 'head'), may hold values from -12 to 12
- norm_gain: float32 [4096], P('head'), may hold values from 0.25 to 1.75
- in_b: bfloat16 [32768, 128], P('seq'), may hold values from -0.25 to 0.25
- out_c: bfloat16 [32768, 128], P('seq'), may hold values from -0.25 to 0.25
- step: float32 [64, 32768], P('head', 'seq'), may hold values from 0.2 to 1
- log_decay: float32 [64, 32768], P('head', 'seq'), may hold values from -2 to 0
- skip: float32 [64], P('head'), may hold values from 0.5 to 1.5
Outputs:
- mixed: bfloat16 [32768, 4096], P('seq', 'head')
The draws below stay inside these ranges and needn't reach their ends.
All inputs are finite; a program needn't handle non-finite values.
Results may differ from the reference program's by a relative error of at most 0.012.
Values may be sent and summed in bfloat16 or wider, within the bound.
A program may use at most 128 MiB of HBM per device.

```python
import math
import jax
import jax.numpy as jnp
from jax import lax

HEADS = 32
KVH = 8
HDIM = 128
SHEADS = 64
SDIM = 64
STATE = 128
SPAN = 256
TOKEN_COUNT = 32768
BLK = 128
WIN = 256


def qk_pair(key):
    baseline_rate = jax.random.fold_in(key, 11)
    key_query, key_keys = jax.random.split(baseline_rate, 2)
    queries = jnp.clip(jax.random.normal(key_query, (TOKEN_COUNT, HEADS * HDIM), jnp.float32), -4.0, 4.0)
    keyvals = jnp.clip(jax.random.normal(key_keys, (TOKEN_COUNT, KVH * HDIM), jnp.float32), -4.0, 4.0)
    queries = queries.reshape(2, TOKEN_COUNT // 2, HEADS * HDIM).astype(jnp.bfloat16)
    keyvals = keyvals.reshape(2, TOKEN_COUNT // 2, KVH * HDIM).astype(jnp.bfloat16)
    return (queries, keyvals)


def draw_query(key, part):
    return qk_pair(key)[0]


def draw_keys(key, part):
    return qk_pair(key)[1]


def draw_values(key, part):
    baseline_rate = jax.random.fold_in(key, 23)
    head_scale = 3.0 ** (jnp.arange(KVH, dtype=jnp.float32) / (KVH - 1))
    raw_values = jnp.clip(jax.random.normal(baseline_rate, (TOKEN_COUNT, KVH, HDIM), jnp.float32), -4.0, 4.0)
    scaled = raw_values * head_scale[None, :, None]
    return scaled.reshape(2, TOKEN_COUNT // 2, KVH * HDIM).astype(jnp.bfloat16)


def draw_log_decay(key, part):
    baseline_rate = jax.random.fold_in(key, 31)
    gradual_key, rate_key, quick_key, noise_key, spike_key, depth_key = jax.random.split(baseline_rate, 6)
    slow_share = 0.5
    slow_heads = jax.random.bernoulli(gradual_key, slow_share, (SHEADS,))
    slow_rate = jnp.exp(jax.random.uniform(rate_key, (SHEADS,), jnp.float32, jnp.log(0.1), jnp.log(0.6))) / TOKEN_COUNT
    fast_rate = jax.random.uniform(quick_key, (SHEADS,), jnp.float32, 1.0 / 50.0, 1.0 / 30.0)
    decay_speeds = jnp.where(slow_heads, slow_rate, fast_rate)
    random_noise = jnp.exp(jax.random.uniform(noise_key, (SHEADS, TOKEN_COUNT), jnp.float32, jnp.log(0.5), jnp.log(2.0)))
    spike_position = jax.random.randint(spike_key, (3,), 0, TOKEN_COUNT)
    spike_depth = jax.random.uniform(depth_key, (3,), jnp.float32, 0.22, 0.5)
    token_location = jnp.arange(TOKEN_COUNT)
    spike_events = jnp.sum(jnp.where(token_location[None, :] == spike_position[:, None], spike_depth[:, None], 0.0), axis=0)
    return -(decay_speeds[:, None] * random_noise + spike_events[None, :])


def block_levels(own_key, extent, cuts, least, largest):
    loudness = 1.0
    for dim, shards_of in cuts:
        heights = jax.random.uniform(jax.random.fold_in(jax.random.fold_in(own_key, 6), dim), (shards_of,), jnp.float32, least / len(cuts), largest / len(cuts))
        loudness = loudness * jnp.repeat(jnp.exp(heights), extent[dim] // shards_of).reshape((-1,) + (1,) * (len(extent) - 1 - dim))
    return loudness


def scatter_about(own_key, extent, spread, reach, cuts=(), kind=jnp.bfloat16):
    array = spread * jax.random.normal(own_key, extent, jnp.float32)
    if cuts:
        array = array * block_levels(own_key, extent, cuts, -0.22, 0.18)
    return jnp.clip(array, -reach, reach).astype(kind)


def setup_inputs(seed: int = 0) -> dict:
    key_list = jax.random.split(jax.random.key(seed), 10)
    query = draw_query(jax.random.fold_in(key_list[9], 71), 0)
    keys = draw_keys(jax.random.fold_in(key_list[9], 71), 0)
    values = draw_values(jax.random.fold_in(key_list[9], 71), 0)
    norm_gain = jnp.clip(1.0 + 0.15 * jax.random.normal(key_list[3], (HEADS * HDIM,), jnp.float32), 0.25, 1.75)
    in_b = scatter_about(key_list[4], (TOKEN_COUNT, STATE), 0.04, 0.25, ((0, 128),))
    out_c = scatter_about(key_list[5], (TOKEN_COUNT, STATE), 0.04, 0.25, ((0, 128),))
    step = jnp.clip(jnp.exp(math.log(1.0) - 1.609438 * jax.random.uniform(key_list[6], (SHEADS, TOKEN_COUNT), jnp.float32) ** block_levels(key_list[6], (SHEADS, TOKEN_COUNT), ((0, 4), (1, 128)), -0.2, 0.2)), 0.2, 1.0)
    log_decay = draw_log_decay(jax.random.fold_in(key_list[9], 71), 0)
    skip = jnp.clip(0.5 + 1.0 * jax.random.uniform(key_list[8], (SHEADS,), jnp.float32) ** block_levels(key_list[8], (SHEADS,), ((0, 4),), -0.2, 0.2), 0.5, 1.5)
    return {"query": query, "keys": keys, "values": values, "norm_gain": norm_gain, "in_b": in_b, "out_c": out_c, "step": step, "log_decay": log_decay, "skip": skip}


def attention_all(query, keys, values):
    group_size = HEADS // KVH
    queries = query.reshape(TOKEN_COUNT, KVH, group_size, HDIM)
    key_pad = jnp.concatenate([jnp.zeros((WIN, KVH, HDIM), jnp.bfloat16), keys.reshape(TOKEN_COUNT, KVH, HDIM)], 0)
    val_pad = jnp.concatenate([jnp.zeros((WIN, KVH, HDIM), jnp.bfloat16), values.reshape(TOKEN_COUNT, KVH, HDIM)], 0)
    score_scale = 1.0 / math.sqrt(HDIM)

    def attend_block(block_no):
        start = (block_no * BLK).astype(jnp.int32)
        query_rows = lax.dynamic_slice_in_dim(queries, start, BLK, 0).astype(jnp.float32)
        key_rows = lax.dynamic_slice_in_dim(key_pad, start, WIN + BLK, 0).astype(jnp.float32)
        val_rows = lax.dynamic_slice_in_dim(val_pad, start, WIN + BLK, 0).astype(jnp.float32)
        query_pos = start + jnp.arange(BLK, dtype=jnp.int32)
        key_pos = start - WIN + jnp.arange(WIN + BLK, dtype=jnp.int32)
        allowed = (key_pos[None, :] <= query_pos[:, None]) & (key_pos[None, :] > query_pos[:, None] - WIN) & (key_pos[None, :] >= 0)
        scores = jnp.einsum('qgjd,kgd->gjqk', query_rows, key_rows) * score_scale
        scores = jnp.where(allowed, scores, -jnp.inf)
        row_peak = lax.optimization_barrier(jnp.max(scores, axis=-1, keepdims=True))
        exp_terms = jnp.exp(scores - row_peak)
        row_total = lax.optimization_barrier(jnp.sum(exp_terms, axis=-1))
        weights = exp_terms.astype(jnp.bfloat16).astype(jnp.float32)
        result = jnp.einsum('gjqk,kgd->qgjd', weights, val_rows)
        result = result / jnp.transpose(row_total, (2, 0, 1))[..., None]
        return result.reshape(BLK, HEADS * HDIM).astype(jnp.bfloat16)
    blocks = lax.map(attend_block, jnp.arange(TOKEN_COUNT // BLK, dtype=jnp.int32))
    return blocks.reshape(TOKEN_COUNT, HEADS * HDIM)

def reference(query, keys, values, norm_gain, in_b, out_c, step, log_decay, skip):
    attended = attention_all(query, keys, values)
    widened = attended.astype(jnp.float32)
    meansq = lax.optimization_barrier(jnp.mean(widened * widened, axis=-1))
    normed = (widened * norm_gain[None, :] * lax.rsqrt(meansq + 1e-06)[:, None]).astype(jnp.bfloat16)
    span_count = TOKEN_COUNT // SPAN
    inputs = normed.astype(jnp.float32).reshape(span_count, SPAN, SHEADS, SDIM)
    in_rows = in_b.astype(jnp.float32).reshape(span_count, SPAN, STATE)
    out_rows = out_c.astype(jnp.float32).reshape(span_count, SPAN, STATE)
    step_rows = step.reshape(SHEADS, span_count, SPAN).transpose(1, 0, 2)
    decay_rows = log_decay.reshape(SHEADS, span_count, SPAN).transpose(1, 0, 2)
    causal = jnp.arange(SPAN)[:, None] >= jnp.arange(SPAN)[None, :]
    highest = lax.Precision.HIGHEST

    def advance(carried, pieces):
        x_rows, b_rows, c_rows, dt_rows, log_rows = pieces
        cum_log = jnp.cumsum(log_rows, axis=1)
        decay_mat = jnp.exp(jnp.where(causal[None], cum_log[:, :, None] - cum_log[:, None, :], -jnp.inf))
        cross_terms = jnp.dot(c_rows, b_rows.T, precision=highest)
        mixing = decay_mat * cross_terms[None] * dt_rows[:, None, :]
        mixing = mixing.astype(jnp.bfloat16).astype(jnp.float32)
        result = jnp.einsum('htu,uhe->the', mixing, x_rows, precision=highest)
        entry_term = jnp.einsum('tn,hen->the', c_rows, carried, precision=highest)
        result = result + entry_term * jnp.exp(cum_log).T[:, :, None]
        result = result + skip[None, :, None] * x_rows
        end_weights = jnp.exp(cum_log[:, -1:] - cum_log) * dt_rows
        weighted = end_weights.T[:, :, None] * x_rows
        carried = jnp.exp(cum_log[:, -1])[:, None, None] * carried + jnp.einsum('uhe,un->hen', weighted, b_rows, precision=highest)
        return (carried, result)
    initial = jnp.zeros((SHEADS, SDIM, STATE), jnp.float32)
    final_state, outputs = lax.scan(advance, initial, (inputs, in_rows, out_rows, step_rows, decay_rows))
    return outputs.reshape(TOKEN_COUNT, SHEADS * SDIM).astype(jnp.bfloat16)
```

```python
import math

import jax
import jax.numpy as jnp
from jax import lax
from jax.experimental import pallas as pl
from jax.experimental.pallas import tpu as pltpu
from jax.sharding import Mesh
from jax.sharding import PartitionSpec as P

HDIM = 128
SDIM = 64
STATE = 128
SPAN = 256
BLK = 128
FEATS = 4096
NZ, NX, NY, NC, NH = 8, 4, 2, 2, 4
CHIPS = NZ * NX * NY
PLANE = NX * NY * NC
AXES = ("z", "x", "y", "core", "head")
SEQ = ("z", "x", "y", "core")
MESH = pl.DeviceIdType.MESH
F32 = jnp.float32
BF16 = jnp.bfloat16


def chip_coords(chip):
    return chip // (NX * NY), (chip // NY) % NX, chip % NY


def seq_coords(index):
    return index // PLANE, (index // (NY * NC)) % NX, (index // NC) % NY, index % NC


def dot(a, b, dims, **kw):
    return lax.dot_general(a, b, (dims, ((), ())), preferred_element_type=F32, **kw)


def kernel(
    q_hbm, k_hbm, v_hbm, gain_hbm, b_hbm, c_hbm, step_hbm, decay_hbm, skip_ref,
    out_ref,
    q_span, k_stage, v_stage, k_win, v_win, gain_v, b_v, c_v, step_v, decay_v,
    cum_v, w_v, v_v, gcol, mix, ecum, att, att_in, sq_out, sq_in, normed, weighted, local,
    tot_out, tot_in, plane_out, plane_in, st_out, st_in, pre_v, pre_log, run_out, run_in,
    en_out, en_in,
    load_sem, halo_send, halo_recv, swap_send, swap_recv, q_send, q_recv, att_send, att_recv,
    sq_send, sq_recv, tot_send, tot_recv, plane_send, plane_recv, st_send, st_recv,
    run_send, run_recv, log_send, log_recv, en_send, en_recv,
):
    z, x, y, core, hg = (lax.axis_index(a) for a in AXES)
    chip = (z * NX + x) * NY + y
    me = (x * NY + y) * NC + core
    seq = z * PLANE + me
    other = 1 - core
    partner = (z, x, y, other, hg)

    after = (chip + 1) % CHIPS
    az, ax, ay = chip_coords(after)
    wraps = (chip == CHIPS - 1).astype(jnp.int32)
    before = (chip + CHIPS - 1) % CHIPS
    bz, bx, by = chip_coords(before)

    span = core * CHIPS + chip
    fz, fx, fy, fc = seq_coords(span)
    source_chip = seq % CHIPS
    sz, sx, sy = chip_coords(source_chip)
    sc = seq // CHIPS
    stays = span == seq

    mine = pl.ds(pl.multiple_of((2 + core) * BLK, BLK), BLK)
    theirs = pl.ds(pl.multiple_of((2 + other) * BLK, BLK), BLK)
    prev_row = pl.ds(pl.multiple_of(core * BLK, BLK), BLK)
    loads = [
        (k_hbm, k_stage), (v_hbm, v_stage), (decay_hbm, decay_v), (step_hbm, step_v),
        (b_hbm, b_v), (c_hbm, c_v), (gain_hbm, gain_v),
        (k_hbm.at[core], k_win.at[mine]), (v_hbm.at[core], v_win.at[mine]),
        (q_hbm.at[core], q_span.at[core]),
    ]
    loads = [pltpu.make_async_copy(s, d, load_sem.at[i]) for i, (s, d) in enumerate(loads)]
    for copy in loads:
        copy.start()

    barrier = pltpu.get_barrier_semaphore()

    def greet(device):
        pl.semaphore_signal(barrier, inc=1, device_id=device, device_id_type=MESH)

    for c in range(NC):
        greet((bz, bx, by, c, hg))
    for r in range(1, NH):
        greet((sz, sx, sy, sc, (hg + r) % NH))

    @pl.when(jnp.logical_not(stays))
    def _():
        greet((sz, sx, sy, sc, hg))

    def plane_device(index):
        return (z, index // (NY * NC), (index // NC) % NY, index % NC, hg)

    def z_device(index):
        return (index, x, y, core, hg)

    def greet_plane(r, carry):
        greet(plane_device((me + r) % PLANE))
        return carry

    lax.fori_loop(1, PLANE, greet_plane, 0)

    def greet_z(r, carry):
        greet(z_device((z + r) % NZ))
        return carry

    lax.fori_loop(1, NZ, greet_z, 0)
    moves = jnp.logical_not(stays).astype(jnp.int32)
    pl.semaphore_wait(barrier, NC + NH - 1 + PLANE - 1 + NZ - 1 + moves)

    loads[0].wait()
    loads[1].wait()

    def cols(g, width=HDIM):
        return pl.ds(g * width, width)

    def halo(i, g, slot):
        stage, window = ((k_stage, k_win), (v_stage, v_win))[i]
        to = (az, ax, ay, jnp.where(wraps == 1, 1 - slot, slot), hg)
        return pltpu.make_async_remote_copy(
            src_ref=stage.at[slot, :, cols(g)], dst_ref=window.at[prev_row, cols(g)],
            send_sem=halo_send.at[i, g, slot], recv_sem=halo_recv.at[i, g, core],
            device_id=to, device_id_type=MESH,
        )

    def halo_arrival(i, g, block):
        window = (k_win, v_win)[i]
        return pltpu.make_async_remote_copy(
            src_ref=window.at[pl.ds(block * BLK, BLK), cols(g)],
            dst_ref=window.at[pl.ds(block * BLK, BLK), cols(g)],
            send_sem=halo_send.at[i, g, 0], recv_sem=halo_recv.at[i, g, block],
            device_id=partner, device_id_type=MESH,
        )

    def swap(i, g):
        stage, window = ((k_stage, k_win), (v_stage, v_win))[i]
        return pltpu.make_async_remote_copy(
            src_ref=stage.at[other, :, cols(g)], dst_ref=window.at[mine, cols(g)],
            send_sem=swap_send.at[i, g], recv_sem=swap_recv.at[i, g],
            device_id=partner, device_id_type=MESH,
        )

    def swap_arrival(i, g):
        window = (k_win, v_win)[i]
        return pltpu.make_async_remote_copy(
            src_ref=window.at[theirs, cols(g)], dst_ref=window.at[theirs, cols(g)],
            send_sem=swap_send.at[i, g], recv_sem=swap_recv.at[i, g],
            device_id=partner, device_id_type=MESH,
        )

    def q_swap(g):
        return pltpu.make_async_remote_copy(
            src_ref=q_hbm.at[other, :, cols(g, 512)],
            dst_ref=q_span.at[core, :, cols(g, 512)],
            send_sem=q_send.at[g], recv_sem=q_recv.at[g],
            device_id=partner, device_id_type=MESH,
        )

    def q_arrival(g):
        return pltpu.make_async_remote_copy(
            src_ref=q_span.at[other, :, cols(g, 512)],
            dst_ref=q_span.at[other, :, cols(g, 512)],
            send_sem=q_send.at[g], recv_sem=q_recv.at[g],
            device_id=partner, device_id_type=MESH,
        )

    for g in range(2):
        for i in range(2):
            for slot in range(2):
                halo(i, g, slot).start()
        q_swap(g).start()
        for i in range(2):
            swap(i, g).start()

    for copy in loads[2:]:
        copy.wait()
    row = lax.broadcasted_iota(jnp.int32, (SPAN, SPAN), 0)
    col = lax.broadcasted_iota(jnp.int32, (SPAN, SPAN), 1)
    causal = row <= col
    cum = dot(decay_v[...], causal.astype(F32), ((1,), (0,)), precision=lax.Precision.HIGHEST)
    total = cum[:, SPAN - 1:]
    tail = jnp.exp(total - cum) * step_v[...]
    shift = jnp.log(step_v[...]) - cum
    for k in range(16):
        cum_v[k] = jnp.broadcast_to(cum[k:k + 1], (8, SPAN))
        w_v[k] = jnp.broadcast_to(tail[k:k + 1], (8, SPAN))
        v_v[k] = jnp.broadcast_to(shift[k:k + 1], (8, SPAN))
        tot_out[k] = jnp.broadcast_to(total[k:k + 1], (8, 128))

    def tot_copy(k, at):
        return pltpu.make_async_remote_copy(
            src_ref=tot_out.at[k], dst_ref=tot_in.at[at],
            send_sem=tot_send.at[k], recv_sem=tot_recv.at[at],
            device_id=plane_device(k), device_id_type=MESH,
        )

    def start_tot(r, carry):
        tot_copy((me + r) % PLANE, me).start()
        return carry

    lax.fori_loop(1, PLANE, start_tot, 0)
    tot_in[me] = tot_out[me]

    cross = dot(b_v[...], c_v[...], ((1,), (1,)))

    def make_mix(k, carry):
        ct = cum_v[k, 0:1, :]
        for ub in range(2):
            line = v_v[k, 0:1, ub * BLK:(ub + 1) * BLK]
            colb = jnp.transpose(jnp.broadcast_to(line, (BLK, BLK)))
            arg = ct + jnp.concatenate([colb, colb], 1)
            rows = slice(ub * BLK, (ub + 1) * BLK)
            arg = jnp.where(causal[rows], arg, -jnp.inf)
            mix[k, rows] = (jnp.exp(arg) * cross[rows]).astype(BF16)
        return carry

    lax.fori_loop(0, 16, make_mix, 0)

    def make_ecum(p, carry):
        lanes = pl.ds(pl.multiple_of(p * BLK, BLK), BLK)
        for tb in range(2):
            part = slice(tb * BLK, (tb + 1) * BLK)
            pair = [
                jnp.broadcast_to(jnp.exp(cum_v[2 * p + h, 0:1, part]), (SDIM, BLK))
                for h in range(2)
            ]
            ecum[part, lanes] = jnp.transpose(jnp.concatenate(pair, 0))
        return carry

    lax.fori_loop(0, 8, make_ecum, 0)
    for p in range(8):
        line = jnp.broadcast_to(gain_v[p:p + 1, :], (BLK, BLK))
        gcol[p * BLK:(p + 1) * BLK, :] = jnp.transpose(line)

    def wait_tot(r, carry):
        tot_copy((me + r) % PLANE, (me + r) % PLANE).wait_recv()
        return carry

    lax.fori_loop(1, PLANE, wait_tot, 0)
    plane_log = tot_in[0]
    for i in range(1, PLANE):
        plane_log = plane_log + tot_in[i]
    plane_out[...] = plane_log
    plane_in[z] = plane_log

    def log_copy(to, at):
        return pltpu.make_async_remote_copy(
            src_ref=plane_out, dst_ref=plane_in.at[at],
            send_sem=log_send.at[to], recv_sem=log_recv.at[at],
            device_id=z_device(to), device_id_type=MESH,
        )

    def start_log(r, carry):
        log_copy((z + r) % NZ, z).start()
        return carry

    lax.fori_loop(1, NZ, start_log, 0)

    scale = math.log2(math.e) / math.sqrt(HDIM)
    j = lax.broadcasted_iota(jnp.int32, (3 * BLK, 4 * BLK), 0)
    i = lax.broadcasted_iota(jnp.int32, (3 * BLK, 4 * BLK), 1) % BLK
    first = (span == 0).astype(jnp.int32)

    def att_copy(g):
        part = pl.ds(g * 512, 512)
        return pltpu.make_async_remote_copy(
            src_ref=att.at[part], dst_ref=att_in.at[part],
            send_sem=att_send.at[g], recv_sem=att_recv.at[g],
            device_id=(fz, fx, fy, fc, hg), device_id_type=MESH,
        )

    def att_keep(g):
        part = pl.ds(g * 512, 512)
        return pltpu.make_async_copy(att.at[part], att_in.at[part], att_recv.at[g])

    sums = [jnp.zeros((1, BLK), F32) for _ in range(2)]
    for g in range(2):
        for t in range(2):
            for block in range(2):
                halo_arrival(t, g, block).wait_recv()
            swap_arrival(t, g).wait_recv()
        q_arrival(g).wait_recv()
        lanes = slice(g * HDIM, (g + 1) * HDIM)
        for a in range(2):
            keys = k_win[a * BLK:(a + 3) * BLK, lanes]
            vals = jnp.transpose(v_win[a * BLK:(a + 3) * BLK, lanes])
            heads = [q_span[a, :, (4 * g + h) * HDIM:(4 * g + h + 1) * HDIM] for h in range(4)]
            score = dot(keys, jnp.concatenate(heads, 0), ((1,), (1,)))
            low = jnp.maximum(i + 1, first * (2 - a) * BLK)
            allowed = (j >= low) & (j <= i + 2 * BLK)
            score = jnp.where(allowed, score, -jnp.inf)
            peak = jnp.max(score, axis=0, keepdims=True)
            terms = jnp.exp2((score - peak) * scale)
            sum_terms = jnp.sum(terms, axis=0, keepdims=True)
            got = dot(vals, terms.astype(BF16), ((1,), (0,)))
            got = (got * (1.0 / sum_terms)).astype(BF16)
            for h in range(4):
                head = got[:, h * BLK:(h + 1) * BLK]
                att[(4 * g + h) * HDIM:(4 * g + h + 1) * HDIM, a * BLK:(a + 1) * BLK] = head
                wide = head.astype(F32)
                sums[a] = sums[a] + jnp.sum(wide * wide, axis=0, keepdims=True)

        @pl.when(stays)
        def _():
            att_keep(g).start()

        @pl.when(jnp.logical_not(stays))
        def _():
            att_copy(g).start()

    sq_out[...] = jnp.broadcast_to(jnp.concatenate(sums, 1), (8, SPAN))

    def sq_copy(to, at):
        return pltpu.make_async_remote_copy(
            src_ref=sq_out, dst_ref=sq_in.at[at],
            send_sem=sq_send.at[to], recv_sem=sq_recv.at[at],
            device_id=(fz, fx, fy, fc, to), device_id_type=MESH,
        )

    def sq_keep():
        return pltpu.make_async_copy(sq_out, sq_in.at[hg], sq_recv.at[hg])

    for r in range(1, NH):
        sq_copy((hg + r) % NH, hg).start()

    @pl.when(stays)
    def _():
        sq_keep().start()

    @pl.when(jnp.logical_not(stays))
    def _():
        sq_copy(hg, hg).start()

    for r in range(1, NH):
        sq_copy((hg + r) % NH, (hg + r) % NH).wait_recv()

    @pl.when(stays)
    def _():
        sq_keep().wait()
        for g in range(2):
            att_keep(g).wait()

    @pl.when(jnp.logical_not(stays))
    def _():
        sq_copy(hg, hg).wait_recv()
        for g in range(2):
            att_copy(g).wait_recv()

    square = sq_in[0] + sq_in[1] + sq_in[2] + sq_in[3]
    rate = lax.rsqrt(square[0:1] / FEATS + 1e-06)

    def make_normed(k, carry):
        rows = pl.ds(pl.multiple_of(k * SDIM, SDIM), SDIM)
        gain = gcol[rows, :]
        value = att_in[rows, :].astype(F32) * jnp.concatenate([gain, gain], 1) * rate
        value = value.astype(BF16)
        normed[rows, :] = value
        weighted[rows, :] = (value.astype(F32) * w_v[k, 0:1, :]).astype(BF16)
        return carry

    lax.fori_loop(0, 16, make_normed, 0)
    states = dot(weighted[...], b_v[...], ((1,), (0,))).astype(BF16)
    for k in range(16):
        st_out[k] = states[k * SDIM:(k + 1) * SDIM]

    def st_copy(k, at):
        return pltpu.make_async_remote_copy(
            src_ref=st_out.at[k], dst_ref=st_in.at[at],
            send_sem=st_send.at[k], recv_sem=st_recv.at[at],
            device_id=plane_device(k), device_id_type=MESH,
        )

    def start_st(r, carry):
        st_copy((me + r) % PLANE, me).start()
        return carry

    lax.fori_loop(1, PLANE, start_st, 0)
    st_in[me] = st_out[me]

    def make_local(p, carry):
        lanes = pl.ds(pl.multiple_of(p * BLK, BLK), BLK)
        pair = []
        for h in range(2):
            k = 2 * p + h
            rows = pl.ds(pl.multiple_of(k * SDIM, SDIM), SDIM)
            value = normed[rows, :]
            pair.append(dot(value, mix[k], ((1,), (0,))) + value.astype(F32) * skip_ref[k])
        both = jnp.concatenate(pair, 0)
        for tb in range(2):
            part = slice(tb * BLK, (tb + 1) * BLK)
            local[part, lanes] = jnp.transpose(both[:, part])
        return carry

    lax.fori_loop(0, 8, make_local, 0)

    def wait_st(r, carry):
        st_copy((me + r) % PLANE, (me + r) % PLANE).wait_recv()
        return carry

    lax.fori_loop(1, PLANE, wait_st, 0)
    running = jnp.zeros((SDIM, STATE), F32)
    logs = jnp.zeros((8, 128), F32)
    for i in range(PLANE):
        pre_v[i] = running
        pre_log[i] = jnp.exp(logs)
        running = jnp.exp(tot_in[i][0:1]) * running + st_in[i].astype(F32)
        logs = logs + tot_in[i]
    run_out[...] = running.astype(BF16)
    run_in[z] = running.astype(BF16)

    def run_copy(to, at):
        return pltpu.make_async_remote_copy(
            src_ref=run_out, dst_ref=run_in.at[at],
            send_sem=run_send.at[to], recv_sem=run_recv.at[at],
            device_id=z_device(to), device_id_type=MESH,
        )

    def start_run(r, carry):
        run_copy((z + r) % NZ, z).start()
        return carry

    lax.fori_loop(1, NZ, start_run, 0)

    def wait_run(r, carry):
        run_copy((z + r) % NZ, (z + r) % NZ).wait_recv()
        log_copy((z + r) % NZ, (z + r) % NZ).wait_recv()
        return carry

    lax.fori_loop(1, NZ, wait_run, 0)
    carried = jnp.zeros((SDIM, STATE), F32)
    for i in range(NZ):
        later = jnp.exp(plane_in[i][0:1]) * carried + run_in[i].astype(F32)
        carried = jnp.where(i < z, later, carried)
    for i in range(PLANE):
        en_out[i] = (pre_v[i] + pre_log[i][0:1] * carried).astype(BF16)

    def en_copy(to, at):
        return pltpu.make_async_remote_copy(
            src_ref=en_out.at[to], dst_ref=en_in.at[at],
            send_sem=en_send.at[to], recv_sem=en_recv.at[at],
            device_id=plane_device(to), device_id_type=MESH,
        )

    def start_en(r, carry):
        en_copy((me + r) % PLANE, me).start()
        return carry

    lax.fori_loop(1, PLANE, start_en, 0)
    en_in[me] = en_out[me]

    def wait_en(r, carry):
        en_copy((me + r) % PLANE, (me + r) % PLANE).wait_recv()
        return carry

    lax.fori_loop(1, PLANE, wait_en, 0)
    entering = en_in[...].reshape(16 * SDIM, STATE)
    entry = dot(c_v[...], entering, ((1,), (1,)))
    out_ref[...] = (local[...] + ecum[...] * entry).astype(BF16)

    for g in range(2):
        for t in range(2):
            for slot in range(2):
                halo(t, g, slot).wait_send()
            swap(t, g).wait_send()
        q_swap(g).wait_send()
    for r in range(1, NH):
        sq_copy((hg + r) % NH, hg).wait_send()

    @pl.when(jnp.logical_not(stays))
    def _():
        sq_copy(hg, hg).wait_send()
        for g in range(2):
            att_copy(g).wait_send()

    def drain_plane(r, carry):
        to = (me + r) % PLANE
        tot_copy(to, me).wait_send()
        st_copy(to, me).wait_send()
        en_copy(to, me).wait_send()
        return carry

    lax.fori_loop(1, PLANE, drain_plane, 0)

    def drain_z(r, carry):
        to = (z + r) % NZ
        log_copy(to, z).wait_send()
        run_copy(to, z).wait_send()
        return carry

    lax.fori_loop(1, NZ, drain_z, 0)


def body(query, keys, values, norm_gain, in_b, out_c, step, log_decay, skip):
    feats = query.shape[2]
    gain = norm_gain.reshape(feats // HDIM, HDIM)
    dma = pltpu.SemaphoreType.DMA
    vm = pltpu.VMEM
    scratch = [
        vm((2, BLK, feats), BF16),
        vm((2, BLK, 256), BF16),
        vm((2, BLK, 256), BF16),
        vm((4 * BLK, 256), BF16),
        vm((4 * BLK, 256), BF16),
        vm((8, HDIM), F32),
        vm((SPAN, STATE), BF16),
        vm((SPAN, STATE), BF16),
        vm((16, SPAN), F32),
        vm((16, SPAN), F32),
        vm((16, 8, SPAN), F32),
        vm((16, 8, SPAN), F32),
        vm((16, 8, SPAN), F32),
        vm((feats, 128), F32),
        vm((16, SPAN, SPAN), BF16),
        vm((SPAN, feats), F32),
        vm((feats, SPAN), BF16),
        vm((feats, SPAN), BF16),
        vm((8, SPAN), F32),
        vm((NH, 8, SPAN), F32),
        vm((feats, SPAN), BF16),
        vm((feats, SPAN), BF16),
        vm((SPAN, feats), F32),
        vm((16, 8, 128), F32),
        vm((PLANE, 8, 128), F32),
        vm((8, 128), F32),
        vm((NZ, 8, 128), F32),
        vm((16, SDIM, STATE), BF16),
        vm((PLANE, SDIM, STATE), BF16),
        vm((PLANE, SDIM, STATE), F32),
        vm((PLANE, 8, 128), F32),
        vm((SDIM, STATE), BF16),
        vm((NZ, SDIM, STATE), BF16),
        vm((PLANE, SDIM, STATE), BF16),
        vm((16, SDIM, STATE), BF16),
        dma((10,)),
        dma((2, 2, 2)), dma((2, 2, 2)),
        dma((2, 2)), dma((2, 2)),
        dma((2,)), dma((2,)),
        dma((2,)), dma((2,)),
        dma((NH,)), dma((NH,)),
        dma((PLANE,)), dma((PLANE,)),
        dma((NZ,)), dma((NZ,)),
        dma((PLANE,)), dma((PLANE,)),
        dma((NZ,)), dma((NZ,)),
        dma((NZ,)), dma((NZ,)),
        dma((PLANE,)), dma((PLANE,)),
    ]
    anywhere = pl.BlockSpec(memory_space=pl.ANY)
    return pl.pallas_call(
        kernel,
        out_shape=jax.ShapeDtypeStruct((SPAN, feats), BF16),
        in_specs=[anywhere] * 8 + [pl.BlockSpec(memory_space=pltpu.SMEM)],
        out_specs=pl.BlockSpec(memory_space=pltpu.VMEM),
        scratch_shapes=scratch,
        compiler_params=pltpu.CompilerParams(collective_id=0, has_side_effects=True),
    )(query, keys, values, gain, in_b, out_c, step, log_decay, skip)


def solution(mesh):
    torus = Mesh(mesh.devices.reshape(NZ, NX, NY, NC, NH), AXES)
    return jax.shard_map(
        body,
        mesh=torus,
        in_specs=(
            P(None, SEQ, "head"),
            P(None, SEQ, "head"),
            P(None, SEQ, "head"),
            P("head"),
            P(SEQ, None),
            P(SEQ, None),
            P("head", SEQ),
            P("head", SEQ),
            P("head"),
        ),
        out_specs=P(SEQ, "head"),
        check_vma=False,
    )
```

```python
import math

import jax
import jax.numpy as jnp
from jax import lax
from jax.experimental import pallas as pl
from jax.experimental.pallas import tpu as pltpu
from jax.sharding import Mesh
from jax.sharding import PartitionSpec as P

HDIM = 128
SDIM = 64
STATE = 128
SPAN = 256
BLK = 128
FEATS = 4096
NZ, NX, NY, NC, NH = 8, 4, 2, 2, 4
CHIPS = NZ * NX * NY
PLANE = NX * NY * NC
CHUNKS = 4
WIDE = 256
SLICE = 16
AXES = ("z", "x", "y", "core", "head")
SEQ = ("z", "x", "y", "core")
MESH = pl.DeviceIdType.MESH
F32 = jnp.float32
BF16 = jnp.bfloat16


def chip_coords(chip):
    return chip // (NX * NY), (chip // NY) % NX, chip % NY


def seq_coords(index):
    return index // PLANE, (index // (NY * NC)) % NX, (index // NC) % NY, index % NC


def dot(a, b, dims, **kw):
    return lax.dot_general(a, b, (dims, ((), ())), preferred_element_type=F32, **kw)


def kernel(
    q_hbm, k_hbm, v_hbm, gain_hbm, b_hbm, c_hbm, step_hbm, decay_hbm, skip_ref,
    out_ref,
    q_span, k_stage, v_stage, k_win, v_win, gain_v, b_v, c_v, step_v, decay_v,
    cum_v, w_v, v_v, gcol, mix, ecum, att, z_in, att_in, sq_out, sq_in, normed, weighted, local,
    tot_out, tot_in, decays, starts, plane_out, plane_in, plane_decay,
    st_out, st_in, pre_v, run_out, run_in, en_out, en_in,
    load_sem, halo_send, halo_recv, swap_send, swap_recv, q_send, q_recv, z_send, z_recv,
    att_send, att_recv, sq_send, sq_recv, tot_send, tot_recv, log_send, log_recv,
    st_send, st_recv, run_send, run_recv, en_send, en_recv,
):
    z, x, y, core, hg = (lax.axis_index(a) for a in AXES)
    chip = (z * NX + x) * NY + y
    me = (x * NY + y) * NC + core
    other = 1 - core
    partner = (z, x, y, other, hg)

    after = (chip + 1) % CHIPS
    az, ax, ay = chip_coords(after)
    wraps = (chip == CHIPS - 1).astype(jnp.int32)
    before = (chip + CHIPS - 1) % CHIPS
    bz, bx, by = chip_coords(before)

    span = core * CHIPS + chip
    fz, fx, fy, fc = seq_coords(span)
    seq = z * PLANE + me
    sz, sx, sy = chip_coords(seq % CHIPS)
    sc = seq // CHIPS
    stays = span == seq
    z_to = (NZ // 2 * core + z // 2, x, y, z % 2, hg)
    z_from = (2 * (z % (NZ // 2)) + core, x, y, z // (NZ // 2), hg)
    z_stays = jnp.logical_and(z_to[0] == z, z_to[3] == core)
    p_to = (z, 2 * core + x // 2, x % 2, y, hg)
    p_from = (z, 2 * (x % 2) + y, core, x // 2, hg)
    p_stays = jnp.logical_and(p_to[1] == x, jnp.logical_and(p_to[2] == y, p_to[3] == core))

    mine = pl.ds(pl.multiple_of((2 + core) * BLK, BLK), BLK)
    theirs = pl.ds(pl.multiple_of((2 + other) * BLK, BLK), BLK)
    prev_row = pl.ds(pl.multiple_of(core * BLK, BLK), BLK)
    loads = [
        (decay_hbm, decay_v), (step_hbm, step_v), (k_hbm, k_stage), (v_hbm, v_stage),
        (k_hbm.at[core], k_win.at[mine]), (v_hbm.at[core], v_win.at[mine]),
        (q_hbm.at[core], q_span.at[core]),
        (b_hbm, b_v), (c_hbm, c_v), (gain_hbm, gain_v),
    ]
    loads = [pltpu.make_async_copy(s, d, load_sem.at[i]) for i, (s, d) in enumerate(loads)]
    for copy in loads:
        copy.start()

    barrier = pltpu.get_barrier_semaphore()

    def greet(device):
        pl.semaphore_signal(barrier, inc=1, device_id=device, device_id_type=MESH)

    def plane_device(index):
        return (z, index // (NY * NC), (index // NC) % NY, index % NC, hg)

    def z_device(index):
        return (index, x, y, core, hg)

    for c in range(NC):
        greet((bz, bx, by, c, hg))

    def greet_plane(r, carry):
        greet(plane_device((me + r) % PLANE))
        return carry

    lax.fori_loop(1, PLANE, greet_plane, 0)

    def greet_z(r, carry):
        greet(z_device((z + r) % NZ))
        return carry

    lax.fori_loop(1, NZ, greet_z, 0)

    @pl.when(jnp.logical_not(z_stays))
    def _():
        greet(z_from)

    for r in range(1, NH):
        greet((sz, sx, sy, sc, (hg + r) % NH))

    @pl.when(jnp.logical_not(stays))
    def _():
        greet((sz, sx, sy, sc, hg))

    loads[0].wait()
    loads[1].wait()
    row = lax.broadcasted_iota(jnp.int32, (SPAN, SPAN), 0)
    col = lax.broadcasted_iota(jnp.int32, (SPAN, SPAN), 1)
    causal = row <= col
    cum = dot(decay_v[...], causal.astype(F32), ((1,), (0,)), precision=lax.Precision.HIGHEST)
    total = cum[:, SPAN - 1:]
    tail = jnp.exp(total - cum) * step_v[...]
    shift = jnp.log(step_v[...]) - cum
    for k in range(16):
        cum_v[k] = jnp.broadcast_to(cum[k:k + 1], (8, SPAN))
        w_v[k] = jnp.broadcast_to(tail[k:k + 1], (8, SPAN))
        v_v[k] = jnp.broadcast_to(shift[k:k + 1], (8, SPAN))
    for o in range(4):
        lines = [total[4 * (n % 4) + o:4 * (n % 4) + o + 1] for n in range(8)]
        tot_out[o] = jnp.broadcast_to(jnp.concatenate(lines, 0), (8, 128))
    for copy in loads[2:]:
        copy.wait()

    moves = jnp.logical_not(stays).astype(jnp.int32) + jnp.logical_not(z_stays).astype(jnp.int32)
    pl.semaphore_wait(barrier, NC + NH - 1 + PLANE - 1 + NZ - 1 + moves)

    def remote(src, dst, send, recv, to):
        return pltpu.make_async_remote_copy(
            src_ref=src, dst_ref=dst, send_sem=send, recv_sem=recv,
            device_id=to, device_id_type=MESH,
        )

    def cols(g, width=HDIM):
        return pl.ds(g * width, width)

    def halo(i, g, slot):
        stage, window = ((k_stage, k_win), (v_stage, v_win))[i]
        to = (az, ax, ay, jnp.where(wraps == 1, 1 - slot, slot), hg)
        return remote(
            stage.at[slot, :, cols(g)], window.at[prev_row, cols(g)],
            halo_send.at[i, g, slot], halo_recv.at[i, g, core], to,
        )

    def halo_arrival(i, g, block):
        part = (k_win, v_win)[i].at[pl.ds(block * BLK, BLK), cols(g)]
        return remote(part, part, halo_send.at[i, g, 0], halo_recv.at[i, g, block], partner)

    def swap(i, g):
        stage, window = ((k_stage, k_win), (v_stage, v_win))[i]
        return remote(
            stage.at[other, :, cols(g)], window.at[mine, cols(g)],
            swap_send.at[i, g], swap_recv.at[i, g], partner,
        )

    def swap_arrival(i, g):
        part = (k_win, v_win)[i].at[theirs, cols(g)]
        return remote(part, part, swap_send.at[i, g], swap_recv.at[i, g], partner)

    def q_swap(g):
        return remote(
            q_hbm.at[other, :, cols(g, 512)], q_span.at[core, :, cols(g, 512)],
            q_send.at[g], q_recv.at[g], partner,
        )

    def q_arrival(g):
        part = q_span.at[other, :, cols(g, 512)]
        return remote(part, part, q_send.at[g], q_recv.at[g], partner)

    for g in range(2):
        for i in range(2):
            for slot in range(2):
                halo(i, g, slot).start()
        q_swap(g).start()
        for i in range(2):
            swap(i, g).start()

    def tot_copy(to, at):
        return remote(
            tot_out.at[to // 4], tot_in.at[at], tot_send.at[to], tot_recv.at[at], plane_device(to)
        )

    def start_tot(r, carry):
        tot_copy((me + r) % PLANE, me).start()
        return carry

    lax.fori_loop(1, PLANE, start_tot, 0)
    tot_in[me] = tot_out[me // 4]
    for p in range(8):
        line = jnp.broadcast_to(gain_v[p:p + 1, :], (BLK, BLK))
        gcol[p * BLK:(p + 1) * BLK, :] = jnp.transpose(line)

    scale = math.log2(math.e) / math.sqrt(HDIM)
    j = lax.broadcasted_iota(jnp.int32, (3 * BLK, 2 * BLK), 0)
    i = lax.broadcasted_iota(jnp.int32, (3 * BLK, 2 * BLK), 1) % BLK
    first = (span == 0).astype(jnp.int32)

    def part(q):
        return pl.ds(q * WIDE, WIDE)

    def z_copy(q):
        return remote(att.at[part(q)], z_in.at[part(q)], z_send.at[q], z_recv.at[q], z_to)

    def z_keep(q):
        return pltpu.make_async_copy(att.at[part(q)], z_in.at[part(q)], z_recv.at[q])

    def p_copy(q):
        return remote(z_in.at[part(q)], att_in.at[part(q)], att_send.at[q], att_recv.at[q], p_to)

    def p_keep(q):
        return pltpu.make_async_copy(z_in.at[part(q)], att_in.at[part(q)], att_recv.at[q])

    def either(here, keep, leave):
        @pl.when(here)
        def _():
            keep()

        @pl.when(jnp.logical_not(here))
        def _():
            leave()

    def sq_copy(to, at):
        return remote(
            sq_out, sq_in.at[at], sq_send.at[to], sq_recv.at[at], (fz, fx, fy, fc, to)
        )

    def sq_keep():
        return pltpu.make_async_copy(sq_out, sq_in.at[hg], sq_recv.at[hg])

    sums = [jnp.zeros((1, BLK), F32) for _ in range(2)]
    for q in range(CHUNKS):
        g = q // 2
        if q % 2 == 0:
            for t in range(2):
                for block in range(2):
                    halo_arrival(t, g, block).wait_recv()
                swap_arrival(t, g).wait_recv()
            q_arrival(g).wait_recv()
        lanes = slice(g * HDIM, (g + 1) * HDIM)
        for a in range(2):
            keys = k_win[a * BLK:(a + 3) * BLK, lanes]
            vals = jnp.transpose(v_win[a * BLK:(a + 3) * BLK, lanes])
            heads = [q_span[a, :, (2 * q + h) * HDIM:(2 * q + h + 1) * HDIM] for h in range(2)]
            score = dot(keys, jnp.concatenate(heads, 0), ((1,), (1,)))
            low = jnp.maximum(i + 1, first * (2 - a) * BLK)
            allowed = (j >= low) & (j <= i + 2 * BLK)
            score = jnp.where(allowed, score, -jnp.inf)
            peak = jnp.max(score, axis=0, keepdims=True)
            terms = jnp.exp2((score - peak) * scale)
            sum_terms = jnp.sum(terms, axis=0, keepdims=True)
            got = dot(vals, terms.astype(BF16), ((1,), (0,)))
            got = (got * (1.0 / sum_terms)).astype(BF16)
            for h in range(2):
                head = got[:, h * BLK:(h + 1) * BLK]
                att[(2 * q + h) * HDIM:(2 * q + h + 1) * HDIM, a * BLK:(a + 1) * BLK] = head
                wide = head.astype(F32)
                sums[a] = sums[a] + jnp.sum(wide * wide, axis=0, keepdims=True)
        if q == 0:
            either(z_stays, z_keep(0).start, z_copy(0).start)

    sq_out[...] = jnp.broadcast_to(jnp.concatenate(sums, 1), (8, SPAN))
    for r in range(1, NH):
        sq_copy((hg + r) % NH, hg).start()
    either(stays, sq_keep().start, sq_copy(hg, hg).start)
    for q in range(1, CHUNKS):
        either(z_stays, z_keep(q).start, z_copy(q).start)

    cross = dot(b_v[...], c_v[...], ((1,), (1,)))

    def make_mix(k, carry):
        ct = cum_v[k, 0:1, :]
        for ub in range(2):
            line = v_v[k, 0:1, ub * BLK:(ub + 1) * BLK]
            colb = jnp.transpose(jnp.broadcast_to(line, (BLK, BLK)))
            arg = ct + jnp.concatenate([colb, colb], 1)
            rows = slice(ub * BLK, (ub + 1) * BLK)
            arg = jnp.where(causal[rows], arg, -jnp.inf)
            mix[k, rows] = (jnp.exp(arg) * cross[rows]).astype(BF16)
        return carry

    lax.fori_loop(0, 16, make_mix, 0)

    def make_ecum(p, carry):
        lanes = pl.ds(pl.multiple_of(p * BLK, BLK), BLK)
        for tb in range(2):
            half = slice(tb * BLK, (tb + 1) * BLK)
            pair = [
                jnp.broadcast_to(jnp.exp(cum_v[2 * p + h, 0:1, half]), (SDIM, BLK))
                for h in range(2)
            ]
            ecum[half, lanes] = jnp.transpose(jnp.concatenate(pair, 0))
        return carry

    lax.fori_loop(0, 8, make_ecum, 0)

    def wait_tot(r, carry):
        tot_copy((me + r) % PLANE, (me + r) % PLANE).wait_recv()
        return carry

    lax.fori_loop(1, PLANE, wait_tot, 0)
    logs = jnp.zeros((8, 128), F32)
    for n in range(PLANE):
        starts[n] = jnp.exp(logs)
        decays[n] = jnp.exp(tot_in[n])
        logs = logs + tot_in[n]
    plane_out[...] = logs
    plane_in[z] = logs

    def log_copy(to, at):
        return remote(plane_out, plane_in.at[at], log_send.at[to], log_recv.at[at], z_device(to))

    def start_log(r, carry):
        log_copy((z + r) % NZ, z).start()
        return carry

    lax.fori_loop(1, NZ, start_log, 0)

    def st_copy(q, to, at):
        return remote(
            st_out.at[q, to], st_in.at[q, at], st_send.at[q, to], st_recv.at[q, at],
            plane_device(to),
        )

    def run_copy(q, to, at):
        return remote(
            run_out.at[q], run_in.at[q, at], run_send.at[q, to], run_recv.at[q, at], z_device(to)
        )

    def en_copy(q, to, at):
        return remote(
            en_out.at[q, to], en_in.at[q, at], en_send.at[q, to], en_recv.at[q, at],
            plane_device(to),
        )

    def ring(count, own, act):
        def visit(r, carry):
            act((own + r) % count)
            return carry

        lax.fori_loop(1, count, visit, 0)

    def arrive(q):
        either(z_stays, z_keep(q).wait, z_copy(q).wait_recv)
        either(p_stays, p_keep(q).start, p_copy(q).start)

    def states(q):
        if q == 0:
            for r in range(1, NH):
                sq_copy((hg + r) % NH, (hg + r) % NH).wait_recv()
            either(stays, sq_keep().wait, sq_copy(hg, hg).wait_recv)
        either(p_stays, p_keep(q).wait, p_copy(q).wait_recv)
        square = sq_in[0] + sq_in[1] + sq_in[2] + sq_in[3]
        rate = lax.rsqrt(square[0:1] / FEATS + 1e-06)

        def make_normed(k, carry):
            rows = pl.ds(pl.multiple_of(k * SDIM, SDIM), SDIM)
            gain = gcol[rows, :]
            value = att_in[rows, :].astype(F32) * jnp.concatenate([gain, gain], 1) * rate
            value = value.astype(BF16)
            normed[rows, :] = value
            weighted[rows, :] = (value.astype(F32) * w_v[k, 0:1, :]).astype(BF16)
            return carry

        lax.fori_loop(4 * q, 4 * q + 4, make_normed, 0)
        state = dot(weighted[q * WIDE:(q + 1) * WIDE], b_v[...], ((1,), (0,)))
        st_out[q] = state.astype(BF16).reshape(PLANE, SLICE, STATE)
        ring(PLANE, me, lambda to: st_copy(q, to, me).start())
        st_in[q, me] = st_out[q, me]

        def make_local(p, carry):
            lanes = pl.ds(pl.multiple_of(p * BLK, BLK), BLK)
            pair = []
            for h in range(2):
                k = 2 * p + h
                rows = pl.ds(pl.multiple_of(k * SDIM, SDIM), SDIM)
                value = normed[rows, :]
                pair.append(dot(value, mix[k], ((1,), (0,))) + value.astype(F32) * skip_ref[k])
            both = jnp.concatenate(pair, 0)
            for tb in range(2):
                half = slice(tb * BLK, (tb + 1) * BLK)
                local[half, lanes] = jnp.transpose(both[:, half])
            return carry

        lax.fori_loop(2 * q, 2 * q + 2, make_local, 0)

    def prefix(q):
        ring(PLANE, me, lambda at: st_copy(q, at, at).wait_recv())
        running = jnp.zeros((SLICE, STATE), F32)
        for n in range(PLANE):
            pre_v[q, n] = running
            running = decays[n, q:q + 1] * running + st_in[q, n].astype(F32)
        run_out[q] = running.astype(BF16)
        ring(NZ, z, lambda to: run_copy(q, to, z).start())
        run_in[q, z] = running.astype(BF16)

    def enter(q):
        if q == 0:
            ring(NZ, z, lambda at: log_copy(at, at).wait_recv())
            for n in range(NZ):
                plane_decay[n] = jnp.exp(plane_in[n])
        ring(NZ, z, lambda at: run_copy(q, at, at).wait_recv())
        carried = jnp.zeros((SLICE, STATE), F32)
        for n in range(NZ):
            later = plane_decay[n, q:q + 1] * carried + run_in[q, n].astype(F32)
            carried = jnp.where(n < z, later, carried)
        for n in range(PLANE):
            en_out[q, n] = (pre_v[q, n] + starts[n, q:q + 1] * carried).astype(BF16)
        ring(PLANE, me, lambda to: en_copy(q, to, me).start())
        en_in[q, me] = en_out[q, me]

    def finish(q):
        ring(PLANE, me, lambda at: en_copy(q, at, at).wait_recv())
        lanes = slice(q * WIDE, (q + 1) * WIDE)
        entry = dot(c_v[...], en_in[q].reshape(WIDE, STATE), ((1,), (1,)))
        out_ref[:, lanes] = (local[:, lanes] + ecum[:, lanes] * entry).astype(BF16)

    for t in range(CHUNKS + 4):
        for lag, stage in ((4, finish), (3, enter), (2, prefix), (1, states), (0, arrive)):
            if 0 <= t - lag < CHUNKS:
                stage(t - lag)

    for g in range(2):
        for t in range(2):
            for slot in range(2):
                halo(t, g, slot).wait_send()
            swap(t, g).wait_send()
        q_swap(g).wait_send()
    for r in range(1, NH):
        sq_copy((hg + r) % NH, hg).wait_send()

    @pl.when(jnp.logical_not(stays))
    def _():
        sq_copy(hg, hg).wait_send()

    @pl.when(jnp.logical_not(z_stays))
    def _():
        for q in range(CHUNKS):
            z_copy(q).wait_send()

    @pl.when(jnp.logical_not(p_stays))
    def _():
        for q in range(CHUNKS):
            p_copy(q).wait_send()

    ring(PLANE, me, lambda to: tot_copy(to, me).wait_send())
    ring(NZ, z, lambda to: log_copy(to, z).wait_send())
    for q in range(CHUNKS):
        ring(PLANE, me, lambda to: st_copy(q, to, me).wait_send())
        ring(NZ, z, lambda to: run_copy(q, to, z).wait_send())
        ring(PLANE, me, lambda to: en_copy(q, to, me).wait_send())


def body(query, keys, values, norm_gain, in_b, out_c, step, log_decay, skip):
    feats = query.shape[2]
    gain = norm_gain.reshape(feats // HDIM, HDIM)
    dma = pltpu.SemaphoreType.DMA
    vm = pltpu.VMEM
    scratch = [
        vm((2, BLK, feats), BF16),
        vm((2, BLK, 256), BF16),
        vm((2, BLK, 256), BF16),
        vm((4 * BLK, 256), BF16),
        vm((4 * BLK, 256), BF16),
        vm((8, HDIM), F32),
        vm((SPAN, STATE), BF16),
        vm((SPAN, STATE), BF16),
        vm((16, SPAN), F32),
        vm((16, SPAN), F32),
        vm((16, 8, SPAN), F32),
        vm((16, 8, SPAN), F32),
        vm((16, 8, SPAN), F32),
        vm((feats, 128), F32),
        vm((16, SPAN, SPAN), BF16),
        vm((SPAN, feats), F32),
        vm((feats, SPAN), BF16),
        vm((feats, SPAN), BF16),
        vm((feats, SPAN), BF16),
        vm((8, SPAN), F32),
        vm((NH, 8, SPAN), F32),
        vm((feats, SPAN), BF16),
        vm((feats, SPAN), BF16),
        vm((SPAN, feats), F32),
        vm((4, 8, 128), F32),
        vm((PLANE, 8, 128), F32),
        vm((PLANE, 8, 128), F32),
        vm((PLANE, 8, 128), F32),
        vm((8, 128), F32),
        vm((NZ, 8, 128), F32),
        vm((NZ, 8, 128), F32),
        vm((CHUNKS, PLANE, SLICE, STATE), BF16),
        vm((CHUNKS, PLANE, SLICE, STATE), BF16),
        vm((CHUNKS, PLANE, SLICE, STATE), F32),
        vm((CHUNKS, SLICE, STATE), BF16),
        vm((CHUNKS, NZ, SLICE, STATE), BF16),
        vm((CHUNKS, PLANE, SLICE, STATE), BF16),
        vm((CHUNKS, PLANE, SLICE, STATE), BF16),
        dma((10,)),
        dma((2, 2, 2)), dma((2, 2, 2)),
        dma((2, 2)), dma((2, 2)),
        dma((2,)), dma((2,)),
        dma((CHUNKS,)), dma((CHUNKS,)),
        dma((CHUNKS,)), dma((CHUNKS,)),
        dma((NH,)), dma((NH,)),
        dma((PLANE,)), dma((PLANE,)),
        dma((NZ,)), dma((NZ,)),
        dma((CHUNKS, PLANE)), dma((CHUNKS, PLANE)),
        dma((CHUNKS, NZ)), dma((CHUNKS, NZ)),
        dma((CHUNKS, PLANE)), dma((CHUNKS, PLANE)),
    ]
    anywhere = pl.BlockSpec(memory_space=pl.ANY)
    return pl.pallas_call(
        kernel,
        out_shape=jax.ShapeDtypeStruct((SPAN, feats), BF16),
        in_specs=[anywhere] * 8 + [pl.BlockSpec(memory_space=pltpu.SMEM)],
        out_specs=pl.BlockSpec(memory_space=pltpu.VMEM),
        scratch_shapes=scratch,
        compiler_params=pltpu.CompilerParams(collective_id=0, has_side_effects=True),
    )(query, keys, values, gain, in_b, out_c, step, log_decay, skip)


def solution(mesh):
    torus = Mesh(mesh.devices.reshape(NZ, NX, NY, NC, NH), AXES)
    return jax.shard_map(
        body,
        mesh=torus,
        in_specs=(
            P(None, SEQ, "head"),
            P(None, SEQ, "head"),
            P(None, SEQ, "head"),
            P("head"),
            P(SEQ, None),
            P(SEQ, None),
            P("head", SEQ),
            P("head", SEQ),
            P("head"),
        ),
        out_specs=P(SEQ, "head"),
        check_vma=False,
    )
```

```python
import math

import jax
import jax.numpy as jnp
from jax import lax
from jax.experimental import pallas as pl
from jax.experimental.pallas import tpu as pltpu
from jax.sharding import Mesh
from jax.sharding import PartitionSpec as P

HDIM = 128
SDIM = 64
STATE = 128
SPAN = 256
BLK = 128
FEATS = 4096
NZ, NX, NY, NC, NH = 8, 4, 2, 2, 4
CHIPS = NZ * NX * NY
PLANE = NX * NY * NC
CHUNKS = 4
WIDE = 256
HALVES = 2
HALF = 512
SLICE = 32
AXES = ("z", "x", "y", "core", "head")
SEQ = ("z", "x", "y", "core")
MESH = pl.DeviceIdType.MESH
F32 = jnp.float32
BF16 = jnp.bfloat16


def chip_coords(chip):
    return chip // (NX * NY), (chip // NY) % NX, chip % NY


def seq_coords(index):
    return index // PLANE, (index // (NY * NC)) % NX, (index // NC) % NY, index % NC


def dot(a, b, dims, **kw):
    return lax.dot_general(a, b, (dims, ((), ())), preferred_element_type=F32, **kw)


def kernel(
    q_hbm, k_hbm, v_hbm, gain_hbm, b_hbm, c_hbm, step_hbm, decay_hbm, skip_ref,
    out_ref,
    q_span, k_stage, v_stage, k_win, v_win, gain_v, b_v, c_v, step_v, decay_v,
    cum_v, w_v, v_v, gcol, mix, ecum, att, z_in, att_in, sq_out, sq_mid, sq_in, normed, weighted, local,
    tot_out, tot_in, decays, starts, plane_out, plane_in,
    st_out, st_in, pre_v, run_out, run_in, en_out, en_in,
    load_sem, halo_send, halo_recv, swap_send, swap_recv, q_send, q_recv, z_send, z_recv,
    relay_send, att_send, att_recv, sqz_send, sqz_recv, sqr_send, sq_send, sq_recv,
    tot_send, tot_recv, log_send, log_recv, st_send, st_recv, run_send, run_recv,
    en_send, en_recv, ready_sem, later_sem,
):
    z, x, y, core, hg = (lax.axis_index(a) for a in AXES)
    chip = (z * NX + x) * NY + y
    me = (x * NY + y) * NC + core
    other = 1 - core
    partner = (z, x, y, other, hg)

    after = (chip + 1) % CHIPS
    az, ax, ay = chip_coords(after)
    wraps = (chip == CHIPS - 1).astype(jnp.int32)
    before = (chip + CHIPS - 1) % CHIPS
    bz, bx, by = chip_coords(before)

    span = core * CHIPS + chip
    long_out = z == jnp.where(core == 0, NZ - 1, 0)
    long_out = jnp.where(long_out, 1, 0)
    relays = jnp.where(z == jnp.where(core == 0, 1, NZ - 2), 1, 0)
    long_in = jnp.where(z == jnp.where(core == 0, NZ // 2, NZ // 2 - 1), 1, 0)
    relay_of = jnp.where(core == 0, 1, NZ - 2)
    to_z = jnp.where(long_out == 1, relay_of, NZ // 2 * core + z // 2)
    to_core = jnp.where(long_out == 1, core, z % 2)
    z_to = (to_z, x, y, to_core, hg)
    from_z = jnp.where(long_in == 1, jnp.where(core == 0, NZ - 2, 1), 2 * (z % (NZ // 2)) + core)
    from_core = jnp.where(long_in == 1, other, z // (NZ // 2))
    z_from = (from_z, x, y, from_core, hg)
    relay_from = (jnp.where(core == 0, NZ - 1, 0), x, y, core, hg)
    relay_to = (jnp.where(core == 0, NZ // 2 - 1, NZ // 2), x, y, other, hg)
    z_stays = jnp.logical_and(to_z == z, to_core == core)
    z_moves = jnp.logical_not(z_stays)
    relaying = relays == 1
    p_to = (z, 2 * core + x // 2, x % 2, y, hg)
    p_from = (z, 2 * (x % 2) + y, core, x // 2, hg)
    p_stays = jnp.logical_and(p_to[1] == x, jnp.logical_and(p_to[2] == y, p_to[3] == core))
    p_moves = jnp.logical_not(p_stays)

    mine = pl.ds(pl.multiple_of((2 + core) * BLK, BLK), BLK)
    theirs = pl.ds(pl.multiple_of((2 + other) * BLK, BLK), BLK)
    prev_row = pl.ds(pl.multiple_of(core * BLK, BLK), BLK)
    loads = [
        (decay_hbm, decay_v), (step_hbm, step_v), (k_hbm, k_stage), (v_hbm, v_stage),
        (k_hbm.at[core], k_win.at[mine]), (v_hbm.at[core], v_win.at[mine]),
        (q_hbm.at[core], q_span.at[core]),
        (b_hbm, b_v), (c_hbm, c_v), (gain_hbm, gain_v),
    ]
    loads = [pltpu.make_async_copy(s, d, load_sem.at[i]) for i, (s, d) in enumerate(loads)]
    for copy in loads:
        copy.start()

    barrier = pltpu.get_barrier_semaphore()

    def greet(device):
        pl.semaphore_signal(barrier, inc=1, device_id=device, device_id_type=MESH)

    def plane_device(index):
        return (z, index // (NY * NC), (index // NC) % NY, index % NC, hg)

    def z_device(index):
        return (index, x, y, core, hg)

    def ring(act):
        def visit(r, carry):
            act((me + r) % PLANE)
            return carry

        lax.fori_loop(1, PLANE, visit, 0)

    def each(low, high, act):
        def visit(n, carry):
            act(n)
            return carry

        lax.fori_loop(low, high, visit, 0)

    greet((bz, bx, by, 0, hg))
    greet((bz, bx, by, 1, hg))
    ring(lambda n: greet(plane_device(n)))
    for r in range(1, NH):
        greet((z, p_from[1], p_from[2], p_from[3], (hg + r) % NH))

    @pl.when(jnp.logical_and(z_moves, from_z > z))
    def _():
        greet(z_from)

    @pl.when(jnp.logical_and(z_moves, to_z > z))
    def _():
        greet(z_to)

    @pl.when(jnp.logical_and(relaying, core == 0))
    def _():
        greet(relay_from)
        greet(relay_to)

    each(z + 1, NZ, lambda n: greet(z_device(n)))

    loads[0].wait()
    loads[1].wait()
    row = lax.broadcasted_iota(jnp.int32, (SPAN, SPAN), 0)
    col = lax.broadcasted_iota(jnp.int32, (SPAN, SPAN), 1)
    causal = row <= col
    cum = dot(decay_v[...], causal.astype(F32), ((1,), (0,)), precision=lax.Precision.HIGHEST)
    total = cum[:, SPAN - 1:]
    tail = jnp.exp(total - cum) * step_v[...]
    shift = jnp.log(step_v[...]) - cum
    for k in range(16):
        cum_v[k] = jnp.broadcast_to(cum[k:k + 1], (8, SPAN))
        w_v[k] = jnp.broadcast_to(tail[k:k + 1], (8, SPAN))
        v_v[k] = jnp.broadcast_to(shift[k:k + 1], (8, SPAN))
    for o in range(8):
        lines = [total[8 * (n % 2) + o:8 * (n % 2) + o + 1] for n in range(8)]
        tot_out[o] = jnp.broadcast_to(jnp.concatenate(lines, 0), (8, 128))
    for copy in loads[2:]:
        copy.wait()

    @pl.when(span == 0)
    def _():
        k_win[:2 * BLK] = jnp.zeros((2 * BLK, 256), BF16)
        v_win[:2 * BLK] = jnp.zeros((2 * BLK, 256), BF16)

    def one(condition):
        return jnp.where(condition, 1, 0)

    greeted = (
        z + one(jnp.logical_and(z_moves, to_z < z)) + one(jnp.logical_and(z_moves, from_z < z))
        + 2 * one(jnp.logical_and(relaying, core == 1))
    )
    pl.semaphore_wait(barrier, NC + PLANE - 1 + NH - 1 + greeted)

    def reply(semaphore, device):
        pl.semaphore_signal(semaphore, inc=1, device_id=device, device_id_type=MESH)

    each(0, z, lambda n: reply(later_sem, z_device(n)))

    @pl.when(jnp.logical_and(z_moves, from_z < z))
    def _():
        reply(ready_sem, z_from)

    @pl.when(jnp.logical_and(relaying, core == 1))
    def _():
        reply(ready_sem, relay_from)

    def remote(src, dst, send, recv, to):
        return pltpu.make_async_remote_copy(
            src_ref=src, dst_ref=dst, send_sem=send, recv_sem=recv,
            device_id=to, device_id_type=MESH,
        )

    def cols(g, width=HDIM):
        return pl.ds(g * width, width)

    def halo(i, g, slot):
        stage, window = ((k_stage, k_win), (v_stage, v_win))[i]
        to = (az, ax, ay, jnp.where(wraps == 1, 1 - slot, slot), hg)
        return remote(
            stage.at[slot, :, cols(g)], window.at[prev_row, cols(g)],
            halo_send.at[i, g, slot], halo_recv.at[i, g, core], to,
        )

    def halo_arrival(i, g, block):
        part = (k_win, v_win)[i].at[pl.ds(block * BLK, BLK), cols(g)]
        return remote(part, part, halo_send.at[i, g, 0], halo_recv.at[i, g, block], partner)

    def swap(i, g):
        stage, window = ((k_stage, k_win), (v_stage, v_win))[i]
        return remote(
            stage.at[other, :, cols(g)], window.at[mine, cols(g)],
            swap_send.at[i, g], swap_recv.at[i, g], partner,
        )

    def swap_arrival(i, g):
        part = (k_win, v_win)[i].at[theirs, cols(g)]
        return remote(part, part, swap_send.at[i, g], swap_recv.at[i, g], partner)

    def q_swap(g):
        return remote(
            q_hbm.at[other, :, cols(g, 512)], q_span.at[core, :, cols(g, 512)],
            q_send.at[g], q_recv.at[g], partner,
        )

    def q_arrival(g):
        part = q_span.at[other, :, cols(g, 512)]
        return remote(part, part, q_send.at[g], q_recv.at[g], partner)

    last_chip = chip == CHIPS - 1
    for g in range(2):
        for i in range(2):
            halo(i, g, 0).start()
            pl.when(jnp.logical_not(last_chip))(halo(i, g, 1).start)
        q_swap(g).start()
        for i in range(2):
            swap(i, g).start()

    def tot_copy(to):
        return remote(
            tot_out.at[to // 2], tot_in.at[me], tot_send.at[0], tot_recv.at[0], plane_device(to)
        )

    ring(lambda to: tot_copy(to).start())
    tot_in[me] = tot_out[me // 2]
    for p in range(8):
        line = jnp.broadcast_to(gain_v[p:p + 1, :], (BLK, BLK))
        gcol[p * BLK:(p + 1) * BLK, :] = jnp.transpose(line)

    scale = math.log2(math.e) / math.sqrt(HDIM)
    j = lax.broadcasted_iota(jnp.int32, (3 * BLK, 4 * BLK), 0)
    i = lax.broadcasted_iota(jnp.int32, (3 * BLK, 4 * BLK), 1) % BLK
    first = one(span == 0)

    def part(q):
        return pl.ds(q * WIDE, WIDE)

    def z_copy(q):
        return remote(
            att.at[part(q)], z_in.at[long_out, part(q)], z_send.at[q], z_recv.at[long_out, q], z_to
        )

    def z_keep(q):
        return pltpu.make_async_copy(att.at[part(q)], z_in.at[0, part(q)], z_recv.at[0, q])

    def relay_copy(q):
        return remote(
            z_in.at[1, part(q)], z_in.at[0, part(q)], relay_send.at[q], z_recv.at[0, q], relay_to
        )

    def z_arrival(at, q):
        return remote(
            z_in.at[at, part(q)], z_in.at[at, part(q)], relay_send.at[q], z_recv.at[at, q], relay_to
        )

    def p_copy(q):
        return remote(z_in.at[0, part(q)], att_in.at[part(q)], att_send.at[q], att_recv.at[q], p_to)

    def p_keep(q):
        return pltpu.make_async_copy(z_in.at[0, part(q)], att_in.at[part(q)], att_recv.at[q])

    def either(here, keep, leave):
        pl.when(here)(keep)
        pl.when(jnp.logical_not(here))(leave)

    def sqz_copy():
        return remote(sq_out, sq_mid.at[long_out], sqz_send.at[0], sqz_recv.at[long_out], z_to)

    def sqz_keep():
        return pltpu.make_async_copy(sq_out, sq_mid.at[0], sqz_recv.at[0])

    def sqr_copy():
        return remote(sq_mid.at[1], sq_mid.at[0], sqr_send.at[0], sqz_recv.at[0], relay_to)

    def sqz_arrival(at):
        return remote(sq_mid.at[at], sq_mid.at[at], sqr_send.at[0], sqz_recv.at[at], relay_to)

    def sq_copy(to, at):
        return remote(
            sq_mid.at[0], sq_in.at[at], sq_send.at[to], sq_recv.at[at],
            (z, p_to[1], p_to[2], p_to[3], to),
        )

    def sq_keep():
        return pltpu.make_async_copy(sq_mid.at[0], sq_in.at[hg], sq_recv.at[hg])

    sums = [jnp.zeros((1, BLK), F32) for _ in range(2)]
    for g in range(2):
        @pl.when(span > 0)
        def _():
            for t in range(2):
                for block in range(2):
                    halo_arrival(t, g, block).wait_recv()

        for t in range(2):
            swap_arrival(t, g).wait_recv()
        q_arrival(g).wait_recv()
        lanes = slice(g * HDIM, (g + 1) * HDIM)
        for a in range(2):
            keys = k_win[a * BLK:(a + 3) * BLK, lanes]
            vals = jnp.transpose(v_win[a * BLK:(a + 3) * BLK, lanes])
            heads = [q_span[a, :, (4 * g + h) * HDIM:(4 * g + h + 1) * HDIM] for h in range(4)]
            score = dot(keys, jnp.concatenate(heads, 0), ((1,), (1,)))
            low = jnp.maximum(i + 1, first * (2 - a) * BLK)
            allowed = (j >= low) & (j <= i + 2 * BLK)
            score = jnp.where(allowed, score, -jnp.inf)
            peak = jnp.max(score, axis=0, keepdims=True)
            terms = jnp.exp2((score - peak) * scale)
            sum_terms = jnp.sum(terms, axis=0, keepdims=True)
            got = dot(vals, terms.astype(BF16), ((1,), (0,)))
            got = (got * (1.0 / sum_terms)).astype(BF16)
            for h in range(4):
                head = got[:, h * BLK:(h + 1) * BLK]
                att[(4 * g + h) * HDIM:(4 * g + h + 1) * HDIM, a * BLK:(a + 1) * BLK] = head
                wide = head.astype(F32)
                sums[a] = sums[a] + jnp.sum(wide * wide, axis=0, keepdims=True)
        if g == 0:
            @pl.when(jnp.logical_and(z_moves, to_z > z))
            def _():
                pl.semaphore_wait(ready_sem, 1)
        else:
            sq_out[...] = jnp.broadcast_to(jnp.concatenate(sums, 1), (8, SPAN))
            either(z_stays, lambda: sqz_keep().start(), lambda: sqz_copy().start())
        for q in (2 * g, 2 * g + 1):
            either(z_stays, z_keep(q).start, z_copy(q).start)

    cross = dot(b_v[...], c_v[...], ((1,), (1,)))

    def make_mix(k, carry):
        ct = cum_v[k, 0:1, :]
        for ub in range(2):
            line = v_v[k, 0:1, ub * BLK:(ub + 1) * BLK]
            colb = jnp.transpose(jnp.broadcast_to(line, (BLK, BLK)))
            arg = ct + jnp.concatenate([colb, colb], 1)
            rows = slice(ub * BLK, (ub + 1) * BLK)
            arg = jnp.where(causal[rows], arg, -jnp.inf)
            mix[k, rows] = (jnp.exp(arg) * cross[rows]).astype(BF16)
        return carry

    lax.fori_loop(0, 16, make_mix, 0)

    def make_ecum(p, carry):
        lanes = pl.ds(pl.multiple_of(p * BLK, BLK), BLK)
        for tb in range(2):
            half = slice(tb * BLK, (tb + 1) * BLK)
            pair = [
                jnp.broadcast_to(jnp.exp(cum_v[2 * p + h, 0:1, half]), (SDIM, BLK))
                for h in range(2)
            ]
            ecum[half, lanes] = jnp.transpose(jnp.concatenate(pair, 0))
        return carry

    lax.fori_loop(0, 8, make_ecum, 0)

    @pl.when(jnp.logical_and(relaying, core == 0))
    def _():
        pl.semaphore_wait(ready_sem, 1)

    def arrive(q):
        @pl.when(relaying)
        def _():
            z_arrival(1, q).wait_recv()
            relay_copy(q).start()

        either(z_stays, z_keep(q).wait, z_arrival(0, q).wait_recv)
        either(p_stays, p_keep(q).start, p_copy(q).start)

    def arrive_squares():
        @pl.when(relaying)
        def _():
            sqz_arrival(1).wait_recv()
            sqr_copy().start()

        either(z_stays, lambda: sqz_keep().wait(), lambda: sqz_arrival(0).wait_recv())
        for r in range(1, NH):
            sq_copy((hg + r) % NH, hg).start()
        either(p_stays, lambda: sq_keep().start(), lambda: sq_copy(hg, hg).start())

    def st_copy(q, to):
        return remote(
            st_out.at[q, to], st_in.at[q, me], st_send.at[q], st_recv.at[q], plane_device(to)
        )

    def run_copy(q, to, at):
        return remote(
            run_out.at[q], run_in.at[q, at], run_send.at[q, to], run_recv.at[q, at], z_device(to)
        )

    def log_copy(to, at):
        return remote(plane_out, plane_in.at[at], log_send.at[to], log_recv.at[at], z_device(to))

    def en_copy(q, to):
        return remote(
            en_out.at[q, to], en_in.at[q, me], en_send.at[q], en_recv.at[q], plane_device(to)
        )

    def sent(buffer, semaphore):
        rest = buffer.at[pl.ds(0, PLANE - 1)]
        return remote(rest, rest, semaphore, semaphore, partner)

    def states(q):
        if q == 0:
            for r in range(1, NH):
                sq_copy((hg + r) % NH, (hg + r) % NH).wait_recv()
            either(p_stays, lambda: sq_keep().wait(), lambda: sq_copy(hg, hg).wait_recv())
        for c in (2 * q, 2 * q + 1):
            either(p_stays, p_keep(c).wait, p_copy(c).wait_recv)
        square = sq_in[0] + sq_in[1] + sq_in[2] + sq_in[3]
        rate = lax.rsqrt(square[0:1] / FEATS + 1e-06)

        def make_normed(k, carry):
            rows = pl.ds(pl.multiple_of(k * SDIM, SDIM), SDIM)
            gain = gcol[rows, :]
            value = att_in[rows, :].astype(F32) * jnp.concatenate([gain, gain], 1) * rate
            value = value.astype(BF16)
            normed[rows, :] = value
            weighted[rows, :] = (value.astype(F32) * w_v[k, 0:1, :]).astype(BF16)
            return carry

        lax.fori_loop(8 * q, 8 * q + 8, make_normed, 0)
        state = dot(weighted[q * HALF:(q + 1) * HALF], b_v[...], ((1,), (0,)))
        st_out[q] = state.astype(BF16).reshape(PLANE, SLICE, STATE)
        ring(lambda to: st_copy(q, to).start())
        st_in[q, me] = st_out[q, me]

    def locals_(q):
        def make_local(p, carry):
            lanes = pl.ds(pl.multiple_of(p * BLK, BLK), BLK)
            pair = []
            for h in range(2):
                k = 2 * p + h
                rows = pl.ds(pl.multiple_of(k * SDIM, SDIM), SDIM)
                value = normed[rows, :]
                pair.append(dot(value, mix[k], ((1,), (0,))) + value.astype(F32) * skip_ref[k])
            both = jnp.concatenate(pair, 0)
            for tb in range(2):
                half = slice(tb * BLK, (tb + 1) * BLK)
                local[half, lanes] = jnp.transpose(both[:, half])
            return carry

        lax.fori_loop(4 * q, 4 * q + 4, make_local, 0)

    def prefix(q):
        sent(st_in.at[q], st_recv.at[q]).wait_recv()
        running = jnp.zeros((SLICE, STATE), F32)
        for n in range(PLANE):
            pre_v[q, n] = running
            running = decays[n, q:q + 1] * running + st_in[q, n].astype(F32)
        run_out[q] = running.astype(BF16)
        each(z + 1, NZ, lambda to: run_copy(q, to, z).start())

    def enter(q):
        if q == 0:
            each(0, z, lambda n: log_copy(n, n).wait_recv())

        def gather(n, carried):
            run_copy(q, n, n).wait_recv()
            decay = jnp.exp(plane_in[n])
            return decay[q:q + 1] * carried + run_in[q, n].astype(F32)

        carried = lax.fori_loop(0, z, gather, jnp.zeros((SLICE, STATE), F32))
        for n in range(PLANE):
            en_out[q, n] = (pre_v[q, n] + starts[n, q:q + 1] * carried).astype(BF16)
        ring(lambda to: en_copy(q, to).start())
        en_in[q, me] = en_out[q, me]

    def finish(q):
        sent(en_in.at[q], en_recv.at[q]).wait_recv()
        lanes = slice(q * HALF, (q + 1) * HALF)
        entry = dot(c_v[...], en_in[q].reshape(HALF, STATE), ((1,), (1,)))
        out_ref[:, lanes] = (local[:, lanes] + ecum[:, lanes] * entry).astype(BF16)

    arrive(0)
    arrive(1)
    arrive_squares()

    sent(tot_in, tot_recv.at[0]).wait_recv()
    logs = jnp.zeros((8, 128), F32)
    for n in range(PLANE):
        starts[n] = jnp.exp(logs)
        decays[n] = jnp.exp(tot_in[n])
        logs = logs + tot_in[n]
    plane_out[...] = logs

    @pl.when(z < NZ - 1)
    def _():
        pl.semaphore_wait(later_sem, NZ - 1 - z)

    each(z + 1, NZ, lambda to: log_copy(to, z).start())
    states(0)
    arrive(2)
    arrive(3)
    locals_(0)
    states(1)
    locals_(1)
    for stage in (prefix, enter, finish):
        for q in range(HALVES):
            stage(q)

    for g in range(2):
        for t in range(2):
            halo(t, g, 0).wait_send()
            pl.when(jnp.logical_not(last_chip))(halo(t, g, 1).wait_send)
            swap(t, g).wait_send()
        q_swap(g).wait_send()
    for r in range(1, NH):
        sq_copy((hg + r) % NH, hg).wait_send()

    @pl.when(z_moves)
    def _():
        sqz_copy().wait_send()
        for q in range(CHUNKS):
            z_copy(q).wait_send()

    @pl.when(relaying)
    def _():
        sqr_copy().wait_send()
        for q in range(CHUNKS):
            relay_copy(q).wait_send()

    @pl.when(p_moves)
    def _():
        sq_copy(hg, hg).wait_send()
        for q in range(CHUNKS):
            p_copy(q).wait_send()

    sent(tot_in, tot_send.at[0]).wait_send()
    each(z + 1, NZ, lambda to: log_copy(to, z).wait_send())
    for q in range(HALVES):
        sent(st_out.at[q], st_send.at[q]).wait_send()
        each(z + 1, NZ, lambda to: run_copy(q, to, z).wait_send())
        sent(en_out.at[q], en_send.at[q]).wait_send()


def body(query, keys, values, norm_gain, in_b, out_c, step, log_decay, skip):
    feats = query.shape[2]
    gain = norm_gain.reshape(feats // HDIM, HDIM)
    dma = pltpu.SemaphoreType.DMA
    vm = pltpu.VMEM
    scratch = [
        vm((2, BLK, feats), BF16),
        vm((2, BLK, 256), BF16),
        vm((2, BLK, 256), BF16),
        vm((4 * BLK, 256), BF16),
        vm((4 * BLK, 256), BF16),
        vm((8, HDIM), F32),
        vm((SPAN, STATE), BF16),
        vm((SPAN, STATE), BF16),
        vm((16, SPAN), F32),
        vm((16, SPAN), F32),
        vm((16, 8, SPAN), F32),
        vm((16, 8, SPAN), F32),
        vm((16, 8, SPAN), F32),
        vm((feats, 128), F32),
        vm((16, SPAN, SPAN), BF16),
        vm((SPAN, feats), F32),
        vm((feats, SPAN), BF16),
        vm((2, feats, SPAN), BF16),
        vm((feats, SPAN), BF16),
        vm((8, SPAN), F32),
        vm((2, 8, SPAN), F32),
        vm((NH, 8, SPAN), F32),
        vm((feats, SPAN), BF16),
        vm((feats, SPAN), BF16),
        vm((SPAN, feats), F32),
        vm((8, 8, 128), F32),
        vm((PLANE, 8, 128), F32),
        vm((PLANE, 8, 128), F32),
        vm((PLANE, 8, 128), F32),
        vm((8, 128), F32),
        vm((NZ, 8, 128), F32),
        vm((HALVES, PLANE, SLICE, STATE), BF16),
        vm((HALVES, PLANE, SLICE, STATE), BF16),
        vm((HALVES, PLANE, SLICE, STATE), F32),
        vm((HALVES, SLICE, STATE), BF16),
        vm((HALVES, NZ, SLICE, STATE), BF16),
        vm((HALVES, PLANE, SLICE, STATE), BF16),
        vm((HALVES, PLANE, SLICE, STATE), BF16),
        dma((10,)),
        dma((2, 2, 2)), dma((2, 2, 2)),
        dma((2, 2)), dma((2, 2)),
        dma((2,)), dma((2,)),
        dma((CHUNKS,)), dma((2, CHUNKS)),
        dma((CHUNKS,)),
        dma((CHUNKS,)), dma((CHUNKS,)),
        dma((1,)), dma((2,)), dma((1,)),
        dma((NH,)), dma((NH,)),
        dma((1,)), dma((1,)),
        dma((NZ,)), dma((NZ,)),
        dma((HALVES,)), dma((HALVES,)),
        dma((HALVES, NZ)), dma((HALVES, NZ)),
        dma((HALVES,)), dma((HALVES,)),
        pltpu.SemaphoreType.REGULAR,
        pltpu.SemaphoreType.REGULAR,
    ]
    anywhere = pl.BlockSpec(memory_space=pl.ANY)
    return pl.pallas_call(
        kernel,
        out_shape=jax.ShapeDtypeStruct((SPAN, feats), BF16),
        in_specs=[anywhere] * 8 + [pl.BlockSpec(memory_space=pltpu.SMEM)],
        out_specs=pl.BlockSpec(memory_space=pltpu.VMEM),
        scratch_shapes=scratch,
        compiler_params=pltpu.CompilerParams(collective_id=0, has_side_effects=True),
    )(query, keys, values, gain, in_b, out_c, step, log_decay, skip)


def solution(mesh):
    torus = Mesh(mesh.devices.reshape(NZ, NX, NY, NC, NH), AXES)
    return jax.shard_map(
        body,
        mesh=torus,
        in_specs=(
            P(None, SEQ, "head"),
            P(None, SEQ, "head"),
            P(None, SEQ, "head"),
            P("head"),
            P(SEQ, None),
            P(SEQ, None),
            P("head", SEQ),
            P("head", SEQ),
            P("head"),
        ),
        out_specs=P(SEQ, "head"),
        check_vma=False,
    )
```

```python
import math

import jax
import jax.numpy as jnp
from jax import lax
from jax.experimental import pallas as pl
from jax.experimental.pallas import tpu as pltpu
from jax.sharding import Mesh
from jax.sharding import PartitionSpec as P

HDIM = 128
SDIM = 64
STATE = 128
SPAN = 256
BLK = 128
FEATS = 4096
NZ, NX, NY, NC, NH = 8, 4, 2, 2, 4
CHIPS = NZ * NX * NY
PLANE = NX * NY * NC
CHUNKS = 4
WIDE = 256
HALVES = 2
HALF = 512
SLICE = 32
AXES = ("z", "x", "y", "core", "head")
SEQ = ("z", "x", "y", "core")
MESH = pl.DeviceIdType.MESH
F32 = jnp.float32
BF16 = jnp.bfloat16


def chip_coords(chip):
    return chip // (NX * NY), (chip // NY) % NX, chip % NY


def seq_coords(index):
    return index // PLANE, (index // (NY * NC)) % NX, (index // NC) % NY, index % NC


def dot(a, b, dims, **kw):
    return lax.dot_general(a, b, (dims, ((), ())), preferred_element_type=F32, **kw)


def kernel(
    q_hbm, k_hbm, v_hbm, gain_hbm, b_hbm, c_hbm, step_hbm, decay_hbm, skip_ref,
    out_ref,
    q_span, k_stage, v_stage, k_win, v_win, gain_v, b_v, c_v, step_v, decay_v,
    cum_v, v_v, gcol, mix, ecum, att, z_in, att_in, sq_out, sq_mid, sq_in, sq_here, weighted, local,
    w_out, w_here, b_here, tot_here, tot_out, tot_in, run_tot, starts, plane_out, plane_in,
    st_out, st_in, pre_out, pre_in, run_out, run_in, en_out, en_in,
    load_sem, halo_send, halo_recv, swap_send, swap_recv, q_send, q_recv, z_send, z_recv,
    relay_send, att_send, att_recv, sqz_send, sqz_recv, sqr_send, sq_send, sq_recv,
    here_send, here_recv, home_send, home_recv, vtot_send, vtot_recv, pre_send, pre_recv,
    tot_send, tot_recv, log_send, log_recv, st_send, st_recv, run_send, run_recv,
    en_send, en_recv, ready_sem, later_sem, home_ready,
):
    z, x, y, core, hg = (lax.axis_index(a) for a in AXES)
    chip = (z * NX + x) * NY + y
    me = (x * NY + y) * NC + core
    other = 1 - core
    partner = (z, x, y, other, hg)

    after = (chip + 1) % CHIPS
    az, ax, ay = chip_coords(after)
    wraps = (chip == CHIPS - 1).astype(jnp.int32)
    before = (chip + CHIPS - 1) % CHIPS
    bz, bx, by = chip_coords(before)

    span = core * CHIPS + chip
    long_out = z == jnp.where(core == 0, NZ - 1, 0)
    long_out = jnp.where(long_out, 1, 0)
    relays = jnp.where(z == jnp.where(core == 0, 1, NZ - 2), 1, 0)
    long_in = jnp.where(z == jnp.where(core == 0, NZ // 2, NZ // 2 - 1), 1, 0)
    relay_of = jnp.where(core == 0, 1, NZ - 2)
    to_z = jnp.where(long_out == 1, relay_of, NZ // 2 * core + z // 2)
    to_core = jnp.where(long_out == 1, core, z % 2)
    z_to = (to_z, x, y, to_core, hg)
    from_z = jnp.where(long_in == 1, jnp.where(core == 0, NZ - 2, 1), 2 * (z % (NZ // 2)) + core)
    from_core = jnp.where(long_in == 1, other, z // (NZ // 2))
    z_from = (from_z, x, y, from_core, hg)
    relay_from = (jnp.where(core == 0, NZ - 1, 0), x, y, core, hg)
    relay_to = (jnp.where(core == 0, NZ // 2 - 1, NZ // 2), x, y, other, hg)
    z_stays = jnp.logical_and(to_z == z, to_core == core)
    z_moves = jnp.logical_not(z_stays)
    relaying = relays == 1
    p_to = (z, 2 * core + x // 2, x % 2, y, hg)
    p_from = (z, 2 * (x % 2) + y, core, x // 2, hg)
    p_stays = jnp.logical_and(p_to[1] == x, jnp.logical_and(p_to[2] == y, p_to[3] == core))
    p_moves = jnp.logical_not(p_stays)

    seq = z * PLANE + me
    fz, fx, fy, fc = seq_coords(span)
    home = (fz, fx, fy, fc, hg)
    sz, sx, sy = chip_coords(seq % CHIPS)
    away = (sz, sx, sy, seq // CHIPS, hg)
    stays = span == seq

    mine = pl.ds(pl.multiple_of((2 + core) * BLK, BLK), BLK)
    theirs = pl.ds(pl.multiple_of((2 + other) * BLK, BLK), BLK)
    prev_row = pl.ds(pl.multiple_of(core * BLK, BLK), BLK)
    loads = [
        (decay_hbm, decay_v), (step_hbm, step_v), (k_hbm, k_stage), (v_hbm, v_stage),
        (k_hbm.at[core], k_win.at[mine]), (v_hbm.at[core], v_win.at[mine]),
        (q_hbm.at[core], q_span.at[core]),
        (b_hbm, b_v), (c_hbm, c_v), (gain_hbm, gain_v),
    ]
    loads = [pltpu.make_async_copy(s, d, load_sem.at[i]) for i, (s, d) in enumerate(loads)]
    for copy in loads:
        copy.start()

    barrier = pltpu.get_barrier_semaphore()

    def greet(device):
        pl.semaphore_signal(barrier, inc=1, device_id=device, device_id_type=MESH)

    def plane_device(index):
        return (z, index // (NY * NC), (index // NC) % NY, index % NC, hg)

    def z_device(index):
        return (index, x, y, core, hg)

    def ring(act):
        def visit(r, carry):
            act((me + r) % PLANE)
            return carry

        lax.fori_loop(1, PLANE, visit, 0)

    def each(low, high, act):
        def visit(n, carry):
            act(n)
            return carry

        lax.fori_loop(low, high, visit, 0)

    greet((bz, bx, by, 0, hg))
    greet((bz, bx, by, 1, hg))
    ring(lambda n: greet(plane_device(n)))
    for r in range(1, NH):
        greet((z, p_from[1], p_from[2], p_from[3], (hg + r) % NH))

    @pl.when(jnp.logical_and(z_moves, from_z > z))
    def _():
        greet(z_from)

    @pl.when(jnp.logical_and(z_moves, to_z > z))
    def _():
        greet(z_to)

    @pl.when(jnp.logical_and(relaying, core == 0))
    def _():
        greet(relay_from)
        greet(relay_to)

    each(z + 1, NZ, lambda n: greet(z_device(n)))
    for r in range(1, NH):
        greet((z, x, y, core, (hg + r) % NH))

    @pl.when(fz > z)
    def _():
        greet(home)

    @pl.when(sz > z)
    def _():
        greet(away)

    loads[0].wait()
    loads[1].wait()
    row = lax.broadcasted_iota(jnp.int32, (SPAN, SPAN), 0)
    col = lax.broadcasted_iota(jnp.int32, (SPAN, SPAN), 1)
    causal = row <= col
    cum = dot(decay_v[...], causal.astype(F32), ((1,), (0,)), precision=lax.Precision.HIGHEST)
    total = cum[:, SPAN - 1:]
    w_out[...] = jnp.exp(total - cum) * step_v[...]
    shift = jnp.log(step_v[...]) - cum
    for k in range(16):
        cum_v[k] = jnp.broadcast_to(cum[k:k + 1], (8, SPAN))
        v_v[k] = jnp.broadcast_to(shift[k:k + 1], (8, SPAN))
    for o in range(8):
        lines = [total[8 * (n % 2) + o:8 * (n % 2) + o + 1] for n in range(8)]
        tot_out[o] = jnp.broadcast_to(jnp.concatenate(lines, 0), (8, 128))
    for copy in loads[2:]:
        copy.wait()

    @pl.when(span == 0)
    def _():
        k_win[:2 * BLK] = jnp.zeros((2 * BLK, 256), BF16)
        v_win[:2 * BLK] = jnp.zeros((2 * BLK, 256), BF16)

    def one(condition):
        return jnp.where(condition, 1, 0)

    greeted = (
        z + one(jnp.logical_and(z_moves, to_z < z)) + one(jnp.logical_and(z_moves, from_z < z))
        + 2 * one(jnp.logical_and(relaying, core == 1)) + one(sz < z) + one(fz < z)
    )
    pl.semaphore_wait(barrier, NC + PLANE - 1 + 2 * (NH - 1) + greeted)

    def reply(semaphore, device):
        pl.semaphore_signal(semaphore, inc=1, device_id=device, device_id_type=MESH)

    each(0, z, lambda n: reply(later_sem, z_device(n)))

    @pl.when(jnp.logical_and(z_moves, from_z < z))
    def _():
        reply(ready_sem, z_from)

    @pl.when(jnp.logical_and(relaying, core == 1))
    def _():
        reply(ready_sem, relay_from)

    @pl.when(fz < z)
    def _():
        reply(home_ready, home)

    def remote(src, dst, send, recv, to):
        return pltpu.make_async_remote_copy(
            src_ref=src, dst_ref=dst, send_sem=send, recv_sem=recv,
            device_id=to, device_id_type=MESH,
        )

    def cols(g, width=HDIM):
        return pl.ds(g * width, width)

    def halo(i, g, slot):
        stage, window = ((k_stage, k_win), (v_stage, v_win))[i]
        to = (az, ax, ay, jnp.where(wraps == 1, 1 - slot, slot), hg)
        return remote(
            stage.at[slot, :, cols(g)], window.at[prev_row, cols(g)],
            halo_send.at[i, g, slot], halo_recv.at[i, g, core], to,
        )

    def halo_arrival(i, g, block):
        part = (k_win, v_win)[i].at[pl.ds(block * BLK, BLK), cols(g)]
        return remote(part, part, halo_send.at[i, g, 0], halo_recv.at[i, g, block], partner)

    def swap(i, g):
        stage, window = ((k_stage, k_win), (v_stage, v_win))[i]
        return remote(
            stage.at[other, :, cols(g)], window.at[mine, cols(g)],
            swap_send.at[i, g], swap_recv.at[i, g], partner,
        )

    def swap_arrival(i, g):
        part = (k_win, v_win)[i].at[theirs, cols(g)]
        return remote(part, part, swap_send.at[i, g], swap_recv.at[i, g], partner)

    def q_swap(g):
        return remote(
            q_hbm.at[other, :, cols(g, 512)], q_span.at[core, :, cols(g, 512)],
            q_send.at[g], q_recv.at[g], partner,
        )

    def q_arrival(g):
        part = q_span.at[other, :, cols(g, 512)]
        return remote(part, part, q_send.at[g], q_recv.at[g], partner)

    last_chip = chip == CHIPS - 1
    for g in range(2):
        for i in range(2):
            halo(i, g, 0).start()
            pl.when(jnp.logical_not(last_chip))(halo(i, g, 1).start)
        q_swap(g).start()
        for i in range(2):
            swap(i, g).start()

    def tot_copy(to):
        return remote(
            tot_out.at[to // 2], tot_in.at[me], tot_send.at[0], tot_recv.at[0], plane_device(to)
        )

    ring(lambda to: tot_copy(to).start())
    tot_in[me] = tot_out[me // 2]
    for p in range(8):
        line = jnp.broadcast_to(gain_v[p:p + 1, :], (BLK, BLK))
        gcol[p * BLK:(p + 1) * BLK, :] = jnp.transpose(line)

    scale = math.log2(math.e) / math.sqrt(HDIM)
    j = lax.broadcasted_iota(jnp.int32, (3 * BLK, 4 * BLK), 0)
    i = lax.broadcasted_iota(jnp.int32, (3 * BLK, 4 * BLK), 1) % BLK
    first = one(span == 0)

    def part(q):
        return pl.ds(q * WIDE, WIDE)

    def z_copy(q):
        return remote(
            att.at[part(q)], z_in.at[long_out, part(q)], z_send.at[q], z_recv.at[long_out, q], z_to
        )

    def z_keep(q):
        return pltpu.make_async_copy(att.at[part(q)], z_in.at[0, part(q)], z_recv.at[0, q])

    def relay_copy(q):
        return remote(
            z_in.at[1, part(q)], z_in.at[0, part(q)], relay_send.at[q], z_recv.at[0, q], relay_to
        )

    def z_arrival(at, q):
        return remote(
            z_in.at[at, part(q)], z_in.at[at, part(q)], relay_send.at[q], z_recv.at[at, q], relay_to
        )

    def p_copy(q):
        return remote(z_in.at[0, part(q)], att_in.at[part(q)], att_send.at[q], att_recv.at[q], p_to)

    def p_keep(q):
        return pltpu.make_async_copy(z_in.at[0, part(q)], att_in.at[part(q)], att_recv.at[q])

    def either(here, keep, leave):
        pl.when(here)(keep)
        pl.when(jnp.logical_not(here))(leave)

    def sqz_copy():
        return remote(sq_out, sq_mid.at[long_out], sqz_send.at[0], sqz_recv.at[long_out], z_to)

    def sqz_keep():
        return pltpu.make_async_copy(sq_out, sq_mid.at[0], sqz_recv.at[0])

    def sqr_copy():
        return remote(sq_mid.at[1], sq_mid.at[0], sqr_send.at[0], sqz_recv.at[0], relay_to)

    def sqz_arrival(at):
        return remote(sq_mid.at[at], sq_mid.at[at], sqr_send.at[0], sqz_recv.at[at], relay_to)

    def sq_copy(to, at):
        return remote(
            sq_mid.at[0], sq_in.at[at], sq_send.at[to], sq_recv.at[at],
            (z, p_to[1], p_to[2], p_to[3], to),
        )

    def sq_keep():
        return pltpu.make_async_copy(sq_mid.at[0], sq_in.at[hg], sq_recv.at[hg])

    home_pairs = ((b_v, b_here), (w_out, w_here), (tot_out, tot_here))

    def home_copy(n):
        return remote(
            home_pairs[n][0], home_pairs[n][1], home_send.at[n], home_recv.at[n], away
        )

    def home_keep(n):
        return pltpu.make_async_copy(home_pairs[n][0], home_pairs[n][1], home_recv.at[n])

    def here_copy(r):
        return remote(
            sq_out, sq_here.at[hg], here_send.at[r], here_recv.at[hg],
            (z, x, y, core, (hg + r) % NH),
        )

    def here_arrival(r):
        n = (hg + r) % NH
        return remote(sq_here.at[n], sq_here.at[n], here_send.at[r], here_recv.at[n], partner)

    sums = [jnp.zeros((1, BLK), F32) for _ in range(2)]
    for g in range(2):
        @pl.when(span > 0)
        def _():
            for t in range(2):
                for block in range(2):
                    halo_arrival(t, g, block).wait_recv()

        for t in range(2):
            swap_arrival(t, g).wait_recv()
        q_arrival(g).wait_recv()
        lanes = slice(g * HDIM, (g + 1) * HDIM)
        for a in range(2):
            keys = k_win[a * BLK:(a + 3) * BLK, lanes]
            vals = jnp.transpose(v_win[a * BLK:(a + 3) * BLK, lanes])
            heads = [q_span[a, :, (4 * g + h) * HDIM:(4 * g + h + 1) * HDIM] for h in range(4)]
            score = dot(keys, jnp.concatenate(heads, 0), ((1,), (1,)))
            low = jnp.maximum(i + 1, first * (2 - a) * BLK)
            allowed = (j >= low) & (j <= i + 2 * BLK)
            score = jnp.where(allowed, score, -jnp.inf)
            peak = jnp.max(score, axis=0, keepdims=True)
            terms = jnp.exp2((score - peak) * scale)
            sum_terms = jnp.sum(terms, axis=0, keepdims=True)
            got = dot(vals, terms.astype(BF16), ((1,), (0,)))
            got = (got * (1.0 / sum_terms)).astype(BF16)
            for h in range(4):
                head = got[:, h * BLK:(h + 1) * BLK]
                att[(4 * g + h) * HDIM:(4 * g + h + 1) * HDIM, a * BLK:(a + 1) * BLK] = head
                wide = head.astype(F32)
                sums[a] = sums[a] + jnp.sum(wide * wide, axis=0, keepdims=True)
        if g == 0:
            @pl.when(jnp.logical_and(z_moves, to_z > z))
            def _():
                pl.semaphore_wait(ready_sem, 1)
        else:
            sq_out[...] = jnp.broadcast_to(jnp.concatenate(sums, 1), (8, SPAN))
            for r in range(1, NH):
                here_copy(r).start()
            sq_here[hg] = sq_out[...]
            either(z_stays, lambda: sqz_keep().start(), lambda: sqz_copy().start())
        for q in (2 * g, 2 * g + 1):
            either(z_stays, z_keep(q).start, z_copy(q).start)
        if g == 0:
            @pl.when(sz > z)
            def _():
                pl.semaphore_wait(home_ready, 1)

            for n in range(3):
                either(stays, home_keep(n).start, home_copy(n).start)

    cross = dot(b_v[...], c_v[...], ((1,), (1,)))

    def make_mix(k, carry):
        ct = cum_v[k, 0:1, :]
        for ub in range(2):
            line = v_v[k, 0:1, ub * BLK:(ub + 1) * BLK]
            colb = jnp.transpose(jnp.broadcast_to(line, (BLK, BLK)))
            arg = ct + jnp.concatenate([colb, colb], 1)
            rows = slice(ub * BLK, (ub + 1) * BLK)
            arg = jnp.where(causal[rows], arg, -jnp.inf)
            mix[k, rows] = (jnp.exp(arg) * cross[rows]).astype(BF16)
        return carry

    lax.fori_loop(0, 16, make_mix, 0)

    def make_ecum(p, carry):
        lanes = pl.ds(pl.multiple_of(p * BLK, BLK), BLK)
        for tb in range(2):
            half = slice(tb * BLK, (tb + 1) * BLK)
            pair = [
                jnp.broadcast_to(jnp.exp(cum_v[2 * p + h, 0:1, half]), (SDIM, BLK))
                for h in range(2)
            ]
            ecum[half, lanes] = jnp.transpose(jnp.concatenate(pair, 0))
        return carry

    lax.fori_loop(0, 8, make_ecum, 0)

    @pl.when(jnp.logical_and(relaying, core == 0))
    def _():
        pl.semaphore_wait(ready_sem, 1)

    def arrive(q):
        @pl.when(relaying)
        def _():
            z_arrival(1, q).wait_recv()
            relay_copy(q).start()

        either(z_stays, z_keep(q).wait, z_arrival(0, q).wait_recv)
        either(p_stays, p_keep(q).start, p_copy(q).start)

    def arrive_squares():
        @pl.when(relaying)
        def _():
            sqz_arrival(1).wait_recv()
            sqr_copy().start()

        either(z_stays, lambda: sqz_keep().wait(), lambda: sqz_arrival(0).wait_recv())
        for r in range(1, NH):
            sq_copy((hg + r) % NH, hg).start()
        either(p_stays, lambda: sq_keep().start(), lambda: sq_copy(hg, hg).start())

    def st_copy(q, to):
        return remote(
            st_out.at[q, to], st_in.at[q, me], st_send.at[q], st_recv.at[q], plane_device(to)
        )

    def vtot_copy(to):
        return remote(
            tot_here.at[to // 2], run_tot.at[me], vtot_send.at[0], vtot_recv.at[0],
            plane_device(to),
        )

    def pre_copy(q, s):
        return remote(
            pre_out.at[q, s], pre_in.at[q, z % 2], pre_send.at[q, s], pre_recv.at[q, z % 2],
            z_device(NZ // 2 * s + z // 2),
        )

    def pre_arrival(q, n):
        return remote(
            pre_in.at[q, n], pre_in.at[q, n], pre_send.at[q, 0], pre_recv.at[q, n], partner
        )

    def run_copy(q, s, to):
        return remote(
            run_out.at[q, s], run_in.at[q, NZ * s + z], run_send.at[q, s, to],
            run_recv.at[q, NZ * s + z], z_device(to),
        )

    def run_arrival(q, n):
        return remote(
            run_in.at[q, n], run_in.at[q, n], run_send.at[q, 0, 0], run_recv.at[q, n], partner
        )

    def run_targets(s, act):
        @pl.when(jnp.logical_and(NZ // 2 * s + z // 2 != z, z % 2 == 0))
        def _():
            act(NZ // 2 * s + z // 2)

        def visit(n):
            pl.when(n != z)(lambda: act(n))

        each(NZ // 2 * s + z // 2 + 1, NZ, visit)

    def log_copy(to, at):
        return remote(plane_out, plane_in.at[at], log_send.at[to], log_recv.at[at], z_device(to))

    def en_copy(q, to):
        return remote(
            en_out.at[q, to], en_in.at[q, me], en_send.at[q], en_recv.at[q], plane_device(to)
        )

    def sent(buffer, semaphore):
        rest = buffer.at[pl.ds(0, PLANE - 1)]
        return remote(rest, rest, semaphore, semaphore, partner)

    def states(q):
        square = sq_here[0] + sq_here[1] + sq_here[2] + sq_here[3]
        rate = lax.rsqrt(square[0:1] / FEATS + 1e-06)
        for k in range(8 * q, 8 * q + 8):
            rows = slice(k * SDIM, (k + 1) * SDIM)
            gain = gcol[rows, :]
            value = att[rows, :].astype(F32) * jnp.concatenate([gain, gain], 1) * rate
            value = value.astype(BF16).astype(F32)
            weighted[rows, :] = (value * w_here[k:k + 1, :]).astype(BF16)
        state = dot(weighted[q * HALF:(q + 1) * HALF], b_here[...], ((1,), (0,)))
        st_out[q] = state.astype(BF16).reshape(PLANE, SLICE, STATE)
        ring(lambda to: st_copy(q, to).start())
        st_in[q, me] = st_out[q, me]

    def locals_(q):
        if q == 0:
            for r in range(1, NH):
                sq_copy((hg + r) % NH, (hg + r) % NH).wait_recv()
            either(p_stays, lambda: sq_keep().wait(), lambda: sq_copy(hg, hg).wait_recv())
        for c in (2 * q, 2 * q + 1):
            either(p_stays, p_keep(c).wait, p_copy(c).wait_recv)
        square = sq_in[0] + sq_in[1] + sq_in[2] + sq_in[3]
        rate = lax.rsqrt(square[0:1] / FEATS + 1e-06)

        def make_local(p, carry):
            lanes = pl.ds(pl.multiple_of(p * BLK, BLK), BLK)
            pair = []
            for h in range(2):
                k = 2 * p + h
                rows = pl.ds(pl.multiple_of(k * SDIM, SDIM), SDIM)
                gain = gcol[rows, :]
                value = att_in[rows, :].astype(F32) * jnp.concatenate([gain, gain], 1) * rate
                value = value.astype(BF16)
                pair.append(dot(value, mix[k], ((1,), (0,))) + value.astype(F32) * skip_ref[k])
            both = jnp.concatenate(pair, 0)
            for tb in range(2):
                half = slice(tb * BLK, (tb + 1) * BLK)
                local[half, lanes] = jnp.transpose(both[:, half])
            return carry

        lax.fori_loop(4 * q, 4 * q + 4, make_local, 0)

    def prefix(q):
        sent(st_in.at[q], st_recv.at[q]).wait_recv()
        for s in range(2):
            running = jnp.zeros((SLICE, STATE), F32)
            for n in range(8):
                pre_out[q, s, n] = running.astype(BF16)
                decay = jnp.exp(run_tot[2 * n + s])
                running = decay[q:q + 1] * running + st_in[q, 2 * n + s].astype(F32)
            run_out[q, s] = running.astype(BF16)
        for s in range(2):
            run_targets(s, lambda to: run_copy(q, s, to).start())
            run_in[q, NZ * s + z] = run_out[q, s]
        for s in range(2):
            own = NZ // 2 * s + z // 2 == z
            pl.when(jnp.logical_not(own))(pre_copy(q, s).start)

            @pl.when(own)
            def _():
                pre_in[q, s] = pre_out[q, s]

    def enter(q):
        for n in range(2):
            @pl.when(2 * (z % (NZ // 2)) + n != z)
            def _():
                pre_arrival(q, n).wait_recv()

        if q == 0:
            each(0, z, lambda n: log_copy(n, n).wait_recv())

        def arrived(n):
            pl.when(n % NZ != z)(run_arrival(q, n).wait_recv)

        def gather(p, carried):
            for n in range(2):
                arrived(2 * p + n)
                decay = jnp.exp(plane_in[p, n])
                carried = decay[q:q + 1] * carried + run_in[q, 2 * p + n].astype(F32)
            return carried

        carried = lax.fori_loop(0, z, gather, jnp.zeros((SLICE, STATE), F32))
        for n in range(8):
            value = pre_in[q, 0, n].astype(F32) + starts[n, q:q + 1] * carried
            en_out[q, n] = value.astype(BF16)
        arrived(2 * z)
        carried = jnp.exp(plane_out[0])[q:q + 1] * carried + run_in[q, 2 * z].astype(F32)
        for n in range(8):
            value = pre_in[q, 1, n].astype(F32) + starts[8 + n, q:q + 1] * carried
            en_out[q, 8 + n] = value.astype(BF16)
        ring(lambda to: en_copy(q, to).start())
        en_in[q, me] = en_out[q, me]

    def finish(q):
        sent(en_in.at[q], en_recv.at[q]).wait_recv()
        lanes = slice(q * HALF, (q + 1) * HALF)
        entry = dot(c_v[...], en_in[q].reshape(HALF, STATE), ((1,), (1,)))
        out_ref[:, lanes] = (local[:, lanes] + ecum[:, lanes] * entry).astype(BF16)

    for n in range(3):
        either(stays, home_keep(n).wait, home_copy(n).wait_recv)
    ring(lambda to: vtot_copy(to).start())
    run_tot[me] = tot_here[me // 2]
    for r in range(1, NH):
        here_arrival(r).wait_recv()
    for q in range(HALVES):
        states(q)

    sent(tot_in, tot_recv.at[0]).wait_recv()
    for r in range(2):
        logs = jnp.zeros((8, 128), F32)
        for n in range(8 * r, 8 * r + 8):
            starts[n] = jnp.exp(logs)
            logs = logs + tot_in[n]
        plane_out[r] = logs

    @pl.when(z < NZ - 1)
    def _():
        pl.semaphore_wait(later_sem, NZ - 1 - z)

    each(z + 1, NZ, lambda to: log_copy(to, z).start())
    arrive(0)
    sent(run_tot, vtot_recv.at[0]).wait_recv()
    prefix(0)
    prefix(1)
    arrive(1)
    arrive_squares()
    arrive(2)
    locals_(0)
    arrive(3)
    enter(0)
    enter(1)
    locals_(1)
    finish(0)
    finish(1)

    for g in range(2):
        for t in range(2):
            halo(t, g, 0).wait_send()
            pl.when(jnp.logical_not(last_chip))(halo(t, g, 1).wait_send)
            swap(t, g).wait_send()
        q_swap(g).wait_send()
    for r in range(1, NH):
        sq_copy((hg + r) % NH, hg).wait_send()

    @pl.when(z_moves)
    def _():
        sqz_copy().wait_send()
        for q in range(CHUNKS):
            z_copy(q).wait_send()

    @pl.when(relaying)
    def _():
        sqr_copy().wait_send()
        for q in range(CHUNKS):
            relay_copy(q).wait_send()

    @pl.when(p_moves)
    def _():
        sq_copy(hg, hg).wait_send()
        for q in range(CHUNKS):
            p_copy(q).wait_send()

    sent(tot_in, tot_send.at[0]).wait_send()
    sent(run_tot, vtot_send.at[0]).wait_send()
    each(z + 1, NZ, lambda to: log_copy(to, z).wait_send())
    for r in range(1, NH):
        here_copy(r).wait_send()

    @pl.when(jnp.logical_not(stays))
    def _():
        for n in range(3):
            home_copy(n).wait_send()

    for q in range(HALVES):
        sent(st_out.at[q], st_send.at[q]).wait_send()
        for s in range(2):
            run_targets(s, lambda to: run_copy(q, s, to).wait_send())
            pl.when(NZ // 2 * s + z // 2 != z)(pre_copy(q, s).wait_send)
        sent(en_out.at[q], en_send.at[q]).wait_send()


def body(query, keys, values, norm_gain, in_b, out_c, step, log_decay, skip):
    feats = query.shape[2]
    gain = norm_gain.reshape(feats // HDIM, HDIM)
    dma = pltpu.SemaphoreType.DMA
    vm = pltpu.VMEM
    scratch = [
        vm((2, BLK, feats), BF16),
        vm((2, BLK, 256), BF16),
        vm((2, BLK, 256), BF16),
        vm((4 * BLK, 256), BF16),
        vm((4 * BLK, 256), BF16),
        vm((8, HDIM), F32),
        vm((SPAN, STATE), BF16),
        vm((SPAN, STATE), BF16),
        vm((16, SPAN), F32),
        vm((16, SPAN), F32),
        vm((16, 8, SPAN), F32),
        vm((16, 8, SPAN), F32),
        vm((feats, 128), F32),
        vm((16, SPAN, SPAN), BF16),
        vm((SPAN, feats), F32),
        vm((feats, SPAN), BF16),
        vm((2, feats, SPAN), BF16),
        vm((feats, SPAN), BF16),
        vm((8, SPAN), F32),
        vm((2, 8, SPAN), F32),
        vm((NH, 8, SPAN), F32),
        vm((NH, 8, SPAN), F32),
        vm((feats, SPAN), BF16),
        vm((SPAN, feats), F32),
        vm((16, SPAN), F32),
        vm((16, SPAN), F32),
        vm((SPAN, STATE), BF16),
        vm((8, 8, 128), F32),
        vm((8, 8, 128), F32),
        vm((PLANE, 8, 128), F32),
        vm((PLANE, 8, 128), F32),
        vm((PLANE, 8, 128), F32),
        vm((2, 8, 128), F32),
        vm((NZ, 2, 8, 128), F32),
        vm((HALVES, PLANE, SLICE, STATE), BF16),
        vm((HALVES, PLANE, SLICE, STATE), BF16),
        vm((HALVES, 2, 8, SLICE, STATE), BF16),
        vm((HALVES, 2, 8, SLICE, STATE), BF16),
        vm((HALVES, 2, SLICE, STATE), BF16),
        vm((HALVES, 2 * NZ, SLICE, STATE), BF16),
        vm((HALVES, PLANE, SLICE, STATE), BF16),
        vm((HALVES, PLANE, SLICE, STATE), BF16),
        dma((10,)),
        dma((2, 2, 2)), dma((2, 2, 2)),
        dma((2, 2)), dma((2, 2)),
        dma((2,)), dma((2,)),
        dma((CHUNKS,)), dma((2, CHUNKS)),
        dma((CHUNKS,)),
        dma((CHUNKS,)), dma((CHUNKS,)),
        dma((1,)), dma((2,)), dma((1,)),
        dma((NH,)), dma((NH,)),
        dma((NH,)), dma((NH,)),
        dma((3,)), dma((3,)),
        dma((1,)), dma((1,)),
        dma((HALVES, 2)), dma((HALVES, 2)),
        dma((1,)), dma((1,)),
        dma((NZ,)), dma((NZ,)),
        dma((HALVES,)), dma((HALVES,)),
        dma((HALVES, 2, NZ)), dma((HALVES, 2 * NZ)),
        dma((HALVES,)), dma((HALVES,)),
        pltpu.SemaphoreType.REGULAR,
        pltpu.SemaphoreType.REGULAR,
        pltpu.SemaphoreType.REGULAR,
    ]
    anywhere = pl.BlockSpec(memory_space=pl.ANY)
    return pl.pallas_call(
        kernel,
        out_shape=jax.ShapeDtypeStruct((SPAN, feats), BF16),
        in_specs=[anywhere] * 8 + [pl.BlockSpec(memory_space=pltpu.SMEM)],
        out_specs=pl.BlockSpec(memory_space=pltpu.VMEM),
        scratch_shapes=scratch,
        compiler_params=pltpu.CompilerParams(collective_id=0, has_side_effects=True),
    )(query, keys, values, gain, in_b, out_c, step, log_decay, skip)


def solution(mesh):
    torus = Mesh(mesh.devices.reshape(NZ, NX, NY, NC, NH), AXES)
    return jax.shard_map(
        body,
        mesh=torus,
        in_specs=(
            P(None, SEQ, "head"),
            P(None, SEQ, "head"),
            P(None, SEQ, "head"),
            P("head"),
            P(SEQ, None),
            P(SEQ, None),
            P("head", SEQ),
            P("head", SEQ),
            P("head"),
        ),
        out_specs=P(SEQ, "head"),
        check_vma=False,
    )
```

```python
import math

import jax
import jax.numpy as jnp
from jax import lax
from jax.experimental import pallas as pl
from jax.experimental.pallas import tpu as pltpu
from jax.sharding import Mesh
from jax.sharding import PartitionSpec as P

HDIM = 128
SDIM = 64
STATE = 128
SPAN = 256
BLK = 128
FEATS = 4096
NZ, NX, NY, NC, NH = 8, 4, 2, 2, 4
CHIPS = NZ * NX * NY
PLANE = NX * NY * NC
CHUNKS = 4
WIDE = 256
HALVES = 2
HALF = 512
SLICE = 32
AXES = ("z", "x", "y", "core", "head")
SEQ = ("z", "x", "y", "core")
MESH = pl.DeviceIdType.MESH
F32 = jnp.float32
BF16 = jnp.bfloat16


def chip_coords(chip):
    return chip // (NX * NY), (chip // NY) % NX, chip % NY


def seq_coords(index):
    return index // PLANE, (index // (NY * NC)) % NX, (index // NC) % NY, index % NC


def dot(a, b, dims, **kw):
    return lax.dot_general(a, b, (dims, ((), ())), preferred_element_type=F32, **kw)


def kernel(
    q_hbm, k_hbm, v_hbm, gain_hbm, b_hbm, c_hbm, step_hbm, decay_hbm, skip_ref,
    out_ref,
    q_span, k_stage, v_stage, k_win, v_win, gain_v, b_v, c_v, step_v, decay_v,
    cum_v, v_v, gcol, mix, ecum, att, z_in, att_in, sq_out, sq_mid, sq_in, sq_here, weighted, local,
    w_out, w_here, b_here, tot_here, tot_out, tot_in, run_tot, starts, plane_out, plane_in,
    st_out, st_in, pre_out, pre_in, run_out, run_in, en_out, en_in,
    load_sem, halo_send, halo_recv, swap_send, swap_recv, q_send, q_recv, z_send, z_recv,
    relay_send, att_send, att_recv, sqz_send, sqz_recv, sqr_send, sq_send, sq_recv,
    here_send, here_recv, home_send, home_recv, vtot_send, vtot_recv, pre_send, pre_recv, pre_on,
    tot_send, tot_recv, log_send, log_recv, st_send, st_recv, run_send, run_recv,
    en_send, en_recv, ready_sem, later_sem, home_ready, head_sem,
):
    z, x, y, core, hg = (lax.axis_index(a) for a in AXES)
    chip = (z * NX + x) * NY + y
    me = (x * NY + y) * NC + core
    other = 1 - core
    partner = (z, x, y, other, hg)

    after = (chip + 1) % CHIPS
    az, ax, ay = chip_coords(after)
    wraps = (chip == CHIPS - 1).astype(jnp.int32)
    before = (chip + CHIPS - 1) % CHIPS
    bz, bx, by = chip_coords(before)

    span = core * CHIPS + chip
    long_out = z == jnp.where(core == 0, NZ - 1, 0)
    long_out = jnp.where(long_out, 1, 0)
    relays = jnp.where(z == jnp.where(core == 0, 1, NZ - 2), 1, 0)
    long_in = jnp.where(z == jnp.where(core == 0, NZ // 2, NZ // 2 - 1), 1, 0)
    relay_of = jnp.where(core == 0, 1, NZ - 2)
    to_z = jnp.where(long_out == 1, relay_of, NZ // 2 * core + z // 2)
    to_core = jnp.where(long_out == 1, core, z % 2)
    z_to = (to_z, x, y, to_core, hg)
    long_half = jnp.where(z == jnp.where(core == 0, 5, 2), 1, 0)
    helps = z == jnp.where(core == 0, 0, NZ - 1)
    half_to = (
        jnp.where(long_half == 1, jnp.where(core == 0, 0, NZ - 1), to_z), x, y,
        jnp.where(long_half == 1, core, to_core), hg,
    )
    half_out = jnp.maximum(long_out, long_half)
    from_z = jnp.where(long_in == 1, jnp.where(core == 0, NZ - 2, 1), 2 * (z % (NZ // 2)) + core)
    from_core = jnp.where(long_in == 1, other, z // (NZ // 2))
    z_from = (from_z, x, y, from_core, hg)
    relay_from = (jnp.where(core == 0, NZ - 1, 0), x, y, core, hg)
    relay_z = jnp.where(
        helps, jnp.where(core == 0, 2, 5), jnp.where(core == 0, NZ // 2 - 1, NZ // 2)
    )
    relay_to = (relay_z, x, y, other, hg)
    z_stays = jnp.logical_and(to_z == z, to_core == core)
    z_moves = jnp.logical_not(z_stays)
    relaying = relays == 1
    p_to = (z, 2 * core + x // 2, x % 2, y, hg)
    p_from = (z, 2 * (x % 2) + y, core, x // 2, hg)
    p_stays = jnp.logical_and(p_to[1] == x, jnp.logical_and(p_to[2] == y, p_to[3] == core))
    p_moves = jnp.logical_not(p_stays)

    seq = z * PLANE + me
    fz, fx, fy, fc = seq_coords(span)
    home = (fz, fx, fy, fc, hg)
    sz, sx, sy = chip_coords(seq % CHIPS)
    away = (sz, sx, sy, seq // CHIPS, hg)
    stays = span == seq

    mine = pl.ds(pl.multiple_of((2 + core) * BLK, BLK), BLK)
    theirs = pl.ds(pl.multiple_of((2 + other) * BLK, BLK), BLK)
    prev_row = pl.ds(pl.multiple_of(core * BLK, BLK), BLK)
    loads = [
        (decay_hbm, decay_v), (step_hbm, step_v), (k_hbm, k_stage), (v_hbm, v_stage),
        (k_hbm.at[core], k_win.at[mine]), (v_hbm.at[core], v_win.at[mine]),
        (q_hbm.at[core], q_span.at[core]),
        (b_hbm, b_v), (c_hbm, c_v), (gain_hbm, gain_v),
    ]
    loads = [pltpu.make_async_copy(s, d, load_sem.at[i]) for i, (s, d) in enumerate(loads)]
    for copy in loads:
        copy.start()

    barrier = pltpu.get_barrier_semaphore()

    def greet(device):
        pl.semaphore_signal(barrier, inc=1, device_id=device, device_id_type=MESH)

    def plane_device(index):
        return (z, index // (NY * NC), (index // NC) % NY, index % NC, hg)

    def z_device(index):
        return (index, x, y, core, hg)

    def ring(act):
        def visit(r, carry):
            act((me + r) % PLANE)
            return carry

        lax.fori_loop(1, PLANE, visit, 0)

    def each(low, high, act):
        def visit(n, carry):
            act(n)
            return carry

        lax.fori_loop(low, high, visit, 0)

    greet((bz, bx, by, 0, hg))
    greet((bz, bx, by, 1, hg))
    ring(lambda n: greet(plane_device(n)))

    def rank(h):
        return jnp.where(h == 0, 0, jnp.where(h == 2, 2, 1))

    level = rank(hg)
    same = (z, x, y, core)

    def to_heads(position, test, act):
        for r in range(1, NH):
            h = (hg + r) % NH

            @pl.when(test(rank(h)))
            def _():
                act((*position, h))

    to_heads(p_from[:4], lambda n: n >= level, greet)
    to_heads(p_to[:4], lambda n: n > level, greet)
    to_heads(same, lambda n: n >= level, greet)

    @pl.when(jnp.logical_and(z_moves, from_z > z))
    def _():
        greet(z_from)

    @pl.when(jnp.logical_and(z_moves, to_z > z))
    def _():
        greet(z_to)

    @pl.when(jnp.logical_and(relaying, core == 0))
    def _():
        greet(relay_from)

    @pl.when(jnp.logical_and(jnp.logical_or(relaying, helps), core == 0))
    def _():
        greet(relay_to)

    @pl.when(jnp.logical_and(z == 5, core == 0))
    def _():
        greet((NZ - 1, x, y, 1, hg))

    each(z + 1, NZ, lambda n: greet(z_device(n)))
    @pl.when(fz > z)
    def _():
        greet(home)

    @pl.when(sz > z)
    def _():
        greet(away)

    loads[0].wait()
    loads[1].wait()
    row = lax.broadcasted_iota(jnp.int32, (SPAN, SPAN), 0)
    col = lax.broadcasted_iota(jnp.int32, (SPAN, SPAN), 1)
    causal = row <= col
    cum = dot(decay_v[...], causal.astype(F32), ((1,), (0,)), precision=lax.Precision.HIGHEST)
    total = cum[:, SPAN - 1:]
    w_out[...] = jnp.exp(total - cum) * step_v[...]
    shift = jnp.log(step_v[...]) - cum
    for k in range(16):
        cum_v[k] = jnp.broadcast_to(cum[k:k + 1], (8, SPAN))
        v_v[k] = jnp.broadcast_to(shift[k:k + 1], (8, SPAN))
    for o in range(8):
        lines = [total[8 * (n % 2) + o:8 * (n % 2) + o + 1] for n in range(8)]
        tot_out[o] = jnp.broadcast_to(jnp.concatenate(lines, 0), (8, 128))
    for copy in loads[2:]:
        copy.wait()

    @pl.when(span == 0)
    def _():
        k_win[:2 * BLK] = jnp.zeros((2 * BLK, 256), BF16)
        v_win[:2 * BLK] = jnp.zeros((2 * BLK, 256), BF16)

    def one(condition):
        return jnp.where(condition, 1, 0)

    greeted = (
        z + one(jnp.logical_and(z_moves, to_z < z)) + one(jnp.logical_and(z_moves, from_z < z))
        + 2 * one(jnp.logical_and(relaying, core == 1)) + one(sz < z) + one(fz < z)
        + one(jnp.logical_and(jnp.logical_or(z == 2, z == NZ - 1), core == 1))
    )
    heads = jnp.where(level == 0, 0, jnp.where(level == 1, 5, 9))
    pl.semaphore_wait(barrier, NC + PLANE - 1 + heads + greeted)

    def reply(semaphore, device):
        pl.semaphore_signal(semaphore, inc=1, device_id=device, device_id_type=MESH)

    each(0, z, lambda n: reply(later_sem, z_device(n)))
    to_heads(p_from[:4], lambda n: n < level, lambda d: reply(head_sem, d))
    to_heads(same, lambda n: n < level, lambda d: reply(head_sem, d))

    @pl.when(jnp.logical_and(z_moves, from_z < z))
    def _():
        reply(ready_sem, z_from)

    @pl.when(jnp.logical_and(relaying, core == 1))
    def _():
        reply(ready_sem, relay_from)

    @pl.when(jnp.logical_and(z == 2, core == 1))
    def _():
        reply(ready_sem, (0, x, y, 0, hg))

    @pl.when(fz < z)
    def _():
        reply(home_ready, home)

    def remote(src, dst, send, recv, to):
        return pltpu.make_async_remote_copy(
            src_ref=src, dst_ref=dst, send_sem=send, recv_sem=recv,
            device_id=to, device_id_type=MESH,
        )

    def either(here, keep, leave):
        pl.when(here)(keep)
        pl.when(jnp.logical_not(here))(leave)

    def cols(g, width=HDIM):
        return pl.ds(g * width, width)

    def halo(i, g, slot):
        stage, window = ((k_stage, k_win), (v_stage, v_win))[i]
        to = (az, ax, ay, jnp.where(wraps == 1, 1 - slot, slot), hg)
        return remote(
            stage.at[slot, :, cols(g)], window.at[prev_row, cols(g)],
            halo_send.at[i, g, slot], halo_recv.at[i, g, core], to,
        )

    def halo_arrival(i, g, block):
        part = (k_win, v_win)[i].at[pl.ds(block * BLK, BLK), cols(g)]
        return remote(part, part, halo_send.at[i, g, 0], halo_recv.at[i, g, block], partner)

    def swap(i, g):
        stage, window = ((k_stage, k_win), (v_stage, v_win))[i]
        return remote(
            stage.at[other, :, cols(g)], window.at[mine, cols(g)],
            swap_send.at[i, g], swap_recv.at[i, g], partner,
        )

    def swap_arrival(i, g):
        part = (k_win, v_win)[i].at[theirs, cols(g)]
        return remote(part, part, swap_send.at[i, g], swap_recv.at[i, g], partner)

    def q_swap(g):
        return remote(
            q_hbm.at[other, :, cols(g, 512)], q_span.at[core, :, cols(g, 512)],
            q_send.at[g], q_recv.at[g], partner,
        )

    def q_arrival(g):
        part = q_span.at[other, :, cols(g, 512)]
        return remote(part, part, q_send.at[g], q_recv.at[g], partner)

    last_chip = chip == CHIPS - 1
    home_pairs = ((b_v, b_here), (w_out, w_here), (tot_out, tot_here))

    def home_copy(n):
        return remote(
            home_pairs[n][0], home_pairs[n][1], home_send.at[n], home_recv.at[n], away
        )

    def home_keep(n):
        return pltpu.make_async_copy(home_pairs[n][0], home_pairs[n][1], home_recv.at[n])

    def send_home():
        for n in range(3):
            either(stays, home_keep(n).start, home_copy(n).start)

    def send_halo(g):
        for i in range(2):
            halo(i, g, 0).start()
            pl.when(jnp.logical_not(last_chip))(halo(i, g, 1).start)
        q_swap(g).start()
        for i in range(2):
            swap(i, g).start()

    send_halo(0)
    pl.when(sz <= z)(send_home)
    send_halo(1)

    def tot_copy(to):
        return remote(
            tot_out.at[to // 2], tot_in.at[me], tot_send.at[0], tot_recv.at[0], plane_device(to)
        )

    ring(lambda to: tot_copy(to).start())
    tot_in[me] = tot_out[me // 2]
    for p in range(8):
        line = jnp.broadcast_to(gain_v[p:p + 1, :], (BLK, BLK))
        gcol[p * BLK:(p + 1) * BLK, :] = jnp.transpose(line)

    scale = math.log2(math.e) / math.sqrt(HDIM)
    j = lax.broadcasted_iota(jnp.int32, (3 * BLK, 4 * BLK), 0)
    i = lax.broadcasted_iota(jnp.int32, (3 * BLK, 4 * BLK), 1) % BLK
    first = one(span == 0)

    def part(q):
        return pl.ds(q * WIDE, WIDE)

    def z_copy(q):
        slot, to = (long_out, z_to) if q < 2 else (half_out, half_to)
        return remote(att.at[part(q)], z_in.at[slot, part(q)], z_send.at[q], z_recv.at[slot, q], to)

    def z_keep(q):
        return pltpu.make_async_copy(att.at[part(q)], z_in.at[0, part(q)], z_recv.at[0, q])

    def relay_copy(q):
        return remote(
            z_in.at[1, part(q)], z_in.at[0, part(q)], relay_send.at[q], z_recv.at[0, q], relay_to
        )

    def z_arrival(at, q):
        return remote(
            z_in.at[at, part(q)], z_in.at[at, part(q)], relay_send.at[q], z_recv.at[at, q], relay_to
        )

    def p_copy(q):
        return remote(z_in.at[0, part(q)], att_in.at[part(q)], att_send.at[q], att_recv.at[q], p_to)

    def p_keep(q):
        return pltpu.make_async_copy(z_in.at[0, part(q)], att_in.at[part(q)], att_recv.at[q])

    def sqz_copy():
        return remote(sq_out, sq_mid.at[long_out], sqz_send.at[0], sqz_recv.at[long_out], z_to)

    def sqz_keep():
        return pltpu.make_async_copy(sq_out, sq_mid.at[0], sqz_recv.at[0])

    def sqr_copy():
        return remote(sq_mid.at[1], sq_mid.at[0], sqr_send.at[0], sqz_recv.at[0], relay_to)

    def sqz_arrival(at):
        return remote(sq_mid.at[at], sq_mid.at[at], sqr_send.at[0], sqz_recv.at[at], relay_to)

    def sq_copy(to, at):
        return remote(
            sq_mid.at[0], sq_in.at[at], sq_send.at[to], sq_recv.at[at],
            (z, p_to[1], p_to[2], p_to[3], to),
        )

    def sq_keep():
        return pltpu.make_async_copy(sq_mid.at[0], sq_in.at[hg], sq_recv.at[hg])

    def here_copy(r):
        return remote(
            sq_out, sq_here.at[hg], here_send.at[r], here_recv.at[hg],
            (z, x, y, core, (hg + r) % NH),
        )

    def here_arrival(r):
        n = (hg + r) % NH
        return remote(sq_here.at[n], sq_here.at[n], here_send.at[r], here_recv.at[n], partner)

    @pl.when(sz > z)
    def _():
        pl.semaphore_wait(home_ready, 1)
        send_home()

    sums = [jnp.zeros((1, BLK), F32) for _ in range(2)]
    for g in range(2):
        @pl.when(span > 0)
        def _():
            for t in range(2):
                for block in range(2):
                    halo_arrival(t, g, block).wait_recv()

        for t in range(2):
            swap_arrival(t, g).wait_recv()
        q_arrival(g).wait_recv()
        lanes = slice(g * HDIM, (g + 1) * HDIM)
        for a in range(2):
            keys = k_win[a * BLK:(a + 3) * BLK, lanes]
            vals = jnp.transpose(v_win[a * BLK:(a + 3) * BLK, lanes])
            heads = [q_span[a, :, (4 * g + h) * HDIM:(4 * g + h + 1) * HDIM] for h in range(4)]
            score = dot(keys, jnp.concatenate(heads, 0), ((1,), (1,)))
            low = jnp.maximum(i + 1, first * (2 - a) * BLK)
            allowed = (j >= low) & (j <= i + 2 * BLK)
            score = jnp.where(allowed, score, -jnp.inf)
            peak = jnp.max(score, axis=0, keepdims=True)
            terms = jnp.exp2((score - peak) * scale)
            sum_terms = jnp.sum(terms, axis=0, keepdims=True)
            got = dot(vals, terms.astype(BF16), ((1,), (0,)))
            got = (got * (1.0 / sum_terms)).astype(BF16)
            for h in range(4):
                head = got[:, h * BLK:(h + 1) * BLK]
                att[(4 * g + h) * HDIM:(4 * g + h + 1) * HDIM, a * BLK:(a + 1) * BLK] = head
                wide = head.astype(F32)
                sums[a] = sums[a] + jnp.sum(wide * wide, axis=0, keepdims=True)
        if g == 0:
            @pl.when(jnp.logical_and(z_moves, to_z > z))
            def _():
                pl.semaphore_wait(ready_sem, 1)
        else:
            sq_out[...] = jnp.broadcast_to(jnp.concatenate(sums, 1), (8, SPAN))

            @pl.when(level < 2)
            def _():
                pl.semaphore_wait(head_sem, jnp.where(level == 0, 6, 2))

            for r in range(1, NH):
                here_copy(r).start()
            sq_here[hg] = sq_out[...]
            either(z_stays, lambda: sqz_keep().start(), lambda: sqz_copy().start())

            @pl.when(z < NZ - 1)
            def _():
                pl.semaphore_wait(later_sem, NZ - 1 - z)

        for q in (2 * g, 2 * g + 1):
            either(z_stays, z_keep(q).start, z_copy(q).start)
    cross = dot(b_v[...], c_v[...], ((1,), (1,)))

    def make_mix(k, carry):
        ct = cum_v[k, 0:1, :]
        for ub in range(2):
            line = v_v[k, 0:1, ub * BLK:(ub + 1) * BLK]
            colb = jnp.transpose(jnp.broadcast_to(line, (BLK, BLK)))
            arg = ct + jnp.concatenate([colb, colb], 1)
            rows = slice(ub * BLK, (ub + 1) * BLK)
            arg = jnp.where(causal[rows], arg, -jnp.inf)
            mix[k, rows] = (jnp.exp(arg) * cross[rows]).astype(BF16)
        return carry

    lax.fori_loop(0, 16, make_mix, 0)

    def make_ecum(p, carry):
        lanes = pl.ds(pl.multiple_of(p * BLK, BLK), BLK)
        for tb in range(2):
            half = slice(tb * BLK, (tb + 1) * BLK)
            pair = [
                jnp.broadcast_to(jnp.exp(cum_v[2 * p + h, 0:1, half]), (SDIM, BLK))
                for h in range(2)
            ]
            ecum[half, lanes] = jnp.transpose(jnp.concatenate(pair, 0))
        return carry

    lax.fori_loop(0, 8, make_ecum, 0)

    @pl.when(jnp.logical_and(jnp.logical_or(relaying, helps), core == 0))
    def _():
        pl.semaphore_wait(ready_sem, 1)

    def relay(q):
        @pl.when(relaying if q < 2 else jnp.logical_or(relaying, helps))
        def _():
            z_arrival(1, q).wait_recv()
            relay_copy(q).start()

    def relay_squares():
        @pl.when(relaying)
        def _():
            sqz_arrival(1).wait_recv()
            sqr_copy().start()

    def arrive(q):
        either(z_stays, z_keep(q).wait, z_arrival(0, q).wait_recv)
        either(p_stays, p_keep(q).start, p_copy(q).start)

    def arrive_squares():
        either(z_stays, lambda: sqz_keep().wait(), lambda: sqz_arrival(0).wait_recv())
        for r in range(1, NH):
            sq_copy((hg + r) % NH, hg).start()
        either(p_stays, lambda: sq_keep().start(), lambda: sq_copy(hg, hg).start())

    def st_copy(q, to):
        return remote(
            st_out.at[q, to], st_in.at[q, me], st_send.at[q], st_recv.at[q], plane_device(to)
        )

    def vtot_copy(to):
        return remote(
            tot_here.at[to // 2], run_tot.at[me], vtot_send.at[0], vtot_recv.at[0],
            plane_device(to),
        )

    tail = pl.ds(1, 7)

    def pre_copy(q, s):
        far = z == (0 if s else NZ - 1)
        to = jnp.where(far, NZ - 2 if s else 1, NZ // 2 * s + z // 2)
        slot = jnp.where(far, 2, z % 2)
        return remote(
            pre_out.at[q, s, tail], pre_in.at[q, slot, tail], pre_send.at[q, s],
            pre_recv.at[q, slot], z_device(to),
        )

    def pre_arrival(q, n):
        part = pre_in.at[q, n, tail]
        return remote(part, part, pre_send.at[q, 0], pre_recv.at[q, n], partner)

    pre_relays = jnp.logical_or(z == 1, z == NZ - 2)

    def pre_pass(q):
        slot = jnp.where(z == 1, 1, 0)
        return remote(
            pre_in.at[q, 2, tail], pre_in.at[q, slot, tail], pre_on.at[q], pre_recv.at[q, slot],
            z_device(jnp.where(z == 1, NZ // 2 - 1, NZ // 2)),
        )

    def pre_relay(q):
        @pl.when(pre_relays)
        def _():
            pre_arrival(q, 2).wait_recv()
            pre_pass(q).start()

    def run_copy(q, s, to):
        return remote(
            run_out.at[q, s], run_in.at[q, NZ * s + z], run_send.at[q, s, to],
            run_recv.at[q, NZ * s + z], z_device(to),
        )

    def run_arrival(q, n):
        return remote(
            run_in.at[q, n], run_in.at[q, n], run_send.at[q, 0, 0], run_recv.at[q, n], partner
        )

    def run_targets(s, act):
        @pl.when(jnp.logical_and(NZ // 2 * s + z // 2 != z, z % 2 == 0))
        def _():
            act(NZ // 2 * s + z // 2)

        def visit(n):
            pl.when(n != z)(lambda: act(n))

        each(NZ // 2 * s + z // 2 + 1, NZ, visit)

    def log_copy(to, at):
        return remote(plane_out, plane_in.at[at], log_send.at[to], log_recv.at[at], z_device(to))

    def en_copy(q, to):
        return remote(
            en_out.at[q, to], en_in.at[q, me], en_send.at[q], en_recv.at[q], plane_device(to)
        )

    def sent(buffer, semaphore):
        rest = buffer.at[pl.ds(0, PLANE - 1)]
        return remote(rest, rest, semaphore, semaphore, partner)

    def states(q):
        square = sq_here[0] + sq_here[1] + sq_here[2] + sq_here[3]
        rate = lax.rsqrt(square[0:1] / FEATS + 1e-06)
        for k in range(8 * q, 8 * q + 8):
            rows = slice(k * SDIM, (k + 1) * SDIM)
            gain = gcol[rows, :]
            value = att[rows, :].astype(F32) * jnp.concatenate([gain, gain], 1) * rate
            value = value.astype(BF16).astype(F32)
            weighted[rows, :] = (value * w_here[k:k + 1, :]).astype(BF16)
        state = dot(weighted[q * HALF:(q + 1) * HALF], b_here[...], ((1,), (0,)))
        st_out[q] = state.astype(BF16).reshape(PLANE, SLICE, STATE)
        ring(lambda to: st_copy(q, to).start())
        st_in[q, me] = st_out[q, me]

    def locals_(q):
        if q == 0:
            for r in range(1, NH):
                sq_copy((hg + r) % NH, (hg + r) % NH).wait_recv()
            either(p_stays, lambda: sq_keep().wait(), lambda: sq_copy(hg, hg).wait_recv())
        for c in (2 * q, 2 * q + 1):
            either(p_stays, p_keep(c).wait, p_copy(c).wait_recv)
        square = sq_in[0] + sq_in[1] + sq_in[2] + sq_in[3]
        rate = lax.rsqrt(square[0:1] / FEATS + 1e-06)

        def make_local(p, carry):
            lanes = pl.ds(pl.multiple_of(p * BLK, BLK), BLK)
            pair = []
            for h in range(2):
                k = 2 * p + h
                rows = pl.ds(pl.multiple_of(k * SDIM, SDIM), SDIM)
                gain = gcol[rows, :]
                value = att_in[rows, :].astype(F32) * jnp.concatenate([gain, gain], 1) * rate
                value = value.astype(BF16)
                pair.append(dot(value, mix[k], ((1,), (0,))) + value.astype(F32) * skip_ref[k])
            both = jnp.concatenate(pair, 0)
            for tb in range(2):
                half = slice(tb * BLK, (tb + 1) * BLK)
                local[half, lanes] = jnp.transpose(both[:, half])
            return carry

        lax.fori_loop(4 * q, 4 * q + 4, make_local, 0)

    def prefix(q):
        sent(st_in.at[q], st_recv.at[q]).wait_recv()
        for s in range(2):
            running = jnp.zeros((SLICE, STATE), F32)
            for n in range(8):
                pre_out[q, s, n] = running.astype(BF16)
                decay = jnp.exp(run_tot[2 * n + s])
                running = decay[q:q + 1] * running + st_in[q, 2 * n + s].astype(F32)
            run_out[q, s] = running.astype(BF16)
        for s in range(2):
            run_targets(s, lambda to: run_copy(q, s, to).start())
            run_in[q, NZ * s + z] = run_out[q, s]
        for s in range(2):
            own = NZ // 2 * s + z // 2 == z
            pl.when(jnp.logical_not(own))(pre_copy(q, s).start)

            @pl.when(own)
            def _():
                pre_in[q, s] = pre_out[q, s]

    def enter(q):
        for n in range(2):
            @pl.when(2 * (z % (NZ // 2)) + n != z)
            def _():
                pre_arrival(q, n).wait_recv()

        if q == 0:
            each(0, z, lambda n: log_copy(n, n).wait_recv())

        def arrived(n):
            pl.when(n % NZ != z)(run_arrival(q, n).wait_recv)

        def gather(p, carried):
            for n in range(2):
                arrived(2 * p + n)
                decay = jnp.exp(plane_in[p, n])
                carried = decay[q:q + 1] * carried + run_in[q, 2 * p + n].astype(F32)
            return carried

        carried = lax.fori_loop(0, z, gather, jnp.zeros((SLICE, STATE), F32))
        en_out[q, 0] = carried.astype(BF16)
        for n in range(1, 8):
            value = pre_in[q, 0, n].astype(F32) + starts[n, q:q + 1] * carried
            en_out[q, n] = value.astype(BF16)
        arrived(2 * z)
        carried = jnp.exp(plane_out[0])[q:q + 1] * carried + run_in[q, 2 * z].astype(F32)
        en_out[q, 8] = carried.astype(BF16)
        for n in range(1, 8):
            value = pre_in[q, 1, n].astype(F32) + starts[8 + n, q:q + 1] * carried
            en_out[q, 8 + n] = value.astype(BF16)
        ring(lambda to: en_copy(q, to).start())
        en_in[q, me] = en_out[q, me]

    def finish(q):
        sent(en_in.at[q], en_recv.at[q]).wait_recv()
        lanes = slice(q * HALF, (q + 1) * HALF)
        entry = dot(c_v[...], en_in[q].reshape(HALF, STATE), ((1,), (1,)))
        out_ref[:, lanes] = (local[:, lanes] + ecum[:, lanes] * entry).astype(BF16)

    relay(0)
    for n in range(3):
        either(stays, home_keep(n).wait, home_copy(n).wait_recv)
    ring(lambda to: vtot_copy(to).start())
    run_tot[me] = tot_here[me // 2]
    for r in range(1, NH):
        here_arrival(r).wait_recv()
    for q in range(HALVES):
        states(q)

    relay(1)
    relay_squares()
    sent(tot_in, tot_recv.at[0]).wait_recv()
    for r in range(2):
        logs = jnp.zeros((8, 128), F32)
        for n in range(8 * r, 8 * r + 8):
            starts[n] = jnp.exp(logs)
            logs = logs + tot_in[n]
        plane_out[r] = logs

    each(z + 1, NZ, lambda to: log_copy(to, z).start())
    arrive(0)
    relay(2)
    arrive(1)
    arrive_squares()
    sent(run_tot, vtot_recv.at[0]).wait_recv()
    prefix(0)
    prefix(1)
    relay(3)
    arrive(2)
    arrive(3)
    pre_relay(0)
    pre_relay(1)
    locals_(0)
    enter(0)
    enter(1)
    locals_(1)
    finish(0)
    finish(1)

    for g in range(2):
        for t in range(2):
            halo(t, g, 0).wait_send()
            pl.when(jnp.logical_not(last_chip))(halo(t, g, 1).wait_send)
            swap(t, g).wait_send()
        q_swap(g).wait_send()
    for r in range(1, NH):
        sq_copy((hg + r) % NH, hg).wait_send()

    @pl.when(z_moves)
    def _():
        sqz_copy().wait_send()
        for q in range(CHUNKS):
            z_copy(q).wait_send()

    @pl.when(relaying)
    def _():
        sqr_copy().wait_send()
        for q in range(2):
            relay_copy(q).wait_send()

    @pl.when(jnp.logical_or(relaying, helps))
    def _():
        for q in range(2, CHUNKS):
            relay_copy(q).wait_send()

    @pl.when(p_moves)
    def _():
        sq_copy(hg, hg).wait_send()
        for q in range(CHUNKS):
            p_copy(q).wait_send()

    sent(tot_in, tot_send.at[0]).wait_send()
    sent(run_tot, vtot_send.at[0]).wait_send()
    each(z + 1, NZ, lambda to: log_copy(to, z).wait_send())
    for r in range(1, NH):
        here_copy(r).wait_send()

    @pl.when(jnp.logical_not(stays))
    def _():
        for n in range(3):
            home_copy(n).wait_send()

    for q in range(HALVES):
        sent(st_out.at[q], st_send.at[q]).wait_send()
        for s in range(2):
            run_targets(s, lambda to: run_copy(q, s, to).wait_send())
            pl.when(NZ // 2 * s + z // 2 != z)(pre_copy(q, s).wait_send)
        pl.when(pre_relays)(pre_pass(q).wait_send)
        sent(en_out.at[q], en_send.at[q]).wait_send()


def body(query, keys, values, norm_gain, in_b, out_c, step, log_decay, skip):
    feats = query.shape[2]
    gain = norm_gain.reshape(feats // HDIM, HDIM)
    dma = pltpu.SemaphoreType.DMA
    vm = pltpu.VMEM
    scratch = [
        vm((2, BLK, feats), BF16),
        vm((2, BLK, 256), BF16),
        vm((2, BLK, 256), BF16),
        vm((4 * BLK, 256), BF16),
        vm((4 * BLK, 256), BF16),
        vm((8, HDIM), F32),
        vm((SPAN, STATE), BF16),
        vm((SPAN, STATE), BF16),
        vm((16, SPAN), F32),
        vm((16, SPAN), F32),
        vm((16, 8, SPAN), F32),
        vm((16, 8, SPAN), F32),
        vm((feats, 128), F32),
        vm((16, SPAN, SPAN), BF16),
        vm((SPAN, feats), F32),
        vm((feats, SPAN), BF16),
        vm((2, feats, SPAN), BF16),
        vm((feats, SPAN), BF16),
        vm((8, SPAN), F32),
        vm((2, 8, SPAN), F32),
        vm((NH, 8, SPAN), F32),
        vm((NH, 8, SPAN), F32),
        vm((feats, SPAN), BF16),
        vm((SPAN, feats), F32),
        vm((16, SPAN), F32),
        vm((16, SPAN), F32),
        vm((SPAN, STATE), BF16),
        vm((8, 8, 128), F32),
        vm((8, 8, 128), F32),
        vm((PLANE, 8, 128), F32),
        vm((PLANE, 8, 128), F32),
        vm((PLANE, 8, 128), F32),
        vm((2, 8, 128), F32),
        vm((NZ, 2, 8, 128), F32),
        vm((HALVES, PLANE, SLICE, STATE), BF16),
        vm((HALVES, PLANE, SLICE, STATE), BF16),
        vm((HALVES, 2, 8, SLICE, STATE), BF16),
        vm((HALVES, 3, 8, SLICE, STATE), BF16),
        vm((HALVES, 2, SLICE, STATE), BF16),
        vm((HALVES, 2 * NZ, SLICE, STATE), BF16),
        vm((HALVES, PLANE, SLICE, STATE), BF16),
        vm((HALVES, PLANE, SLICE, STATE), BF16),
        dma((10,)),
        dma((2, 2, 2)), dma((2, 2, 2)),
        dma((2, 2)), dma((2, 2)),
        dma((2,)), dma((2,)),
        dma((CHUNKS,)), dma((2, CHUNKS)),
        dma((CHUNKS,)),
        dma((CHUNKS,)), dma((CHUNKS,)),
        dma((1,)), dma((2,)), dma((1,)),
        dma((NH,)), dma((NH,)),
        dma((NH,)), dma((NH,)),
        dma((3,)), dma((3,)),
        dma((1,)), dma((1,)),
        dma((HALVES, 2)), dma((HALVES, 3)), dma((HALVES,)),
        dma((1,)), dma((1,)),
        dma((NZ,)), dma((NZ,)),
        dma((HALVES,)), dma((HALVES,)),
        dma((HALVES, 2, NZ)), dma((HALVES, 2 * NZ)),
        dma((HALVES,)), dma((HALVES,)),
        pltpu.SemaphoreType.REGULAR,
        pltpu.SemaphoreType.REGULAR,
        pltpu.SemaphoreType.REGULAR,
        pltpu.SemaphoreType.REGULAR,
    ]
    anywhere = pl.BlockSpec(memory_space=pl.ANY)
    return pl.pallas_call(
        kernel,
        out_shape=jax.ShapeDtypeStruct((SPAN, feats), BF16),
        in_specs=[anywhere] * 8 + [pl.BlockSpec(memory_space=pltpu.SMEM)],
        out_specs=pl.BlockSpec(memory_space=pltpu.VMEM),
        scratch_shapes=scratch,
        compiler_params=pltpu.CompilerParams(collective_id=0, has_side_effects=True),
    )(query, keys, values, gain, in_b, out_c, step, log_decay, skip)


def solution(mesh):
    torus = Mesh(mesh.devices.reshape(NZ, NX, NY, NC, NH), AXES)
    return jax.shard_map(
        body,
        mesh=torus,
        in_specs=(
            P(None, SEQ, "head"),
            P(None, SEQ, "head"),
            P(None, SEQ, "head"),
            P("head"),
            P(SEQ, None),
            P(SEQ, None),
            P("head", SEQ),
            P("head", SEQ),
            P("head"),
        ),
        out_specs=P(SEQ, "head"),
        check_vma=False,
    )
```

```python
import math

import jax
import jax.numpy as jnp
from jax import lax
from jax.experimental import pallas as pl
from jax.experimental.pallas import tpu as pltpu
from jax.sharding import Mesh
from jax.sharding import PartitionSpec as P

HDIM = 128
SDIM = 64
STATE = 128
SPAN = 256
BLK = 128
FEATS = 4096
NZ, NX, NY, NC, NH = 8, 4, 2, 2, 4
CHIPS = NZ * NX * NY
PLANE = NX * NY * NC
CHUNKS = 4
WIDE = 256
HALVES = 2
HALF = 512
SLICE = 32
AXES = ("z", "x", "y", "core", "head")
SEQ = ("z", "x", "y", "core")
MESH = pl.DeviceIdType.MESH
F32 = jnp.float32
BF16 = jnp.bfloat16


def chip_coords(chip):
    return chip // (NX * NY), (chip // NY) % NX, chip % NY


def seq_coords(index):
    return index // PLANE, (index // (NY * NC)) % NX, (index // NC) % NY, index % NC


def dot(a, b, dims, **kw):
    return lax.dot_general(a, b, (dims, ((), ())), preferred_element_type=F32, **kw)


def kernel(
    q_hbm, k_hbm, v_hbm, gain_hbm, b_hbm, c_hbm, step_hbm, decay_hbm, skip_hbm,
    out_ref,
    q_span, k_stage, v_stage, k_win, v_win, gain_v, b_v, c_v, step_v, decay_v,
    cum_v, v_v, gcol, mix, ecum, att, z_in, att_in, sq_out, sq_mid, sq_in, sq_here, weighted, local,
    w_low, w_here, b_here, tot_low, tot_row, tot_here, tot_out, tot_in, run_tot, starts, plane_out, plane_in,
    st_out, st_in, pre_out, pre_in, run_out, run_in, en_out, en_in,
    skip_ref, load_sem, halo_send, halo_recv, swap_send, swap_recv, q_send, q_recv, z_send, z_recv,
    relay_send, att_send, att_recv, sqz_send, sqz_recv, sqr_send, sq_send, sq_recv,
    here_send, here_recv, home_send, home_recv, vtot_send, vtot_recv, pre_send, pre_recv, pre_on,
    tot_send, tot_recv, log_send, log_recv, st_send, st_recv, run_send, run_recv,
    en_send, en_recv, ready_sem, later_sem, home_ready, head_sem,
):
    z, x, y, core, hg = (lax.axis_index(a) for a in AXES)
    chip = (z * NX + x) * NY + y
    me = (x * NY + y) * NC + core
    other = 1 - core
    partner = (z, x, y, other, hg)

    after = (chip + 1) % CHIPS
    az, ax, ay = chip_coords(after)
    wraps = (chip == CHIPS - 1).astype(jnp.int32)
    before = (chip + CHIPS - 1) % CHIPS
    bz, bx, by = chip_coords(before)

    span = core * CHIPS + chip
    long_out = z == jnp.where(core == 0, NZ - 1, 0)
    long_out = jnp.where(long_out, 1, 0)
    relays = jnp.where(z == jnp.where(core == 0, 1, NZ - 2), 1, 0)
    long_in = jnp.where(z == jnp.where(core == 0, NZ // 2, NZ // 2 - 1), 1, 0)
    relay_of = jnp.where(core == 0, 1, NZ - 2)
    to_z = jnp.where(long_out == 1, relay_of, NZ // 2 * core + z // 2)
    to_core = jnp.where(long_out == 1, core, z % 2)
    z_to = (to_z, x, y, to_core, hg)
    long_half = jnp.where(z == jnp.where(core == 0, 5, 2), 1, 0)
    helps = z == jnp.where(core == 0, 0, NZ - 1)
    half_to = (
        jnp.where(long_half == 1, jnp.where(core == 0, 0, NZ - 1), to_z), x, y,
        jnp.where(long_half == 1, core, to_core), hg,
    )
    half_out = jnp.maximum(long_out, long_half)
    from_z = jnp.where(long_in == 1, jnp.where(core == 0, NZ - 2, 1), 2 * (z % (NZ // 2)) + core)
    from_core = jnp.where(long_in == 1, other, z // (NZ // 2))
    z_from = (from_z, x, y, from_core, hg)
    relay_from = (jnp.where(core == 0, NZ - 1, 0), x, y, core, hg)
    relay_z = jnp.where(
        helps, jnp.where(core == 0, 2, 5), jnp.where(core == 0, NZ // 2 - 1, NZ // 2)
    )
    relay_to = (relay_z, x, y, other, hg)
    z_stays = jnp.logical_and(to_z == z, to_core == core)
    z_moves = jnp.logical_not(z_stays)
    relaying = relays == 1
    p_to = (z, 2 * core + x // 2, x % 2, y, hg)
    p_from = (z, 2 * (x % 2) + y, core, x // 2, hg)
    p_stays = jnp.logical_and(p_to[1] == x, jnp.logical_and(p_to[2] == y, p_to[3] == core))
    p_moves = jnp.logical_not(p_stays)

    seq = z * PLANE + me
    fz, fx, fy, fc = seq_coords(span)
    home = (fz, fx, fy, fc, hg)
    sz, sx, sy = chip_coords(seq % CHIPS)
    away = (sz, sx, sy, seq // CHIPS, hg)
    stays = span == seq

    mine = pl.ds(pl.multiple_of((2 + core) * BLK, BLK), BLK)
    theirs = pl.ds(pl.multiple_of((2 + other) * BLK, BLK), BLK)
    prev_row = pl.ds(pl.multiple_of(core * BLK, BLK), BLK)
    loads = [
        (decay_hbm, decay_v), (step_hbm, step_v), (k_hbm, k_stage), (v_hbm, v_stage),
        (k_hbm.at[core], k_win.at[mine]), (v_hbm.at[core], v_win.at[mine]),
        (q_hbm.at[core], q_span.at[core]),
        (b_hbm, b_v), (c_hbm, c_v), (gain_hbm, gain_v), (skip_hbm, skip_ref),
    ]
    loads = [pltpu.make_async_copy(s, d, load_sem.at[i]) for i, (s, d) in enumerate(loads)]
    for copy in loads:
        copy.start()

    barrier = pltpu.get_barrier_semaphore()

    def greet(device):
        pl.semaphore_signal(barrier, inc=1, device_id=device, device_id_type=MESH)

    def plane_device(index):
        return (z, index // (NY * NC), (index // NC) % NY, index % NC, hg)

    def z_device(index):
        return (index, x, y, core, hg)

    def ring(act):
        def visit(r, carry):
            act((me + r) % PLANE)
            return carry

        lax.fori_loop(1, PLANE, visit, 0)

    def each(low, high, act):
        def visit(n, carry):
            act(n)
            return carry

        lax.fori_loop(low, high, visit, 0)

    greet((bz, bx, by, 0, hg))
    greet((bz, bx, by, 1, hg))
    ring(lambda n: greet(plane_device(n)))

    def rank(h):
        return jnp.where(h == 0, 0, jnp.where(h == 2, 2, 1))

    level = rank(hg)
    same = (z, x, y, core)

    def to_heads(position, test, act):
        for r in range(1, NH):
            h = (hg + r) % NH

            @pl.when(test(rank(h)))
            def _():
                act((*position, h))

    to_heads(p_from[:4], lambda n: n >= level, greet)
    to_heads(p_to[:4], lambda n: n > level, greet)
    to_heads(same, lambda n: n >= level, greet)

    @pl.when(jnp.logical_and(z_moves, from_z > z))
    def _():
        greet(z_from)

    @pl.when(jnp.logical_and(z_moves, to_z > z))
    def _():
        greet(z_to)

    @pl.when(jnp.logical_and(relaying, core == 0))
    def _():
        greet(relay_from)

    @pl.when(jnp.logical_and(jnp.logical_or(relaying, helps), core == 0))
    def _():
        greet(relay_to)

    @pl.when(jnp.logical_and(z == 5, core == 0))
    def _():
        greet((NZ - 1, x, y, 1, hg))

    each(z + 1, NZ, lambda n: greet(z_device(n)))
    @pl.when(fz > z)
    def _():
        greet(home)

    @pl.when(sz > z)
    def _():
        greet(away)

    loads[0].wait()
    loads[1].wait()
    row = lax.broadcasted_iota(jnp.int32, (SPAN, SPAN), 0)
    col = lax.broadcasted_iota(jnp.int32, (SPAN, SPAN), 1)
    causal = row <= col
    cum = dot(decay_v[...], causal.astype(F32), ((1,), (0,)), precision=lax.Precision.HIGHEST)
    total = cum[:, SPAN - 1:]
    tail_weight = jnp.exp(total - cum) * step_v[...]
    w_low[...] = tail_weight.astype(BF16)
    tot_low[...] = jnp.broadcast_to(total, (16, 128))
    shift = jnp.log(step_v[...]) - cum
    for k in range(16):
        cum_v[k] = jnp.broadcast_to(cum[k:k + 1], (8, SPAN))
        v_v[k] = jnp.broadcast_to(shift[k:k + 1], (8, SPAN))
    for o in range(8):
        lines = [total[8 * (n % 2) + o:8 * (n % 2) + o + 1] for n in range(8)]
        tot_out[o] = jnp.broadcast_to(jnp.concatenate(lines, 0), (8, 128))
    for copy in loads[2:]:
        copy.wait()

    @pl.when(span == 0)
    def _():
        k_win[:2 * BLK] = jnp.zeros((2 * BLK, 256), BF16)
        v_win[:2 * BLK] = jnp.zeros((2 * BLK, 256), BF16)

    def one(condition):
        return jnp.where(condition, 1, 0)

    greeted = (
        z + one(jnp.logical_and(z_moves, to_z < z)) + one(jnp.logical_and(z_moves, from_z < z))
        + 2 * one(jnp.logical_and(relaying, core == 1)) + one(sz < z) + one(fz < z)
        + one(jnp.logical_and(jnp.logical_or(z == 2, z == NZ - 1), core == 1))
    )
    heads = jnp.where(level == 0, 0, jnp.where(level == 1, 5, 9))
    pl.semaphore_wait(barrier, NC + PLANE - 1 + heads + greeted)

    def reply(semaphore, device):
        pl.semaphore_signal(semaphore, inc=1, device_id=device, device_id_type=MESH)

    each(0, z, lambda n: reply(later_sem, z_device(n)))
    to_heads(p_from[:4], lambda n: n < level, lambda d: reply(head_sem, d))
    to_heads(same, lambda n: n < level, lambda d: reply(head_sem, d))

    @pl.when(jnp.logical_and(z_moves, from_z < z))
    def _():
        reply(ready_sem, z_from)

    @pl.when(jnp.logical_and(relaying, core == 1))
    def _():
        reply(ready_sem, relay_from)

    @pl.when(jnp.logical_and(z == 2, core == 1))
    def _():
        reply(ready_sem, (0, x, y, 0, hg))

    @pl.when(fz < z)
    def _():
        reply(home_ready, home)

    def remote(src, dst, send, recv, to):
        return pltpu.make_async_remote_copy(
            src_ref=src, dst_ref=dst, send_sem=send, recv_sem=recv,
            device_id=to, device_id_type=MESH,
        )

    def either(here, keep, leave):
        pl.when(here)(keep)
        pl.when(jnp.logical_not(here))(leave)

    def cols(g, width=HDIM):
        return pl.ds(g * width, width)

    def halo(i, g, slot):
        stage, window = ((k_stage, k_win), (v_stage, v_win))[i]
        to = (az, ax, ay, jnp.where(wraps == 1, 1 - slot, slot), hg)
        return remote(
            stage.at[slot, :, cols(g)], window.at[prev_row, cols(g)],
            halo_send.at[i, g, slot], halo_recv.at[i, g, core], to,
        )

    def halo_arrival(i, g, block):
        part = (k_win, v_win)[i].at[pl.ds(block * BLK, BLK), cols(g)]
        return remote(part, part, halo_send.at[i, g, 0], halo_recv.at[i, g, block], partner)

    def swap(i, g):
        stage, window = ((k_stage, k_win), (v_stage, v_win))[i]
        return remote(
            stage.at[other, :, cols(g)], window.at[mine, cols(g)],
            swap_send.at[i, g], swap_recv.at[i, g], partner,
        )

    def swap_arrival(i, g):
        part = (k_win, v_win)[i].at[theirs, cols(g)]
        return remote(part, part, swap_send.at[i, g], swap_recv.at[i, g], partner)

    def q_swap(g):
        return remote(
            q_hbm.at[other, :, cols(g, 512)], q_span.at[core, :, cols(g, 512)],
            q_send.at[g], q_recv.at[g], partner,
        )

    def q_arrival(g):
        part = q_span.at[other, :, cols(g, 512)]
        return remote(part, part, q_send.at[g], q_recv.at[g], partner)

    last_chip = chip == CHIPS - 1
    home_pairs = ((b_v, b_here), (w_low, w_here), (tot_low, tot_row))

    def home_copy(n):
        return remote(
            home_pairs[n][0], home_pairs[n][1], home_send.at[n], home_recv.at[n], away
        )

    def home_keep(n):
        return pltpu.make_async_copy(home_pairs[n][0], home_pairs[n][1], home_recv.at[n])

    def send_home():
        for n in range(3):
            either(stays, home_keep(n).start, home_copy(n).start)

    def send_halo(g):
        for i in range(2):
            halo(i, g, 0).start()
            pl.when(jnp.logical_not(last_chip))(halo(i, g, 1).start)
        q_swap(g).start()
        for i in range(2):
            swap(i, g).start()

    send_halo(0)
    pl.when(sz <= z)(send_home)
    send_halo(1)

    def tot_copy(to):
        return remote(
            tot_out.at[to // 2], tot_in.at[me], tot_send.at[0], tot_recv.at[0], plane_device(to)
        )

    ring(lambda to: tot_copy(to).start())
    tot_in[me] = tot_out[me // 2]
    for p in range(8):
        line = jnp.broadcast_to(gain_v[p:p + 1, :], (BLK, BLK))
        gcol[p * BLK:(p + 1) * BLK, :] = jnp.transpose(line)

    scale = math.log2(math.e) / math.sqrt(HDIM)
    j = lax.broadcasted_iota(jnp.int32, (3 * BLK, 4 * BLK), 0)
    i = lax.broadcasted_iota(jnp.int32, (3 * BLK, 4 * BLK), 1) % BLK
    first = one(span == 0)

    def part(q):
        return pl.ds(q * WIDE, WIDE)

    def z_copy(q):
        slot, to = (long_out, z_to) if q < 2 else (half_out, half_to)
        return remote(att.at[part(q)], z_in.at[slot, part(q)], z_send.at[q], z_recv.at[slot, q], to)

    def z_keep(q):
        return pltpu.make_async_copy(att.at[part(q)], z_in.at[0, part(q)], z_recv.at[0, q])

    def relay_copy(q):
        return remote(
            z_in.at[1, part(q)], z_in.at[0, part(q)], relay_send.at[q], z_recv.at[0, q], relay_to
        )

    def z_arrival(at, q):
        return remote(
            z_in.at[at, part(q)], z_in.at[at, part(q)], relay_send.at[q], z_recv.at[at, q], relay_to
        )

    def p_copy(q):
        return remote(z_in.at[0, part(q)], att_in.at[part(q)], att_send.at[q], att_recv.at[q], p_to)

    def p_keep(q):
        return pltpu.make_async_copy(z_in.at[0, part(q)], att_in.at[part(q)], att_recv.at[q])

    def sqz_copy():
        return remote(sq_out, sq_mid.at[long_out], sqz_send.at[0], sqz_recv.at[long_out], z_to)

    def sqz_keep():
        return pltpu.make_async_copy(sq_out, sq_mid.at[0], sqz_recv.at[0])

    def sqr_copy():
        return remote(sq_mid.at[1], sq_mid.at[0], sqr_send.at[0], sqz_recv.at[0], relay_to)

    def sqz_arrival(at):
        return remote(sq_mid.at[at], sq_mid.at[at], sqr_send.at[0], sqz_recv.at[at], relay_to)

    def sq_copy(to, at):
        return remote(
            sq_mid.at[0], sq_in.at[at], sq_send.at[to], sq_recv.at[at],
            (z, p_to[1], p_to[2], p_to[3], to),
        )

    def sq_keep():
        return pltpu.make_async_copy(sq_mid.at[0], sq_in.at[hg], sq_recv.at[hg])

    def here_copy(r):
        return remote(
            sq_out, sq_here.at[hg], here_send.at[r], here_recv.at[hg],
            (z, x, y, core, (hg + r) % NH),
        )

    def here_arrival(r):
        n = (hg + r) % NH
        return remote(sq_here.at[n], sq_here.at[n], here_send.at[r], here_recv.at[n], partner)

    @pl.when(sz > z)
    def _():
        pl.semaphore_wait(home_ready, 1)
        send_home()

    sums = [jnp.zeros((1, BLK), F32) for _ in range(2)]
    for g in range(2):
        @pl.when(span > 0)
        def _():
            for t in range(2):
                for block in range(2):
                    halo_arrival(t, g, block).wait_recv()

        for t in range(2):
            swap_arrival(t, g).wait_recv()
        q_arrival(g).wait_recv()
        lanes = slice(g * HDIM, (g + 1) * HDIM)
        for a in range(2):
            keys = k_win[a * BLK:(a + 3) * BLK, lanes]
            vals = jnp.transpose(v_win[a * BLK:(a + 3) * BLK, lanes])
            heads = [q_span[a, :, (4 * g + h) * HDIM:(4 * g + h + 1) * HDIM] for h in range(4)]
            score = dot(keys, jnp.concatenate(heads, 0), ((1,), (1,)))
            low = jnp.maximum(i + 1, first * (2 - a) * BLK)
            allowed = (j >= low) & (j <= i + 2 * BLK)
            score = jnp.where(allowed, score, -jnp.inf)
            peak = jnp.max(score, axis=0, keepdims=True)
            terms = jnp.exp2((score - peak) * scale)
            sum_terms = jnp.sum(terms, axis=0, keepdims=True)
            got = dot(vals, terms.astype(BF16), ((1,), (0,)))
            got = (got * (1.0 / sum_terms)).astype(BF16)
            for h in range(4):
                head = got[:, h * BLK:(h + 1) * BLK]
                att[(4 * g + h) * HDIM:(4 * g + h + 1) * HDIM, a * BLK:(a + 1) * BLK] = head
                wide = head.astype(F32)
                sums[a] = sums[a] + jnp.sum(wide * wide, axis=0, keepdims=True)
        if g == 0:
            @pl.when(jnp.logical_and(z_moves, to_z > z))
            def _():
                pl.semaphore_wait(ready_sem, 1)
        else:
            sq_out[...] = jnp.broadcast_to(jnp.concatenate(sums, 1), (8, SPAN))

            @pl.when(level < 2)
            def _():
                pl.semaphore_wait(head_sem, jnp.where(level == 0, 6, 2))

            for r in range(1, NH):
                here_copy(r).start()
            sq_here[hg] = sq_out[...]
            either(z_stays, lambda: sqz_keep().start(), lambda: sqz_copy().start())

            @pl.when(z < NZ - 1)
            def _():
                pl.semaphore_wait(later_sem, NZ - 1 - z)

        for q in (2 * g, 2 * g + 1):
            either(z_stays, z_keep(q).start, z_copy(q).start)
    cross = dot(b_v[...], c_v[...], ((1,), (1,)))

    def make_mix(k, carry):
        ct = cum_v[k, 0:1, :]
        for ub in range(2):
            line = v_v[k, 0:1, ub * BLK:(ub + 1) * BLK]
            colb = jnp.transpose(jnp.broadcast_to(line, (BLK, BLK)))
            arg = ct + jnp.concatenate([colb, colb], 1)
            rows = slice(ub * BLK, (ub + 1) * BLK)
            arg = jnp.where(causal[rows], arg, -jnp.inf)
            mix[k, rows] = (jnp.exp(arg) * cross[rows]).astype(BF16)
        return carry

    lax.fori_loop(0, 16, make_mix, 0)

    def make_ecum(p, carry):
        lanes = pl.ds(pl.multiple_of(p * BLK, BLK), BLK)
        for tb in range(2):
            half = slice(tb * BLK, (tb + 1) * BLK)
            pair = [
                jnp.broadcast_to(jnp.exp(cum_v[2 * p + h, 0:1, half]), (SDIM, BLK))
                for h in range(2)
            ]
            ecum[half, lanes] = jnp.transpose(jnp.concatenate(pair, 0))
        return carry

    lax.fori_loop(0, 8, make_ecum, 0)

    @pl.when(jnp.logical_and(jnp.logical_or(relaying, helps), core == 0))
    def _():
        pl.semaphore_wait(ready_sem, 1)

    def relay(q):
        @pl.when(relaying if q < 2 else jnp.logical_or(relaying, helps))
        def _():
            z_arrival(1, q).wait_recv()
            relay_copy(q).start()

    def relay_squares():
        @pl.when(relaying)
        def _():
            sqz_arrival(1).wait_recv()
            sqr_copy().start()

    def arrive(q):
        either(z_stays, z_keep(q).wait, z_arrival(0, q).wait_recv)
        either(p_stays, p_keep(q).start, p_copy(q).start)

    def arrive_squares():
        either(z_stays, lambda: sqz_keep().wait(), lambda: sqz_arrival(0).wait_recv())
        for r in range(1, NH):
            sq_copy((hg + r) % NH, hg).start()
        either(p_stays, lambda: sq_keep().start(), lambda: sq_copy(hg, hg).start())

    def st_copy(q, to):
        return remote(
            st_out.at[q, to], st_in.at[q, me], st_send.at[q], st_recv.at[q], plane_device(to)
        )

    def vtot_copy(to):
        return remote(
            tot_here.at[to // 2], run_tot.at[me], vtot_send.at[0], vtot_recv.at[0],
            plane_device(to),
        )

    after_first = pl.ds(1, 7)

    def pre_copy(q, s):
        far = z == (0 if s else NZ - 1)
        to = jnp.where(far, NZ - 2 if s else 1, NZ // 2 * s + z // 2)
        slot = jnp.where(far, 2, z % 2)
        return remote(
            pre_out.at[q, s, after_first], pre_in.at[q, slot, after_first], pre_send.at[q, s],
            pre_recv.at[q, slot], z_device(to),
        )

    def pre_arrival(q, n):
        part = pre_in.at[q, n, after_first]
        return remote(part, part, pre_send.at[q, 0], pre_recv.at[q, n], partner)

    pre_relays = jnp.logical_or(z == 1, z == NZ - 2)

    def pre_pass(q):
        slot = jnp.where(z == 1, 1, 0)
        return remote(
            pre_in.at[q, 2, after_first], pre_in.at[q, slot, after_first], pre_on.at[q], pre_recv.at[q, slot],
            z_device(jnp.where(z == 1, NZ // 2 - 1, NZ // 2)),
        )

    def pre_relay(q):
        @pl.when(pre_relays)
        def _():
            pre_arrival(q, 2).wait_recv()
            pre_pass(q).start()

    def run_copy(q, s, to):
        return remote(
            run_out.at[q, s], run_in.at[q, NZ * s + z], run_send.at[q, s, to],
            run_recv.at[q, NZ * s + z], z_device(to),
        )

    def run_arrival(q, n):
        return remote(
            run_in.at[q, n], run_in.at[q, n], run_send.at[q, 0, 0], run_recv.at[q, n], partner
        )

    def run_targets(s, act):
        @pl.when(jnp.logical_and(NZ // 2 * s + z // 2 != z, z % 2 == 0))
        def _():
            act(NZ // 2 * s + z // 2)

        def visit(n):
            pl.when(n != z)(lambda: act(n))

        each(NZ // 2 * s + z // 2 + 1, NZ, visit)

    def log_copy(to, at):
        return remote(plane_out, plane_in.at[at], log_send.at[to], log_recv.at[at], z_device(to))

    def en_copy(q, to):
        return remote(
            en_out.at[q, to], en_in.at[q, me], en_send.at[q], en_recv.at[q], plane_device(to)
        )

    def sent(buffer, semaphore):
        rest = buffer.at[pl.ds(0, PLANE - 1)]
        return remote(rest, rest, semaphore, semaphore, partner)

    def states(q):
        square = sq_here[0] + sq_here[1] + sq_here[2] + sq_here[3]
        rate = lax.rsqrt(square[0:1] / FEATS + 1e-06)
        for k in range(8 * q, 8 * q + 8):
            rows = slice(k * SDIM, (k + 1) * SDIM)
            gain = gcol[rows, :]
            value = att[rows, :].astype(F32) * jnp.concatenate([gain, gain], 1) * rate
            value = value.astype(BF16).astype(F32)
            weighted[rows, :] = (value * w_here[k:k + 1, :].astype(F32)).astype(BF16)
        state = dot(weighted[q * HALF:(q + 1) * HALF], b_here[...], ((1,), (0,)))
        st_out[q] = state.astype(BF16).reshape(PLANE, SLICE, STATE)
        ring(lambda to: st_copy(q, to).start())
        st_in[q, me] = st_out[q, me]

    def locals_(q):
        if q == 0:
            for r in range(1, NH):
                sq_copy((hg + r) % NH, (hg + r) % NH).wait_recv()
            either(p_stays, lambda: sq_keep().wait(), lambda: sq_copy(hg, hg).wait_recv())
        for c in (2 * q, 2 * q + 1):
            either(p_stays, p_keep(c).wait, p_copy(c).wait_recv)
        square = sq_in[0] + sq_in[1] + sq_in[2] + sq_in[3]
        rate = lax.rsqrt(square[0:1] / FEATS + 1e-06)

        def make_local(p, carry):
            lanes = pl.ds(pl.multiple_of(p * BLK, BLK), BLK)
            pair = []
            for h in range(2):
                k = 2 * p + h
                rows = pl.ds(pl.multiple_of(k * SDIM, SDIM), SDIM)
                gain = gcol[rows, :]
                value = att_in[rows, :].astype(F32) * jnp.concatenate([gain, gain], 1) * rate
                value = value.astype(BF16)
                pair.append(dot(value, mix[k], ((1,), (0,))) + value.astype(F32) * skip_ref[k])
            both = jnp.concatenate(pair, 0)
            for tb in range(2):
                half = slice(tb * BLK, (tb + 1) * BLK)
                local[half, lanes] = jnp.transpose(both[:, half])
            return carry

        lax.fori_loop(4 * q, 4 * q + 4, make_local, 0)

    def prefix(q):
        sent(st_in.at[q], st_recv.at[q]).wait_recv()
        for s in range(2):
            running = jnp.zeros((SLICE, STATE), F32)
            for n in range(8):
                pre_out[q, s, n] = running.astype(BF16)
                decay = jnp.exp(run_tot[2 * n + s])
                running = decay[q:q + 1] * running + st_in[q, 2 * n + s].astype(F32)
            run_out[q, s] = running.astype(BF16)
        for s in range(2):
            run_targets(s, lambda to: run_copy(q, s, to).start())
            run_in[q, NZ * s + z] = run_out[q, s]
        for s in range(2):
            own = NZ // 2 * s + z // 2 == z
            pl.when(jnp.logical_not(own))(pre_copy(q, s).start)

            @pl.when(own)
            def _():
                pre_in[q, s] = pre_out[q, s]

    def enter(q):
        for n in range(2):
            @pl.when(2 * (z % (NZ // 2)) + n != z)
            def _():
                pre_arrival(q, n).wait_recv()

        if q == 0:
            each(0, z, lambda n: log_copy(n, n).wait_recv())

        def arrived(n):
            pl.when(n % NZ != z)(run_arrival(q, n).wait_recv)

        def gather(p, carried):
            for n in range(2):
                arrived(2 * p + n)
                decay = jnp.exp(plane_in[p, n])
                carried = decay[q:q + 1] * carried + run_in[q, 2 * p + n].astype(F32)
            return carried

        carried = lax.fori_loop(0, z, gather, jnp.zeros((SLICE, STATE), F32))
        en_out[q, 0] = carried.astype(BF16)
        for n in range(1, 8):
            value = pre_in[q, 0, n].astype(F32) + starts[n, q:q + 1] * carried
            en_out[q, n] = value.astype(BF16)
        arrived(2 * z)
        carried = jnp.exp(plane_out[0])[q:q + 1] * carried + run_in[q, 2 * z].astype(F32)
        en_out[q, 8] = carried.astype(BF16)
        for n in range(1, 8):
            value = pre_in[q, 1, n].astype(F32) + starts[8 + n, q:q + 1] * carried
            en_out[q, 8 + n] = value.astype(BF16)
        ring(lambda to: en_copy(q, to).start())
        en_in[q, me] = en_out[q, me]

    def finish(q):
        sent(en_in.at[q], en_recv.at[q]).wait_recv()
        lanes = slice(q * HALF, (q + 1) * HALF)
        entry = dot(c_v[...], en_in[q].reshape(HALF, STATE), ((1,), (1,)))
        out_ref[:, lanes] = (local[:, lanes] + ecum[:, lanes] * entry).astype(BF16)

    relay(0)
    for n in range(3):
        either(stays, home_keep(n).wait, home_copy(n).wait_recv)
    for o in range(8):
        lines = [tot_row[8 * (n % 2) + o:8 * (n % 2) + o + 1] for n in range(8)]
        tot_here[o] = jnp.concatenate(lines, 0)
    ring(lambda to: vtot_copy(to).start())
    run_tot[me] = tot_here[me // 2]
    for r in range(1, NH):
        here_arrival(r).wait_recv()
    for q in range(HALVES):
        states(q)

    relay(1)
    relay_squares()
    sent(tot_in, tot_recv.at[0]).wait_recv()
    for r in range(2):
        logs = jnp.zeros((8, 128), F32)
        for n in range(8 * r, 8 * r + 8):
            starts[n] = jnp.exp(logs)
            logs = logs + tot_in[n]
        plane_out[r] = logs

    each(z + 1, NZ, lambda to: log_copy(to, z).start())
    arrive(0)
    relay(2)
    arrive(1)
    arrive_squares()
    sent(run_tot, vtot_recv.at[0]).wait_recv()
    prefix(0)
    prefix(1)
    relay(3)
    arrive(2)
    arrive(3)
    pre_relay(0)
    pre_relay(1)
    locals_(0)
    enter(0)
    enter(1)
    locals_(1)
    finish(0)
    finish(1)

    for g in range(2):
        for t in range(2):
            halo(t, g, 0).wait_send()
            pl.when(jnp.logical_not(last_chip))(halo(t, g, 1).wait_send)
            swap(t, g).wait_send()
        q_swap(g).wait_send()
    for r in range(1, NH):
        sq_copy((hg + r) % NH, hg).wait_send()

    @pl.when(z_moves)
    def _():
        sqz_copy().wait_send()
        for q in range(CHUNKS):
            z_copy(q).wait_send()

    @pl.when(relaying)
    def _():
        sqr_copy().wait_send()
        for q in range(2):
            relay_copy(q).wait_send()

    @pl.when(jnp.logical_or(relaying, helps))
    def _():
        for q in range(2, CHUNKS):
            relay_copy(q).wait_send()

    @pl.when(p_moves)
    def _():
        sq_copy(hg, hg).wait_send()
        for q in range(CHUNKS):
            p_copy(q).wait_send()

    sent(tot_in, tot_send.at[0]).wait_send()
    sent(run_tot, vtot_send.at[0]).wait_send()
    each(z + 1, NZ, lambda to: log_copy(to, z).wait_send())
    for r in range(1, NH):
        here_copy(r).wait_send()

    @pl.when(jnp.logical_not(stays))
    def _():
        for n in range(3):
            home_copy(n).wait_send()

    for q in range(HALVES):
        sent(st_out.at[q], st_send.at[q]).wait_send()
        for s in range(2):
            run_targets(s, lambda to: run_copy(q, s, to).wait_send())
            pl.when(NZ // 2 * s + z // 2 != z)(pre_copy(q, s).wait_send)
        pl.when(pre_relays)(pre_pass(q).wait_send)
        sent(en_out.at[q], en_send.at[q]).wait_send()


def body(query, keys, values, norm_gain, in_b, out_c, step, log_decay, skip):
    feats = query.shape[2]
    gain = norm_gain.reshape(feats // HDIM, HDIM)
    dma = pltpu.SemaphoreType.DMA
    vm = pltpu.VMEM
    scratch = [
        vm((2, BLK, feats), BF16),
        vm((2, BLK, 256), BF16),
        vm((2, BLK, 256), BF16),
        vm((4 * BLK, 256), BF16),
        vm((4 * BLK, 256), BF16),
        vm((8, HDIM), F32),
        vm((SPAN, STATE), BF16),
        vm((SPAN, STATE), BF16),
        vm((16, SPAN), F32),
        vm((16, SPAN), F32),
        vm((16, 8, SPAN), F32),
        vm((16, 8, SPAN), F32),
        vm((feats, 128), F32),
        vm((16, SPAN, SPAN), BF16),
        vm((SPAN, feats), F32),
        vm((feats, SPAN), BF16),
        vm((2, feats, SPAN), BF16),
        vm((feats, SPAN), BF16),
        vm((8, SPAN), F32),
        vm((2, 8, SPAN), F32),
        vm((NH, 8, SPAN), F32),
        vm((NH, 8, SPAN), F32),
        vm((feats, SPAN), BF16),
        vm((SPAN, feats), F32),
        vm((16, SPAN), BF16),
        vm((16, SPAN), BF16),
        vm((SPAN, STATE), BF16),
        vm((16, 128), F32),
        vm((16, 128), F32),
        vm((8, 8, 128), F32),
        vm((8, 8, 128), F32),
        vm((PLANE, 8, 128), F32),
        vm((PLANE, 8, 128), F32),
        vm((PLANE, 8, 128), F32),
        vm((2, 8, 128), F32),
        vm((NZ, 2, 8, 128), F32),
        vm((HALVES, PLANE, SLICE, STATE), BF16),
        vm((HALVES, PLANE, SLICE, STATE), BF16),
        vm((HALVES, 2, 8, SLICE, STATE), BF16),
        vm((HALVES, 3, 8, SLICE, STATE), BF16),
        vm((HALVES, 2, SLICE, STATE), BF16),
        vm((HALVES, 2 * NZ, SLICE, STATE), BF16),
        vm((HALVES, PLANE, SLICE, STATE), BF16),
        vm((HALVES, PLANE, SLICE, STATE), BF16),
        pltpu.SMEM((16,), F32),
        dma((11,)),
        dma((2, 2, 2)), dma((2, 2, 2)),
        dma((2, 2)), dma((2, 2)),
        dma((2,)), dma((2,)),
        dma((CHUNKS,)), dma((2, CHUNKS)),
        dma((CHUNKS,)),
        dma((CHUNKS,)), dma((CHUNKS,)),
        dma((1,)), dma((2,)), dma((1,)),
        dma((NH,)), dma((NH,)),
        dma((NH,)), dma((NH,)),
        dma((3,)), dma((3,)),
        dma((1,)), dma((1,)),
        dma((HALVES, 2)), dma((HALVES, 3)), dma((HALVES,)),
        dma((1,)), dma((1,)),
        dma((NZ,)), dma((NZ,)),
        dma((HALVES,)), dma((HALVES,)),
        dma((HALVES, 2, NZ)), dma((HALVES, 2 * NZ)),
        dma((HALVES,)), dma((HALVES,)),
        pltpu.SemaphoreType.REGULAR,
        pltpu.SemaphoreType.REGULAR,
        pltpu.SemaphoreType.REGULAR,
        pltpu.SemaphoreType.REGULAR,
    ]
    anywhere = pl.BlockSpec(memory_space=pltpu.HBM)
    pinned = [
        pltpu.with_memory_space_constraint(a, pltpu.HBM)
        for a in (query, keys, values, gain, in_b, out_c, step, log_decay, skip)
    ]
    return pl.pallas_call(
        kernel,
        out_shape=jax.ShapeDtypeStruct((SPAN, feats), BF16),
        in_specs=[anywhere] * 9,
        out_specs=pl.BlockSpec(memory_space=pltpu.VMEM),
        scratch_shapes=scratch,
        compiler_params=pltpu.CompilerParams(
            collective_id=0, has_side_effects=True, vmem_limit_bytes=24 * 1024 * 1024
        ),
    )(*pinned)


def solution(mesh):
    torus = Mesh(mesh.devices.reshape(NZ, NX, NY, NC, NH), AXES)
    return jax.shard_map(
        body,
        mesh=torus,
        in_specs=(
            P(None, SEQ, "head"),
            P(None, SEQ, "head"),
            P(None, SEQ, "head"),
            P("head"),
            P(SEQ, None),
            P(SEQ, None),
            P("head", SEQ),
            P("head", SEQ),
            P("head"),
        ),
        out_specs=P(SEQ, "head"),
        check_vma=False,
    )
```

```python
import math

import jax
import jax.numpy as jnp
from jax import lax
from jax.experimental import pallas as pl
from jax.experimental.pallas import tpu as pltpu
from jax.sharding import Mesh
from jax.sharding import PartitionSpec as P

HDIM = 128
SDIM = 64
STATE = 128
SPAN = 256
BLK = 128
FEATS = 4096
NZ, NX, NY, NC, NH = 8, 4, 2, 2, 4
CHIPS = NZ * NX * NY
PLANE = NX * NY * NC
CHUNKS = 4
WIDE = 256
HALVES = 2
HALF = 512
SLICE = 32
AXES = ("z", "x", "y", "core", "head")
SEQ = ("z", "x", "y", "core")
MESH = pl.DeviceIdType.MESH
F32 = jnp.float32
BF16 = jnp.bfloat16


def chip_coords(chip):
    return chip // (NX * NY), (chip // NY) % NX, chip % NY


def seq_coords(index):
    return index // PLANE, (index // (NY * NC)) % NX, (index // NC) % NY, index % NC


def dot(a, b, dims, **kw):
    return lax.dot_general(a, b, (dims, ((), ())), preferred_element_type=F32, **kw)


def kernel(
    q_hbm, k_hbm, v_hbm, gain_hbm, b_hbm, c_hbm, step_hbm, decay_hbm, skip_hbm,
    out_ref,
    q_span, k_stage, v_stage, k_win, v_win, gain_v, b_v, c_v, step_v, decay_v,
    cum_v, v_v, gcol, mix, ecum, att, z_in, att_in, sq_out, sq_mid, sq_in, sq_here, weighted, local,
    w_low, w_here, b_here, tot_low, tot_row, tot_here, tot_out, tot_in, run_tot, starts, plane_out, plane_in,
    st_out, st_in, pre_out, pre_in, run_out, run_in, en_out, en_in,
    skip_ref, load_sem, halo_send, halo_recv, swap_send, swap_recv, q_send, q_recv, z_send, z_recv,
    relay_send, att_send, att_recv, sqz_send, sqz_recv, sqr_send, sq_send, sq_recv,
    here_send, here_recv, home_send, home_recv, vtot_send, vtot_recv, pre_send, pre_recv, pre_on,
    tot_send, tot_recv, log_send, log_recv, st_send, st_recv, run_send, run_recv,
    en_send, en_recv, ready_sem, later_sem, home_ready, head_sem,
):
    z, x, y, core, hg = (lax.axis_index(a) for a in AXES)
    chip = (z * NX + x) * NY + y
    me = (x * NY + y) * NC + core
    other = 1 - core
    partner = (z, x, y, other, hg)

    after = (chip + 1) % CHIPS
    az, ax, ay = chip_coords(after)
    wraps = (chip == CHIPS - 1).astype(jnp.int32)
    before = (chip + CHIPS - 1) % CHIPS
    bz, bx, by = chip_coords(before)

    span = core * CHIPS + chip
    long_out = z == jnp.where(core == 0, NZ - 1, 0)
    long_out = jnp.where(long_out, 1, 0)
    relays = jnp.where(z == jnp.where(core == 0, 1, NZ - 2), 1, 0)
    long_in = jnp.where(z == jnp.where(core == 0, NZ // 2, NZ // 2 - 1), 1, 0)
    relay_of = jnp.where(core == 0, 1, NZ - 2)
    to_z = jnp.where(long_out == 1, relay_of, NZ // 2 * core + z // 2)
    to_core = jnp.where(long_out == 1, core, z % 2)
    z_to = (to_z, x, y, to_core, hg)
    long_half = jnp.where(z == jnp.where(core == 0, 5, 2), 1, 0)
    helps = z == jnp.where(core == 0, 0, NZ - 1)
    half_to = (
        jnp.where(long_half == 1, jnp.where(core == 0, 0, NZ - 1), to_z), x, y,
        jnp.where(long_half == 1, core, to_core), hg,
    )
    half_out = jnp.maximum(long_out, long_half)
    from_z = jnp.where(long_in == 1, jnp.where(core == 0, NZ - 2, 1), 2 * (z % (NZ // 2)) + core)
    from_core = jnp.where(long_in == 1, other, z // (NZ // 2))
    z_from = (from_z, x, y, from_core, hg)
    relay_from = (jnp.where(core == 0, NZ - 1, 0), x, y, core, hg)
    relay_z = jnp.where(
        helps, jnp.where(core == 0, 2, 5), jnp.where(core == 0, NZ // 2 - 1, NZ // 2)
    )
    relay_to = (relay_z, x, y, other, hg)
    z_stays = jnp.logical_and(to_z == z, to_core == core)
    z_moves = jnp.logical_not(z_stays)
    relaying = relays == 1
    p_to = (z, 2 * core + x // 2, x % 2, y, hg)
    p_from = (z, 2 * (x % 2) + y, core, x // 2, hg)
    p_stays = jnp.logical_and(p_to[1] == x, jnp.logical_and(p_to[2] == y, p_to[3] == core))
    p_moves = jnp.logical_not(p_stays)

    seq = z * PLANE + me
    fz, fx, fy, fc = seq_coords(span)
    home = (fz, fx, fy, fc, hg)
    sz, sx, sy = chip_coords(seq % CHIPS)
    away = (sz, sx, sy, seq // CHIPS, hg)
    stays = span == seq

    mine = pl.ds(pl.multiple_of((2 + core) * BLK, BLK), BLK)
    theirs = pl.ds(pl.multiple_of((2 + other) * BLK, BLK), BLK)
    prev_row = pl.ds(pl.multiple_of(core * BLK, BLK), BLK)
    loads = [
        (decay_hbm, decay_v), (step_hbm, step_v), (k_hbm, k_stage), (v_hbm, v_stage),
        (k_hbm.at[core], k_win.at[mine]), (v_hbm.at[core], v_win.at[mine]),
        (q_hbm.at[core], q_span.at[core]),
        (b_hbm, b_v), (c_hbm, c_v), (gain_hbm, gain_v), (skip_hbm, skip_ref),
    ]
    loads = [pltpu.make_async_copy(s, d, load_sem.at[i]) for i, (s, d) in enumerate(loads)]
    for copy in loads:
        copy.start()

    barrier = pltpu.get_barrier_semaphore()

    def greet(device):
        pl.semaphore_signal(barrier, inc=1, device_id=device, device_id_type=MESH)

    def plane_device(index):
        return (z, index // (NY * NC), (index // NC) % NY, index % NC, hg)

    def z_device(index):
        return (index, x, y, core, hg)

    def ring(act):
        def visit(r, carry):
            act((me + r) % PLANE)
            return carry

        lax.fori_loop(1, PLANE, visit, 0)

    def each(low, high, act):
        def visit(n, carry):
            act(n)
            return carry

        lax.fori_loop(low, high, visit, 0)

    greet((bz, bx, by, 0, hg))
    greet((bz, bx, by, 1, hg))
    ring(lambda n: greet(plane_device(n)))

    def rank(h):
        return jnp.where(h == 0, 0, jnp.where(h == 2, 2, 1))

    level = rank(hg)
    same = (z, x, y, core)

    def to_heads(position, test, act):
        for r in range(1, NH):
            h = (hg + r) % NH

            @pl.when(test(rank(h)))
            def _():
                act((*position, h))

    to_heads(p_from[:4], lambda n: n >= level, greet)
    to_heads(p_to[:4], lambda n: n > level, greet)
    to_heads(same, lambda n: n >= level, greet)

    @pl.when(jnp.logical_and(z_moves, from_z > z))
    def _():
        greet(z_from)

    @pl.when(jnp.logical_and(z_moves, to_z > z))
    def _():
        greet(z_to)

    @pl.when(jnp.logical_and(relaying, core == 0))
    def _():
        greet(relay_from)

    @pl.when(jnp.logical_and(jnp.logical_or(relaying, helps), core == 0))
    def _():
        greet(relay_to)

    @pl.when(jnp.logical_and(z == 5, core == 0))
    def _():
        greet((NZ - 1, x, y, 1, hg))

    each(z + 1, NZ, lambda n: greet(z_device(n)))
    @pl.when(fz > z)
    def _():
        greet(home)

    @pl.when(sz > z)
    def _():
        greet(away)

    loads[0].wait()
    loads[1].wait()
    row = lax.broadcasted_iota(jnp.int32, (SPAN, SPAN), 0)
    col = lax.broadcasted_iota(jnp.int32, (SPAN, SPAN), 1)
    causal = row <= col
    cum = dot(decay_v[...], causal.astype(F32), ((1,), (0,)), precision=lax.Precision.HIGHEST)
    total = cum[:, SPAN - 1:]
    tail_weight = jnp.exp(total - cum) * step_v[...]
    w_low[...] = tail_weight.astype(BF16)
    tot_low[...] = jnp.broadcast_to(total, (16, 128))
    shift = jnp.log(step_v[...]) - cum
    for k in range(16):
        cum_v[k] = jnp.broadcast_to(cum[k:k + 1], (8, SPAN))
        v_v[k] = jnp.broadcast_to(shift[k:k + 1], (8, SPAN))
    for o in range(8):
        lines = [total[8 * (n % 2) + o:8 * (n % 2) + o + 1] for n in range(8)]
        tot_out[o] = jnp.broadcast_to(jnp.concatenate(lines, 0), (8, 128))
    for copy in loads[2:]:
        copy.wait()

    @pl.when(span == 0)
    def _():
        k_win[:2 * BLK] = jnp.zeros((2 * BLK, 256), BF16)
        v_win[:2 * BLK] = jnp.zeros((2 * BLK, 256), BF16)

    def one(condition):
        return jnp.where(condition, 1, 0)

    greeted = (
        z + one(jnp.logical_and(z_moves, to_z < z)) + one(jnp.logical_and(z_moves, from_z < z))
        + 2 * one(jnp.logical_and(relaying, core == 1)) + one(sz < z) + one(fz < z)
        + one(jnp.logical_and(jnp.logical_or(z == 2, z == NZ - 1), core == 1))
    )
    heads = jnp.where(level == 0, 0, jnp.where(level == 1, 5, 9))
    pl.semaphore_wait(barrier, NC + PLANE - 1 + heads + greeted)

    def reply(semaphore, device):
        pl.semaphore_signal(semaphore, inc=1, device_id=device, device_id_type=MESH)

    each(0, z, lambda n: reply(later_sem, z_device(n)))
    to_heads(p_from[:4], lambda n: n < level, lambda d: reply(head_sem, d))
    to_heads(same, lambda n: n < level, lambda d: reply(head_sem, d))

    @pl.when(jnp.logical_and(z_moves, from_z < z))
    def _():
        reply(ready_sem, z_from)

    @pl.when(jnp.logical_and(relaying, core == 1))
    def _():
        reply(ready_sem, relay_from)

    @pl.when(jnp.logical_and(z == 2, core == 1))
    def _():
        reply(ready_sem, (0, x, y, 0, hg))

    @pl.when(fz < z)
    def _():
        reply(home_ready, home)

    def remote(src, dst, send, recv, to):
        return pltpu.make_async_remote_copy(
            src_ref=src, dst_ref=dst, send_sem=send, recv_sem=recv,
            device_id=to, device_id_type=MESH,
        )

    def either(here, keep, leave):
        pl.when(here)(keep)
        pl.when(jnp.logical_not(here))(leave)

    def cols(g, width=HDIM):
        return pl.ds(g * width, width)

    def halo(i, g, slot):
        stage, window = ((k_stage, k_win), (v_stage, v_win))[i]
        to = (az, ax, ay, jnp.where(wraps == 1, 1 - slot, slot), hg)
        return remote(
            stage.at[slot, :, cols(g)], window.at[prev_row, cols(g)],
            halo_send.at[i, g, slot], halo_recv.at[i, g, core], to,
        )

    def halo_arrival(i, g, block):
        part = (k_win, v_win)[i].at[pl.ds(block * BLK, BLK), cols(g)]
        return remote(part, part, halo_send.at[i, g, 0], halo_recv.at[i, g, block], partner)

    def swap(i, g):
        stage, window = ((k_stage, k_win), (v_stage, v_win))[i]
        return remote(
            stage.at[other, :, cols(g)], window.at[mine, cols(g)],
            swap_send.at[i, g], swap_recv.at[i, g], partner,
        )

    def swap_arrival(i, g):
        part = (k_win, v_win)[i].at[theirs, cols(g)]
        return remote(part, part, swap_send.at[i, g], swap_recv.at[i, g], partner)

    def q_swap(g):
        return remote(
            q_hbm.at[other, :, cols(g, 512)], q_span.at[core, :, cols(g, 512)],
            q_send.at[g], q_recv.at[g], partner,
        )

    def q_arrival(g):
        part = q_span.at[other, :, cols(g, 512)]
        return remote(part, part, q_send.at[g], q_recv.at[g], partner)

    last_chip = chip == CHIPS - 1
    home_pairs = ((b_v, b_here), (w_low, w_here), (tot_low, tot_row))

    def home_copy(n):
        return remote(
            home_pairs[n][0], home_pairs[n][1], home_send.at[n], home_recv.at[n], away
        )

    def home_keep(n):
        return pltpu.make_async_copy(home_pairs[n][0], home_pairs[n][1], home_recv.at[n])

    def send_home():
        for n in range(3):
            either(stays, home_keep(n).start, home_copy(n).start)

    def send_halo(g):
        for i in range(2):
            halo(i, g, 0).start()
            pl.when(jnp.logical_not(last_chip))(halo(i, g, 1).start)
        q_swap(g).start()
        for i in range(2):
            swap(i, g).start()

    send_halo(0)
    pl.when(sz <= z)(send_home)
    send_halo(1)

    def tot_copy(to):
        return remote(
            tot_out.at[to // 2], tot_in.at[me], tot_send.at[0], tot_recv.at[0], plane_device(to)
        )

    ring(lambda to: tot_copy(to).start())
    tot_in[me] = tot_out[me // 2]
    for p in range(8):
        line = jnp.broadcast_to(gain_v[p:p + 1, :], (BLK, BLK))
        gcol[p * BLK:(p + 1) * BLK, :] = jnp.transpose(line)

    scale = math.log2(math.e) / math.sqrt(HDIM)
    j = lax.broadcasted_iota(jnp.int32, (3 * BLK, 4 * BLK), 0)
    i = lax.broadcasted_iota(jnp.int32, (3 * BLK, 4 * BLK), 1) % BLK
    first = one(span == 0)

    def part(q):
        return pl.ds(q * WIDE, WIDE)

    def z_copy(q):
        slot, to = (long_out, z_to) if q < 2 else (half_out, half_to)
        return remote(att.at[part(q)], z_in.at[slot, part(q)], z_send.at[q], z_recv.at[slot, q], to)

    def z_keep(q):
        return pltpu.make_async_copy(att.at[part(q)], z_in.at[0, part(q)], z_recv.at[0, q])

    def relay_copy(q):
        return remote(
            z_in.at[1, part(q)], z_in.at[0, part(q)], relay_send.at[q], z_recv.at[0, q], relay_to
        )

    def z_arrival(at, q):
        return remote(
            z_in.at[at, part(q)], z_in.at[at, part(q)], relay_send.at[q], z_recv.at[at, q], relay_to
        )

    def p_copy(q):
        return remote(z_in.at[0, part(q)], att_in.at[part(q)], att_send.at[q], att_recv.at[q], p_to)

    def p_keep(q):
        return pltpu.make_async_copy(z_in.at[0, part(q)], att_in.at[part(q)], att_recv.at[q])

    def sqz_copy():
        return remote(sq_out, sq_mid.at[long_out], sqz_send.at[0], sqz_recv.at[long_out], z_to)

    def sqz_keep():
        return pltpu.make_async_copy(sq_out, sq_mid.at[0], sqz_recv.at[0])

    def sqr_copy():
        return remote(sq_mid.at[1], sq_mid.at[0], sqr_send.at[0], sqz_recv.at[0], relay_to)

    def sqz_arrival(at):
        return remote(sq_mid.at[at], sq_mid.at[at], sqr_send.at[0], sqz_recv.at[at], relay_to)

    def sq_copy(to, at):
        return remote(
            sq_mid.at[0], sq_in.at[at], sq_send.at[to], sq_recv.at[at],
            (z, p_to[1], p_to[2], p_to[3], to),
        )

    def sq_keep():
        return pltpu.make_async_copy(sq_mid.at[0], sq_in.at[hg], sq_recv.at[hg])

    def here_copy(r):
        return remote(
            sq_out, sq_here.at[hg], here_send.at[r], here_recv.at[hg],
            (z, x, y, core, (hg + r) % NH),
        )

    def here_arrival(r):
        n = (hg + r) % NH
        return remote(sq_here.at[n], sq_here.at[n], here_send.at[r], here_recv.at[n], partner)

    @pl.when(sz > z)
    def _():
        pl.semaphore_wait(home_ready, 1)
        send_home()

    sums = [jnp.zeros((1, BLK), F32) for _ in range(2)]
    for g in range(2):
        @pl.when(span > 0)
        def _():
            for t in range(2):
                for block in range(2):
                    halo_arrival(t, g, block).wait_recv()

        for t in range(2):
            swap_arrival(t, g).wait_recv()
        q_arrival(g).wait_recv()
        lanes = slice(g * HDIM, (g + 1) * HDIM)
        for a in range(2):
            keys = k_win[a * BLK:(a + 3) * BLK, lanes]
            vals = jnp.transpose(v_win[a * BLK:(a + 3) * BLK, lanes])
            heads = [q_span[a, :, (4 * g + h) * HDIM:(4 * g + h + 1) * HDIM] for h in range(4)]
            score = dot(keys, jnp.concatenate(heads, 0), ((1,), (1,)))
            low = jnp.maximum(i + 1, first * (2 - a) * BLK)
            allowed = (j >= low) & (j <= i + 2 * BLK)
            score = jnp.where(allowed, score, -jnp.inf)
            peak = jnp.max(score, axis=0, keepdims=True)
            terms = jnp.exp2((score - peak) * scale)
            sum_terms = jnp.sum(terms, axis=0, keepdims=True)
            got = dot(vals, terms.astype(BF16), ((1,), (0,)))
            got = (got * (1.0 / sum_terms)).astype(BF16)
            for h in range(4):
                head = got[:, h * BLK:(h + 1) * BLK]
                att[(4 * g + h) * HDIM:(4 * g + h + 1) * HDIM, a * BLK:(a + 1) * BLK] = head
                wide = head.astype(F32)
                sums[a] = sums[a] + jnp.sum(wide * wide, axis=0, keepdims=True)
        if g == 0:
            @pl.when(jnp.logical_and(z_moves, to_z > z))
            def _():
                pl.semaphore_wait(ready_sem, 1)
        else:
            sq_out[...] = jnp.broadcast_to(jnp.concatenate(sums, 1), (8, SPAN))

            @pl.when(level < 2)
            def _():
                pl.semaphore_wait(head_sem, jnp.where(level == 0, 6, 2))

            for r in range(1, NH):
                here_copy(r).start()
            sq_here[hg] = sq_out[...]
            either(z_stays, lambda: sqz_keep().start(), lambda: sqz_copy().start())

            @pl.when(z < NZ - 1)
            def _():
                pl.semaphore_wait(later_sem, NZ - 1 - z)

        for q in (2 * g, 2 * g + 1):
            either(z_stays, z_keep(q).start, z_copy(q).start)
    cross = dot(b_v[...], c_v[...], ((1,), (1,)))

    def make_mix(k, carry):
        ct = cum_v[k, 0:1, :]
        for ub in range(2):
            line = v_v[k, 0:1, ub * BLK:(ub + 1) * BLK]
            colb = jnp.transpose(jnp.broadcast_to(line, (BLK, BLK)))
            arg = ct + jnp.concatenate([colb, colb], 1)
            rows = slice(ub * BLK, (ub + 1) * BLK)
            arg = jnp.where(causal[rows], arg, -jnp.inf)
            mix[k, rows] = (jnp.exp(arg) * cross[rows]).astype(BF16)
        return carry

    lax.fori_loop(0, 16, make_mix, 0)

    def make_ecum(p, carry):
        lanes = pl.ds(pl.multiple_of(p * BLK, BLK), BLK)
        for tb in range(2):
            half = slice(tb * BLK, (tb + 1) * BLK)
            pair = [
                jnp.broadcast_to(jnp.exp(cum_v[2 * p + h, 0:1, half]), (SDIM, BLK))
                for h in range(2)
            ]
            ecum[half, lanes] = jnp.transpose(jnp.concatenate(pair, 0))
        return carry

    lax.fori_loop(0, 8, make_ecum, 0)

    @pl.when(jnp.logical_and(jnp.logical_or(relaying, helps), core == 0))
    def _():
        pl.semaphore_wait(ready_sem, 1)

    def relay(q, here):
        @pl.when(here)
        def _():
            z_arrival(1, q).wait_recv()
            relay_copy(q).start()

    def relay_squares():
        @pl.when(relaying)
        def _():
            sqz_arrival(1).wait_recv()
            sqr_copy().start()

    def arrive(q):
        either(z_stays, z_keep(q).wait, z_arrival(0, q).wait_recv)
        either(p_stays, p_keep(q).start, p_copy(q).start)

    def arrive_squares():
        either(z_stays, lambda: sqz_keep().wait(), lambda: sqz_arrival(0).wait_recv())
        for r in range(1, NH):
            sq_copy((hg + r) % NH, hg).start()
        either(p_stays, lambda: sq_keep().start(), lambda: sq_copy(hg, hg).start())

    def st_copy(q, to):
        return remote(
            st_out.at[q, to], st_in.at[q, me], st_send.at[q], st_recv.at[q], plane_device(to)
        )

    def vtot_copy(to):
        return remote(
            tot_here.at[to // 2], run_tot.at[me], vtot_send.at[0], vtot_recv.at[0],
            plane_device(to),
        )

    after_first = pl.ds(1, 7)

    def pre_copy(q, s):
        far = z == (0 if s else NZ - 1)
        to = jnp.where(far, NZ - 2 if s else 1, NZ // 2 * s + z // 2)
        slot = jnp.where(far, 2, z % 2)
        return remote(
            pre_out.at[q, s, after_first], pre_in.at[q, slot, after_first], pre_send.at[q, s],
            pre_recv.at[q, slot], z_device(to),
        )

    def pre_arrival(q, n):
        part = pre_in.at[q, n, after_first]
        return remote(part, part, pre_send.at[q, 0], pre_recv.at[q, n], partner)

    pre_relays = jnp.logical_or(z == 1, z == NZ - 2)

    def pre_pass(q):
        slot = jnp.where(z == 1, 1, 0)
        return remote(
            pre_in.at[q, 2, after_first], pre_in.at[q, slot, after_first], pre_on.at[q], pre_recv.at[q, slot],
            z_device(jnp.where(z == 1, NZ // 2 - 1, NZ // 2)),
        )

    def pre_relay(q):
        @pl.when(pre_relays)
        def _():
            pre_arrival(q, 2).wait_recv()
            pre_pass(q).start()

    def run_copy(q, s, to):
        return remote(
            run_out.at[q, s], run_in.at[q, NZ * s + z], run_send.at[q, s, to],
            run_recv.at[q, NZ * s + z], z_device(to),
        )

    def run_arrival(q, n):
        return remote(
            run_in.at[q, n], run_in.at[q, n], run_send.at[q, 0, 0], run_recv.at[q, n], partner
        )

    def run_targets(s, act):
        @pl.when(jnp.logical_and(NZ // 2 * s + z // 2 != z, z % 2 == 0))
        def _():
            act(NZ // 2 * s + z // 2)

        def visit(n):
            pl.when(n != z)(lambda: act(n))

        each(NZ // 2 * s + z // 2 + 1, NZ, visit)

    def log_copy(to, at):
        return remote(plane_out, plane_in.at[at], log_send.at[to], log_recv.at[at], z_device(to))

    def en_copy(q, to):
        return remote(
            en_out.at[q, to], en_in.at[q, me], en_send.at[q], en_recv.at[q], plane_device(to)
        )

    def sent(buffer, semaphore):
        rest = buffer.at[pl.ds(0, PLANE - 1)]
        return remote(rest, rest, semaphore, semaphore, partner)

    def states(q):
        square = sq_here[0] + sq_here[1] + sq_here[2] + sq_here[3]
        rate = lax.rsqrt(square[0:1] / FEATS + 1e-06)
        for k in range(8 * q, 8 * q + 8):
            rows = slice(k * SDIM, (k + 1) * SDIM)
            gain = gcol[rows, :]
            value = att[rows, :].astype(F32) * jnp.concatenate([gain, gain], 1) * rate
            value = value.astype(BF16).astype(F32)
            weighted[rows, :] = (value * w_here[k:k + 1, :].astype(F32)).astype(BF16)
        state = dot(weighted[q * HALF:(q + 1) * HALF], b_here[...], ((1,), (0,)))
        st_out[q] = state.astype(BF16).reshape(PLANE, SLICE, STATE)
        ring(lambda to: st_copy(q, to).start())
        st_in[q, me] = st_out[q, me]

    def locals_(q):
        if q == 0:
            for r in range(1, NH):
                sq_copy((hg + r) % NH, (hg + r) % NH).wait_recv()
            either(p_stays, lambda: sq_keep().wait(), lambda: sq_copy(hg, hg).wait_recv())
        for c in (2 * q, 2 * q + 1):
            either(p_stays, p_keep(c).wait, p_copy(c).wait_recv)
        square = sq_in[0] + sq_in[1] + sq_in[2] + sq_in[3]
        rate = lax.rsqrt(square[0:1] / FEATS + 1e-06)

        def make_local(p, carry):
            lanes = pl.ds(pl.multiple_of(p * BLK, BLK), BLK)
            pair = []
            for h in range(2):
                k = 2 * p + h
                rows = pl.ds(pl.multiple_of(k * SDIM, SDIM), SDIM)
                gain = gcol[rows, :]
                value = att_in[rows, :].astype(F32) * jnp.concatenate([gain, gain], 1) * rate
                value = value.astype(BF16)
                pair.append(dot(value, mix[k], ((1,), (0,))) + value.astype(F32) * skip_ref[k])
            both = jnp.concatenate(pair, 0)
            for tb in range(2):
                half = slice(tb * BLK, (tb + 1) * BLK)
                local[half, lanes] = jnp.transpose(both[:, half])
            return carry

        lax.fori_loop(4 * q, 4 * q + 4, make_local, 0)

    def prefix(q):
        sent(st_in.at[q], st_recv.at[q]).wait_recv()
        for s in range(2):
            running = jnp.zeros((SLICE, STATE), F32)
            for n in range(8):
                pre_out[q, s, n] = running.astype(BF16)
                decay = jnp.exp(run_tot[2 * n + s])
                running = decay[q:q + 1] * running + st_in[q, 2 * n + s].astype(F32)
            run_out[q, s] = running.astype(BF16)
        for s in range(2):
            run_targets(s, lambda to: run_copy(q, s, to).start())
            run_in[q, NZ * s + z] = run_out[q, s]
        for s in range(2):
            own = NZ // 2 * s + z // 2 == z
            pl.when(jnp.logical_not(own))(pre_copy(q, s).start)

            @pl.when(own)
            def _():
                pre_in[q, s] = pre_out[q, s]

    def enter(q):
        for n in range(2):
            @pl.when(2 * (z % (NZ // 2)) + n != z)
            def _():
                pre_arrival(q, n).wait_recv()

        if q == 0:
            each(0, z, lambda n: log_copy(n, n).wait_recv())

        def arrived(n):
            pl.when(n % NZ != z)(run_arrival(q, n).wait_recv)

        def gather(p, carried):
            for n in range(2):
                arrived(2 * p + n)
                decay = jnp.exp(plane_in[p, n])
                carried = decay[q:q + 1] * carried + run_in[q, 2 * p + n].astype(F32)
            return carried

        carried = lax.fori_loop(0, z, gather, jnp.zeros((SLICE, STATE), F32))
        en_out[q, 0] = carried.astype(BF16)
        for n in range(1, 8):
            value = pre_in[q, 0, n].astype(F32) + starts[n, q:q + 1] * carried
            en_out[q, n] = value.astype(BF16)
        arrived(2 * z)
        carried = jnp.exp(plane_out[0])[q:q + 1] * carried + run_in[q, 2 * z].astype(F32)
        en_out[q, 8] = carried.astype(BF16)
        for n in range(1, 8):
            value = pre_in[q, 1, n].astype(F32) + starts[8 + n, q:q + 1] * carried
            en_out[q, 8 + n] = value.astype(BF16)
        ring(lambda to: en_copy(q, to).start())
        en_in[q, me] = en_out[q, me]

    def finish(q):
        sent(en_in.at[q], en_recv.at[q]).wait_recv()
        lanes = slice(q * HALF, (q + 1) * HALF)
        entry = dot(c_v[...], en_in[q].reshape(HALF, STATE), ((1,), (1,)))
        out_ref[:, lanes] = (local[:, lanes] + ecum[:, lanes] * entry).astype(BF16)

    relay(0, relaying)
    for n in range(3):
        either(stays, home_keep(n).wait, home_copy(n).wait_recv)
    for o in range(8):
        lines = [tot_row[8 * (n % 2) + o:8 * (n % 2) + o + 1] for n in range(8)]
        tot_here[o] = jnp.concatenate(lines, 0)
    ring(lambda to: vtot_copy(to).start())
    run_tot[me] = tot_here[me // 2]
    for r in range(1, NH):
        here_arrival(r).wait_recv()
    for q in range(HALVES):
        states(q)

    relay(1, relaying)
    relay_squares()
    sent(tot_in, tot_recv.at[0]).wait_recv()
    for r in range(2):
        logs = jnp.zeros((8, 128), F32)
        for n in range(8 * r, 8 * r + 8):
            starts[n] = jnp.exp(logs)
            logs = logs + tot_in[n]
        plane_out[r] = logs

    each(z + 1, NZ, lambda to: log_copy(to, z).start())
    late = jnp.logical_or(
        jnp.logical_and(core == 0, z // 2 == 2), jnp.logical_and(core == 1, z // 2 == 1)
    )
    prompt = jnp.logical_not(late)
    pl.when(prompt)(lambda: arrive(0))
    relay(2, relaying)
    pl.when(prompt)(lambda: arrive(1))
    relay(3, relaying)
    sent(run_tot, vtot_recv.at[0]).wait_recv()
    prefix(0)
    prefix(1)
    relay(2, helps)
    relay(3, helps)
    for q in range(2):
        pl.when(late)(lambda: arrive(q))
    arrive_squares()
    arrive(2)
    arrive(3)
    pre_relay(0)
    pre_relay(1)
    enter(0)
    enter(1)
    locals_(0)
    locals_(1)
    finish(0)
    finish(1)

    for g in range(2):
        for t in range(2):
            halo(t, g, 0).wait_send()
            pl.when(jnp.logical_not(last_chip))(halo(t, g, 1).wait_send)
            swap(t, g).wait_send()
        q_swap(g).wait_send()
    for r in range(1, NH):
        sq_copy((hg + r) % NH, hg).wait_send()

    @pl.when(z_moves)
    def _():
        sqz_copy().wait_send()
        for q in range(CHUNKS):
            z_copy(q).wait_send()

    @pl.when(relaying)
    def _():
        sqr_copy().wait_send()
        for q in range(2):
            relay_copy(q).wait_send()

    @pl.when(jnp.logical_or(relaying, helps))
    def _():
        for q in range(2, CHUNKS):
            relay_copy(q).wait_send()

    @pl.when(p_moves)
    def _():
        sq_copy(hg, hg).wait_send()
        for q in range(CHUNKS):
            p_copy(q).wait_send()

    sent(tot_in, tot_send.at[0]).wait_send()
    sent(run_tot, vtot_send.at[0]).wait_send()
    each(z + 1, NZ, lambda to: log_copy(to, z).wait_send())
    for r in range(1, NH):
        here_copy(r).wait_send()

    @pl.when(jnp.logical_not(stays))
    def _():
        for n in range(3):
            home_copy(n).wait_send()

    for q in range(HALVES):
        sent(st_out.at[q], st_send.at[q]).wait_send()
        for s in range(2):
            run_targets(s, lambda to: run_copy(q, s, to).wait_send())
            pl.when(NZ // 2 * s + z // 2 != z)(pre_copy(q, s).wait_send)
        pl.when(pre_relays)(pre_pass(q).wait_send)
        sent(en_out.at[q], en_send.at[q]).wait_send()


def body(query, keys, values, norm_gain, in_b, out_c, step, log_decay, skip):
    feats = query.shape[2]
    gain = norm_gain.reshape(feats // HDIM, HDIM)
    dma = pltpu.SemaphoreType.DMA
    vm = pltpu.VMEM
    scratch = [
        vm((2, BLK, feats), BF16),
        vm((2, BLK, 256), BF16),
        vm((2, BLK, 256), BF16),
        vm((4 * BLK, 256), BF16),
        vm((4 * BLK, 256), BF16),
        vm((8, HDIM), F32),
        vm((SPAN, STATE), BF16),
        vm((SPAN, STATE), BF16),
        vm((16, SPAN), F32),
        vm((16, SPAN), F32),
        vm((16, 8, SPAN), F32),
        vm((16, 8, SPAN), F32),
        vm((feats, 128), F32),
        vm((16, SPAN, SPAN), BF16),
        vm((SPAN, feats), F32),
        vm((feats, SPAN), BF16),
        vm((2, feats, SPAN), BF16),
        vm((feats, SPAN), BF16),
        vm((8, SPAN), F32),
        vm((2, 8, SPAN), F32),
        vm((NH, 8, SPAN), F32),
        vm((NH, 8, SPAN), F32),
        vm((feats, SPAN), BF16),
        vm((SPAN, feats), F32),
        vm((16, SPAN), BF16),
        vm((16, SPAN), BF16),
        vm((SPAN, STATE), BF16),
        vm((16, 128), F32),
        vm((16, 128), F32),
        vm((8, 8, 128), F32),
        vm((8, 8, 128), F32),
        vm((PLANE, 8, 128), F32),
        vm((PLANE, 8, 128), F32),
        vm((PLANE, 8, 128), F32),
        vm((2, 8, 128), F32),
        vm((NZ, 2, 8, 128), F32),
        vm((HALVES, PLANE, SLICE, STATE), BF16),
        vm((HALVES, PLANE, SLICE, STATE), BF16),
        vm((HALVES, 2, 8, SLICE, STATE), BF16),
        vm((HALVES, 3, 8, SLICE, STATE), BF16),
        vm((HALVES, 2, SLICE, STATE), BF16),
        vm((HALVES, 2 * NZ, SLICE, STATE), BF16),
        vm((HALVES, PLANE, SLICE, STATE), BF16),
        vm((HALVES, PLANE, SLICE, STATE), BF16),
        pltpu.SMEM((16,), F32),
        dma((11,)),
        dma((2, 2, 2)), dma((2, 2, 2)),
        dma((2, 2)), dma((2, 2)),
        dma((2,)), dma((2,)),
        dma((CHUNKS,)), dma((2, CHUNKS)),
        dma((CHUNKS,)),
        dma((CHUNKS,)), dma((CHUNKS,)),
        dma((1,)), dma((2,)), dma((1,)),
        dma((NH,)), dma((NH,)),
        dma((NH,)), dma((NH,)),
        dma((3,)), dma((3,)),
        dma((1,)), dma((1,)),
        dma((HALVES, 2)), dma((HALVES, 3)), dma((HALVES,)),
        dma((1,)), dma((1,)),
        dma((NZ,)), dma((NZ,)),
        dma((HALVES,)), dma((HALVES,)),
        dma((HALVES, 2, NZ)), dma((HALVES, 2 * NZ)),
        dma((HALVES,)), dma((HALVES,)),
        pltpu.SemaphoreType.REGULAR,
        pltpu.SemaphoreType.REGULAR,
        pltpu.SemaphoreType.REGULAR,
        pltpu.SemaphoreType.REGULAR,
    ]
    anywhere = pl.BlockSpec(memory_space=pltpu.HBM)
    pinned = [
        pltpu.with_memory_space_constraint(a, pltpu.HBM)
        for a in (query, keys, values, gain, in_b, out_c, step, log_decay, skip)
    ]
    return pl.pallas_call(
        kernel,
        out_shape=jax.ShapeDtypeStruct((SPAN, feats), BF16),
        in_specs=[anywhere] * 9,
        out_specs=pl.BlockSpec(memory_space=pltpu.VMEM),
        scratch_shapes=scratch,
        compiler_params=pltpu.CompilerParams(
            collective_id=0, has_side_effects=True, vmem_limit_bytes=24 * 1024 * 1024
        ),
    )(*pinned)


def solution(mesh):
    torus = Mesh(mesh.devices.reshape(NZ, NX, NY, NC, NH), AXES)
    return jax.shard_map(
        body,
        mesh=torus,
        in_specs=(
            P(None, SEQ, "head"),
            P(None, SEQ, "head"),
            P(None, SEQ, "head"),
            P("head"),
            P(SEQ, None),
            P(SEQ, None),
            P("head", SEQ),
            P("head", SEQ),
            P("head"),
        ),
        out_specs=P(SEQ, "head"),
        check_vma=False,
    )
```

```python
import math

import jax
import jax.numpy as jnp
from jax import lax
from jax.experimental import pallas as pl
from jax.experimental.pallas import tpu as pltpu
from jax.sharding import Mesh
from jax.sharding import PartitionSpec as P

HDIM = 128
SDIM = 64
STATE = 128
SPAN = 256
BLK = 128
FEATS = 4096
NZ, NX, NY, NC, NH = 8, 4, 2, 2, 4
CHIPS = NZ * NX * NY
PLANE = NX * NY * NC
CHUNKS = 4
WIDE = 256
HALVES = 2
HALF = 512
SLICE = 32
AXES = ("z", "x", "y", "core", "head")
SEQ = ("z", "x", "y", "core")
MESH = pl.DeviceIdType.MESH
F32 = jnp.float32
BF16 = jnp.bfloat16


def chip_coords(chip):
    return chip // (NX * NY), (chip // NY) % NX, chip % NY


def seq_coords(index):
    return index // PLANE, (index // (NY * NC)) % NX, (index // NC) % NY, index % NC


def dot(a, b, dims, **kw):
    return lax.dot_general(a, b, (dims, ((), ())), preferred_element_type=F32, **kw)


def kernel(
    q_hbm, k_hbm, v_hbm, gain_hbm, b_hbm, c_hbm, step_hbm, decay_hbm, skip_hbm,
    out_ref,
    q_span, k_stage, v_stage, k_win, v_win, gain_v, b_v, c_v, step_v, decay_v,
    cum_v, v_v, gcol, mix, ecum, att, z_in, att_in, sq_out, sq_mid, sq_in, sq_here, weighted, local,
    w_low, w_here, b_here, tot_low, tot_row, tot_here, tot_out, tot_in, run_tot, starts, plane_out, plane_in,
    st_out, st_in, pre_out, pre_in, run_out, run_in, en_out, en_in,
    skip_ref, load_sem, halo_send, halo_recv, swap_send, swap_recv, q_send, q_recv, z_send, z_recv,
    relay_send, att_send, att_recv, sqz_send, sqz_recv, sqr_send, sq_send, sq_recv,
    here_send, here_recv, home_send, home_recv, vtot_send, vtot_recv, pre_send, pre_recv, pre_on,
    tot_send, tot_recv, log_send, log_recv, st_send, st_recv, run_send, run_recv,
    en_send, en_recv, ready_sem, later_sem, home_ready, head_sem,
):
    z, x, y, core, hg = (lax.axis_index(a) for a in AXES)
    chip = (z * NX + x) * NY + y
    me = (x * NY + y) * NC + core
    other = 1 - core
    partner = (z, x, y, other, hg)

    after = (chip + 1) % CHIPS
    az, ax, ay = chip_coords(after)
    wraps = (chip == CHIPS - 1).astype(jnp.int32)
    before = (chip + CHIPS - 1) % CHIPS
    bz, bx, by = chip_coords(before)

    span = core * CHIPS + chip
    long_out = z == jnp.where(core == 0, NZ - 1, 0)
    long_out = jnp.where(long_out, 1, 0)
    relays = jnp.where(z == jnp.where(core == 0, 1, NZ - 2), 1, 0)
    long_in = jnp.where(z == jnp.where(core == 0, NZ // 2, NZ // 2 - 1), 1, 0)
    relay_of = jnp.where(core == 0, 1, NZ - 2)
    to_z = jnp.where(long_out == 1, relay_of, NZ // 2 * core + z // 2)
    to_core = jnp.where(long_out == 1, core, z % 2)
    z_to = (to_z, x, y, to_core, hg)
    long_half = jnp.where(z == jnp.where(core == 0, 5, 2), 1, 0)
    helps = z == jnp.where(core == 0, 0, NZ - 1)
    half_to = (
        jnp.where(long_half == 1, jnp.where(core == 0, 0, NZ - 1), to_z), x, y,
        jnp.where(long_half == 1, core, to_core), hg,
    )
    half_out = jnp.maximum(long_out, long_half)
    from_z = jnp.where(long_in == 1, jnp.where(core == 0, NZ - 2, 1), 2 * (z % (NZ // 2)) + core)
    from_core = jnp.where(long_in == 1, other, z // (NZ // 2))
    z_from = (from_z, x, y, from_core, hg)
    relay_from = (jnp.where(core == 0, NZ - 1, 0), x, y, core, hg)
    relay_z = jnp.where(
        helps, jnp.where(core == 0, 2, 5), jnp.where(core == 0, NZ // 2 - 1, NZ // 2)
    )
    relay_to = (relay_z, x, y, other, hg)
    z_stays = jnp.logical_and(to_z == z, to_core == core)
    z_moves = jnp.logical_not(z_stays)
    relaying = relays == 1
    p_to = (z, 2 * core + x // 2, x % 2, y, hg)
    p_from = (z, 2 * (x % 2) + y, core, x // 2, hg)
    p_stays = jnp.logical_and(p_to[1] == x, jnp.logical_and(p_to[2] == y, p_to[3] == core))
    p_moves = jnp.logical_not(p_stays)

    seq = z * PLANE + me
    fz, fx, fy, fc = seq_coords(span)
    home = (fz, fx, fy, fc, hg)
    sz, sx, sy = chip_coords(seq % CHIPS)
    away = (sz, sx, sy, seq // CHIPS, hg)
    stays = span == seq

    barrier = pltpu.get_barrier_semaphore()

    def greet(device):
        pl.semaphore_signal(barrier, inc=1, device_id=device, device_id_type=MESH)

    def plane_device(index):
        return (z, index // (NY * NC), (index // NC) % NY, index % NC, hg)

    def z_device(index):
        return (index, x, y, core, hg)

    def ring(act):
        def visit(r, carry):
            act((me + r) % PLANE)
            return carry

        lax.fori_loop(1, PLANE, visit, 0)

    def each(low, high, act):
        def visit(n, carry):
            act(n)
            return carry

        lax.fori_loop(low, high, visit, 0)

    greet((bz, bx, by, 0, hg))
    greet((bz, bx, by, 1, hg))
    ring(lambda n: greet(plane_device(n)))

    def rank(h):
        return jnp.where(h == 0, 0, jnp.where(h == 2, 2, 1))

    level = rank(hg)
    same = (z, x, y, core)

    def to_heads(position, test, act):
        for r in range(1, NH):
            h = (hg + r) % NH

            @pl.when(test(rank(h)))
            def _():
                act((*position, h))

    to_heads(p_from[:4], lambda n: n >= level, greet)
    to_heads(p_to[:4], lambda n: n > level, greet)
    to_heads(same, lambda n: n >= level, greet)

    @pl.when(jnp.logical_and(z_moves, from_z > z))
    def _():
        greet(z_from)

    @pl.when(jnp.logical_and(z_moves, to_z > z))
    def _():
        greet(z_to)

    @pl.when(jnp.logical_and(relaying, core == 0))
    def _():
        greet(relay_from)

    @pl.when(jnp.logical_and(jnp.logical_or(relaying, helps), core == 0))
    def _():
        greet(relay_to)

    @pl.when(jnp.logical_and(z == 5, core == 0))
    def _():
        greet((NZ - 1, x, y, 1, hg))

    each(z + 1, NZ, lambda n: greet(z_device(n)))
    @pl.when(fz > z)
    def _():
        greet(home)

    @pl.when(sz > z)
    def _():
        greet(away)

    mine = pl.ds(pl.multiple_of((2 + core) * BLK, BLK), BLK)
    theirs = pl.ds(pl.multiple_of((2 + other) * BLK, BLK), BLK)
    prev_row = pl.ds(pl.multiple_of(core * BLK, BLK), BLK)
    loads = [
        (decay_hbm, decay_v), (step_hbm, step_v), (k_hbm, k_stage), (v_hbm, v_stage),
        (k_hbm.at[core], k_win.at[mine]), (v_hbm.at[core], v_win.at[mine]),
        (q_hbm.at[core], q_span.at[core]),
        (b_hbm, b_v), (c_hbm, c_v), (gain_hbm, gain_v), (skip_hbm, skip_ref),
    ]
    loads = [pltpu.make_async_copy(s, d, load_sem.at[i]) for i, (s, d) in enumerate(loads)]
    for copy in loads:
        copy.start()

    loads[0].wait()
    loads[1].wait()
    row = lax.broadcasted_iota(jnp.int32, (SPAN, SPAN), 0)
    col = lax.broadcasted_iota(jnp.int32, (SPAN, SPAN), 1)
    causal = row <= col
    cum = dot(decay_v[...], causal.astype(F32), ((1,), (0,)), precision=lax.Precision.HIGHEST)
    total = cum[:, SPAN - 1:]
    tail_weight = jnp.exp(total - cum) * step_v[...]
    w_low[...] = tail_weight.astype(BF16)
    tot_low[...] = jnp.broadcast_to(total, (16, 128))
    shift = jnp.log(step_v[...]) - cum
    for k in range(16):
        cum_v[k] = jnp.broadcast_to(cum[k:k + 1], (8, SPAN))
        v_v[k] = jnp.broadcast_to(shift[k:k + 1], (8, SPAN))
    for o in range(8):
        lines = [total[8 * (n % 2) + o:8 * (n % 2) + o + 1] for n in range(8)]
        tot_out[o] = jnp.broadcast_to(jnp.concatenate(lines, 0), (8, 128))
    for copy in loads[2:]:
        copy.wait()

    @pl.when(span == 0)
    def _():
        k_win[:2 * BLK] = jnp.zeros((2 * BLK, 256), BF16)
        v_win[:2 * BLK] = jnp.zeros((2 * BLK, 256), BF16)

    def one(condition):
        return jnp.where(condition, 1, 0)

    greeted = (
        z + one(jnp.logical_and(z_moves, to_z < z)) + one(jnp.logical_and(z_moves, from_z < z))
        + 2 * one(jnp.logical_and(relaying, core == 1)) + one(sz < z) + one(fz < z)
        + one(jnp.logical_and(jnp.logical_or(z == 2, z == NZ - 1), core == 1))
    )
    heads = jnp.where(level == 0, 0, jnp.where(level == 1, 5, 9))
    pl.semaphore_wait(barrier, NC + PLANE - 1 + heads + greeted)

    def reply(semaphore, device):
        pl.semaphore_signal(semaphore, inc=1, device_id=device, device_id_type=MESH)

    each(0, z, lambda n: reply(later_sem, z_device(n)))
    to_heads(p_from[:4], lambda n: n < level, lambda d: reply(head_sem, d))
    to_heads(same, lambda n: n < level, lambda d: reply(head_sem, d))

    @pl.when(jnp.logical_and(z_moves, from_z < z))
    def _():
        reply(ready_sem, z_from)

    @pl.when(jnp.logical_and(relaying, core == 1))
    def _():
        reply(ready_sem, relay_from)

    @pl.when(jnp.logical_and(z == 2, core == 1))
    def _():
        reply(ready_sem, (0, x, y, 0, hg))

    @pl.when(fz < z)
    def _():
        reply(home_ready, home)

    def remote(src, dst, send, recv, to):
        return pltpu.make_async_remote_copy(
            src_ref=src, dst_ref=dst, send_sem=send, recv_sem=recv,
            device_id=to, device_id_type=MESH,
        )

    def either(here, keep, leave):
        pl.when(here)(keep)
        pl.when(jnp.logical_not(here))(leave)

    def cols(g, width=HDIM):
        return pl.ds(g * width, width)

    def halo(i, g, slot):
        stage, window = ((k_stage, k_win), (v_stage, v_win))[i]
        to = (az, ax, ay, jnp.where(wraps == 1, 1 - slot, slot), hg)
        return remote(
            stage.at[slot, :, cols(g)], window.at[prev_row, cols(g)],
            halo_send.at[i, g, slot], halo_recv.at[i, g, core], to,
        )

    def halo_arrival(i, g, block):
        part = (k_win, v_win)[i].at[pl.ds(block * BLK, BLK), cols(g)]
        return remote(part, part, halo_send.at[i, g, 0], halo_recv.at[i, g, block], partner)

    def swap(i, g):
        stage, window = ((k_stage, k_win), (v_stage, v_win))[i]
        return remote(
            stage.at[other, :, cols(g)], window.at[mine, cols(g)],
            swap_send.at[i, g], swap_recv.at[i, g], partner,
        )

    def swap_arrival(i, g):
        part = (k_win, v_win)[i].at[theirs, cols(g)]
        return remote(part, part, swap_send.at[i, g], swap_recv.at[i, g], partner)

    def q_swap(g):
        return remote(
            q_hbm.at[other, :, cols(g, 512)], q_span.at[core, :, cols(g, 512)],
            q_send.at[g], q_recv.at[g], partner,
        )

    def q_arrival(g):
        part = q_span.at[other, :, cols(g, 512)]
        return remote(part, part, q_send.at[g], q_recv.at[g], partner)

    last_chip = chip == CHIPS - 1
    home_pairs = ((b_v, b_here), (w_low, w_here), (tot_low, tot_row))

    def home_copy(n):
        return remote(
            home_pairs[n][0], home_pairs[n][1], home_send.at[n], home_recv.at[n], away
        )

    def home_keep(n):
        return pltpu.make_async_copy(home_pairs[n][0], home_pairs[n][1], home_recv.at[n])

    def send_home():
        for n in range(3):
            either(stays, home_keep(n).start, home_copy(n).start)

    def send_halo(g):
        for i in range(2):
            halo(i, g, 0).start()
            pl.when(jnp.logical_not(last_chip))(halo(i, g, 1).start)
        q_swap(g).start()
        for i in range(2):
            swap(i, g).start()

    send_halo(0)
    pl.when(sz <= z)(send_home)
    send_halo(1)

    def tot_copy(to):
        return remote(
            tot_out.at[to // 2], tot_in.at[me], tot_send.at[0], tot_recv.at[0], plane_device(to)
        )

    ring(lambda to: tot_copy(to).start())
    tot_in[me] = tot_out[me // 2]
    for p in range(8):
        line = jnp.broadcast_to(gain_v[p:p + 1, :], (BLK, BLK))
        gcol[p * BLK:(p + 1) * BLK, :] = jnp.transpose(line)

    scale = math.log2(math.e) / math.sqrt(HDIM)
    j = lax.broadcasted_iota(jnp.int32, (BLK, 4 * BLK), 0)
    i = lax.broadcasted_iota(jnp.int32, (BLK, 4 * BLK), 1) % BLK
    first = one(span == 0)
    recent = j > i + first * BLK
    until = j <= i

    def part(q):
        return pl.ds(q * WIDE, WIDE)

    def z_copy(q):
        slot, to = (long_out, z_to) if q < 2 else (half_out, half_to)
        return remote(att.at[part(q)], z_in.at[slot, part(q)], z_send.at[q], z_recv.at[slot, q], to)

    def z_keep(q):
        return pltpu.make_async_copy(att.at[part(q)], z_in.at[0, part(q)], z_recv.at[0, q])

    def relay_copy(q):
        return remote(
            z_in.at[1, part(q)], z_in.at[0, part(q)], relay_send.at[q], z_recv.at[0, q], relay_to
        )

    def z_arrival(at, q):
        return remote(
            z_in.at[at, part(q)], z_in.at[at, part(q)], relay_send.at[q], z_recv.at[at, q], relay_to
        )

    def p_copy(q):
        return remote(z_in.at[0, part(q)], att_in.at[part(q)], att_send.at[q], att_recv.at[q], p_to)

    def p_keep(q):
        return pltpu.make_async_copy(z_in.at[0, part(q)], att_in.at[part(q)], att_recv.at[q])

    def sqz_copy():
        return remote(sq_out, sq_mid.at[long_out], sqz_send.at[0], sqz_recv.at[long_out], z_to)

    def sqz_keep():
        return pltpu.make_async_copy(sq_out, sq_mid.at[0], sqz_recv.at[0])

    def sqr_copy():
        return remote(sq_mid.at[1], sq_mid.at[0], sqr_send.at[0], sqz_recv.at[0], relay_to)

    def sqz_arrival(at):
        return remote(sq_mid.at[at], sq_mid.at[at], sqr_send.at[0], sqz_recv.at[at], relay_to)

    def sq_copy(to, at):
        return remote(
            sq_mid.at[0], sq_in.at[at], sq_send.at[to], sq_recv.at[at],
            (z, p_to[1], p_to[2], p_to[3], to),
        )

    def sq_keep():
        return pltpu.make_async_copy(sq_mid.at[0], sq_in.at[hg], sq_recv.at[hg])

    def here_copy(r):
        return remote(
            sq_out, sq_here.at[hg], here_send.at[r], here_recv.at[hg],
            (z, x, y, core, (hg + r) % NH),
        )

    def here_arrival(r):
        n = (hg + r) % NH
        return remote(sq_here.at[n], sq_here.at[n], here_send.at[r], here_recv.at[n], partner)

    @pl.when(sz > z)
    def _():
        pl.semaphore_wait(home_ready, 1)
        send_home()

    sums = [jnp.zeros((1, BLK), F32) for _ in range(2)]
    for g in range(2):
        @pl.when(span > 0)
        def _():
            for t in range(2):
                for block in range(2):
                    halo_arrival(t, g, block).wait_recv()

        for t in range(2):
            swap_arrival(t, g).wait_recv()
        q_arrival(g).wait_recv()
        lanes = slice(g * HDIM, (g + 1) * HDIM)
        for a in range(2):
            keys = k_win[a * BLK:(a + 3) * BLK, lanes]
            vals = jnp.transpose(v_win[a * BLK:(a + 3) * BLK, lanes])
            heads = [q_span[a, :, (4 * g + h) * HDIM:(4 * g + h + 1) * HDIM] for h in range(4)]
            score = dot(keys, jnp.concatenate(heads, 0), ((1,), (1,)))
            middle = score[BLK:2 * BLK]
            if a == 0:
                middle = jnp.where(first == 1, -jnp.inf, middle)
            score = jnp.concatenate([
                jnp.where(recent, score[:BLK], -jnp.inf), middle,
                jnp.where(until, score[2 * BLK:], -jnp.inf),
            ], 0)
            peak = jnp.max(score, axis=0, keepdims=True)
            terms = jnp.exp2((score - peak) * scale)
            sum_terms = jnp.sum(terms, axis=0, keepdims=True)
            got = dot(vals, terms.astype(BF16), ((1,), (0,)))
            got = (got * (1.0 / sum_terms)).astype(BF16)
            for h in range(4):
                head = got[:, h * BLK:(h + 1) * BLK]
                att[(4 * g + h) * HDIM:(4 * g + h + 1) * HDIM, a * BLK:(a + 1) * BLK] = head
                wide = head.astype(F32)
                sums[a] = sums[a] + jnp.sum(wide * wide, axis=0, keepdims=True)
        if g == 0:
            @pl.when(jnp.logical_and(z_moves, to_z > z))
            def _():
                pl.semaphore_wait(ready_sem, 1)
        else:
            sq_out[...] = jnp.broadcast_to(jnp.concatenate(sums, 1), (8, SPAN))

            @pl.when(level < 2)
            def _():
                pl.semaphore_wait(head_sem, jnp.where(level == 0, 6, 2))

            for r in range(1, NH):
                here_copy(r).start()
            sq_here[hg] = sq_out[...]
            either(z_stays, lambda: sqz_keep().start(), lambda: sqz_copy().start())

            @pl.when(z < NZ - 1)
            def _():
                pl.semaphore_wait(later_sem, NZ - 1 - z)

        for q in (2 * g, 2 * g + 1):
            either(z_stays, z_keep(q).start, z_copy(q).start)
    cross = dot(b_v[...], c_v[...], ((1,), (1,)))

    def make_mix(k, carry):
        ct = cum_v[k, 0:1, :]
        for ub in range(2):
            line = v_v[k, 0:1, ub * BLK:(ub + 1) * BLK]
            colb = jnp.transpose(jnp.broadcast_to(line, (BLK, BLK)))
            arg = ct + jnp.concatenate([colb, colb], 1)
            rows = slice(ub * BLK, (ub + 1) * BLK)
            arg = jnp.where(causal[rows], arg, -jnp.inf)
            mix[k, rows] = (jnp.exp(arg) * cross[rows]).astype(BF16)
        return carry

    lax.fori_loop(0, 16, make_mix, 0)

    def make_ecum(p, carry):
        lanes = pl.ds(pl.multiple_of(p * BLK, BLK), BLK)
        for tb in range(2):
            half = slice(tb * BLK, (tb + 1) * BLK)
            pair = [
                jnp.broadcast_to(jnp.exp(cum_v[2 * p + h, 0:1, half]), (SDIM, BLK))
                for h in range(2)
            ]
            ecum[half, lanes] = jnp.transpose(jnp.concatenate(pair, 0))
        return carry

    lax.fori_loop(0, 8, make_ecum, 0)

    @pl.when(jnp.logical_and(jnp.logical_or(relaying, helps), core == 0))
    def _():
        pl.semaphore_wait(ready_sem, 1)

    def relay(q, here):
        @pl.when(here)
        def _():
            z_arrival(1, q).wait_recv()
            relay_copy(q).start()

    def relay_squares():
        @pl.when(relaying)
        def _():
            sqz_arrival(1).wait_recv()
            sqr_copy().start()

    def arrive(q):
        either(z_stays, z_keep(q).wait, z_arrival(0, q).wait_recv)
        either(p_stays, p_keep(q).start, p_copy(q).start)

    def arrive_squares():
        either(z_stays, lambda: sqz_keep().wait(), lambda: sqz_arrival(0).wait_recv())
        for r in range(1, NH):
            sq_copy((hg + r) % NH, hg).start()
        either(p_stays, lambda: sq_keep().start(), lambda: sq_copy(hg, hg).start())

    def st_copy(q, to):
        return remote(
            st_out.at[q, to], st_in.at[q, me], st_send.at[q], st_recv.at[q], plane_device(to)
        )

    def vtot_copy(to):
        return remote(
            tot_here.at[to // 2], run_tot.at[me], vtot_send.at[0], vtot_recv.at[0],
            plane_device(to),
        )

    after_first = pl.ds(1, 7)

    def pre_copy(q, s):
        far = z == (0 if s else NZ - 1)
        to = jnp.where(far, NZ - 2 if s else 1, NZ // 2 * s + z // 2)
        slot = jnp.where(far, 2, z % 2)
        return remote(
            pre_out.at[q, s, after_first], pre_in.at[q, slot, after_first], pre_send.at[q, s],
            pre_recv.at[q, slot], z_device(to),
        )

    def pre_arrival(q, n):
        part = pre_in.at[q, n, after_first]
        return remote(part, part, pre_send.at[q, 0], pre_recv.at[q, n], partner)

    pre_relays = jnp.logical_or(z == 1, z == NZ - 2)

    def pre_pass(q):
        slot = jnp.where(z == 1, 1, 0)
        return remote(
            pre_in.at[q, 2, after_first], pre_in.at[q, slot, after_first], pre_on.at[q], pre_recv.at[q, slot],
            z_device(jnp.where(z == 1, NZ // 2 - 1, NZ // 2)),
        )

    def pre_relay(q):
        @pl.when(pre_relays)
        def _():
            pre_arrival(q, 2).wait_recv()
            pre_pass(q).start()

    def run_copy(q, s, to):
        return remote(
            run_out.at[q, s], run_in.at[q, NZ * s + z], run_send.at[q, s, to],
            run_recv.at[q, NZ * s + z], z_device(to),
        )

    def run_arrival(q, n):
        return remote(
            run_in.at[q, n], run_in.at[q, n], run_send.at[q, 0, 0], run_recv.at[q, n], partner
        )

    def run_targets(s, act):
        @pl.when(jnp.logical_and(NZ // 2 * s + z // 2 != z, z % 2 == 0))
        def _():
            act(NZ // 2 * s + z // 2)

        def visit(n):
            pl.when(n != z)(lambda: act(n))

        each(NZ // 2 * s + z // 2 + 1, NZ, visit)

    def log_copy(to, at):
        return remote(plane_out, plane_in.at[at], log_send.at[to], log_recv.at[at], z_device(to))

    def en_copy(q, to):
        return remote(
            en_out.at[q, to], en_in.at[q, me], en_send.at[q], en_recv.at[q], plane_device(to)
        )

    def sent(buffer, semaphore):
        rest = buffer.at[pl.ds(0, PLANE - 1)]
        return remote(rest, rest, semaphore, semaphore, partner)

    def states(q):
        square = sq_here[0] + sq_here[1] + sq_here[2] + sq_here[3]
        rate = lax.rsqrt(square[0:1] / FEATS + 1e-06)
        for k in range(8 * q, 8 * q + 8):
            rows = slice(k * SDIM, (k + 1) * SDIM)
            gain = gcol[rows, :]
            value = att[rows, :].astype(F32) * jnp.concatenate([gain, gain], 1) * rate
            value = value.astype(BF16).astype(F32)
            weighted[rows, :] = (value * w_here[k:k + 1, :].astype(F32)).astype(BF16)
        state = dot(weighted[q * HALF:(q + 1) * HALF], b_here[...], ((1,), (0,)))
        st_out[q] = state.astype(BF16).reshape(PLANE, SLICE, STATE)
        ring(lambda to: st_copy(q, to).start())
        st_in[q, me] = st_out[q, me]

    def locals_(q):
        if q == 0:
            for r in range(1, NH):
                sq_copy((hg + r) % NH, (hg + r) % NH).wait_recv()
            either(p_stays, lambda: sq_keep().wait(), lambda: sq_copy(hg, hg).wait_recv())
        for c in (2 * q, 2 * q + 1):
            either(p_stays, p_keep(c).wait, p_copy(c).wait_recv)
        square = sq_in[0] + sq_in[1] + sq_in[2] + sq_in[3]
        rate = lax.rsqrt(square[0:1] / FEATS + 1e-06)

        def make_local(p, carry):
            lanes = pl.ds(pl.multiple_of(p * BLK, BLK), BLK)
            pair = []
            for h in range(2):
                k = 2 * p + h
                rows = pl.ds(pl.multiple_of(k * SDIM, SDIM), SDIM)
                gain = gcol[rows, :]
                value = att_in[rows, :].astype(F32) * jnp.concatenate([gain, gain], 1) * rate
                value = value.astype(BF16)
                pair.append(dot(value, mix[k], ((1,), (0,))) + value.astype(F32) * skip_ref[k])
            both = jnp.concatenate(pair, 0)
            for tb in range(2):
                half = slice(tb * BLK, (tb + 1) * BLK)
                local[half, lanes] = jnp.transpose(both[:, half])
            return carry

        lax.fori_loop(4 * q, 4 * q + 4, make_local, 0)

    def prefix(q):
        sent(st_in.at[q], st_recv.at[q]).wait_recv()
        for s in range(2):
            running = jnp.zeros((SLICE, STATE), F32)
            for n in range(8):
                pre_out[q, s, n] = running.astype(BF16)
                decay = jnp.exp(run_tot[2 * n + s])
                running = decay[q:q + 1] * running + st_in[q, 2 * n + s].astype(F32)
            run_out[q, s] = running.astype(BF16)
        for s in range(2):
            run_targets(s, lambda to: run_copy(q, s, to).start())
            run_in[q, NZ * s + z] = run_out[q, s]
        for s in range(2):
            own = NZ // 2 * s + z // 2 == z
            pl.when(jnp.logical_not(own))(pre_copy(q, s).start)

            @pl.when(own)
            def _():
                pre_in[q, s] = pre_out[q, s]

    def enter(q):
        for n in range(2):
            @pl.when(2 * (z % (NZ // 2)) + n != z)
            def _():
                pre_arrival(q, n).wait_recv()

        if q == 0:
            each(0, z, lambda n: log_copy(n, n).wait_recv())

        def arrived(n):
            pl.when(n % NZ != z)(run_arrival(q, n).wait_recv)

        def gather(p, carried):
            for n in range(2):
                arrived(2 * p + n)
                decay = jnp.exp(plane_in[p, n])
                carried = decay[q:q + 1] * carried + run_in[q, 2 * p + n].astype(F32)
            return carried

        carried = lax.fori_loop(0, z, gather, jnp.zeros((SLICE, STATE), F32))
        en_out[q, 0] = carried.astype(BF16)
        for n in range(1, 8):
            value = pre_in[q, 0, n].astype(F32) + starts[n, q:q + 1] * carried
            en_out[q, n] = value.astype(BF16)
        arrived(2 * z)
        carried = jnp.exp(plane_out[0])[q:q + 1] * carried + run_in[q, 2 * z].astype(F32)
        en_out[q, 8] = carried.astype(BF16)
        for n in range(1, 8):
            value = pre_in[q, 1, n].astype(F32) + starts[8 + n, q:q + 1] * carried
            en_out[q, 8 + n] = value.astype(BF16)
        ring(lambda to: en_copy(q, to).start())
        en_in[q, me] = en_out[q, me]

    def finish(q):
        sent(en_in.at[q], en_recv.at[q]).wait_recv()
        lanes = slice(q * HALF, (q + 1) * HALF)
        entry = dot(c_v[...], en_in[q].reshape(HALF, STATE), ((1,), (1,)))
        out_ref[:, lanes] = (local[:, lanes] + ecum[:, lanes] * entry).astype(BF16)

    relay(0, relaying)
    for n in range(3):
        either(stays, home_keep(n).wait, home_copy(n).wait_recv)
    for o in range(8):
        lines = [tot_row[8 * (n % 2) + o:8 * (n % 2) + o + 1] for n in range(8)]
        tot_here[o] = jnp.concatenate(lines, 0)
    ring(lambda to: vtot_copy(to).start())
    run_tot[me] = tot_here[me // 2]
    for r in range(1, NH):
        here_arrival(r).wait_recv()
    for q in range(HALVES):
        states(q)

    relay(1, relaying)
    relay_squares()
    sent(tot_in, tot_recv.at[0]).wait_recv()
    for r in range(2):
        logs = jnp.zeros((8, 128), F32)
        for n in range(8 * r, 8 * r + 8):
            starts[n] = jnp.exp(logs)
            logs = logs + tot_in[n]
        plane_out[r] = logs

    each(z + 1, NZ, lambda to: log_copy(to, z).start())
    late = jnp.logical_or(
        jnp.logical_and(core == 0, z // 2 == 2), jnp.logical_and(core == 1, z // 2 == 1)
    )
    prompt = jnp.logical_not(late)
    pl.when(prompt)(lambda: arrive(0))
    relay(2, relaying)
    pl.when(prompt)(lambda: arrive(1))
    relay(3, relaying)
    relay(2, jnp.logical_and(helps, z == 0))
    sent(run_tot, vtot_recv.at[0]).wait_recv()
    prefix(0)
    prefix(1)
    relay(2, jnp.logical_and(helps, z > 0))
    relay(3, helps)
    for q in range(2):
        pl.when(late)(lambda: arrive(q))
    arrive_squares()
    arrive(2)
    arrive(3)
    pre_relay(0)
    pre_relay(1)
    enter(0)
    enter(1)
    locals_(0)
    finish(0)
    locals_(1)
    finish(1)

    for g in range(2):
        for t in range(2):
            halo(t, g, 0).wait_send()
            pl.when(jnp.logical_not(last_chip))(halo(t, g, 1).wait_send)
            swap(t, g).wait_send()
        q_swap(g).wait_send()
    for r in range(1, NH):
        sq_copy((hg + r) % NH, hg).wait_send()

    @pl.when(z_moves)
    def _():
        sqz_copy().wait_send()
        for q in range(CHUNKS):
            z_copy(q).wait_send()

    @pl.when(relaying)
    def _():
        sqr_copy().wait_send()
        for q in range(2):
            relay_copy(q).wait_send()

    @pl.when(jnp.logical_or(relaying, helps))
    def _():
        for q in range(2, CHUNKS):
            relay_copy(q).wait_send()

    @pl.when(p_moves)
    def _():
        sq_copy(hg, hg).wait_send()
        for q in range(CHUNKS):
            p_copy(q).wait_send()

    sent(tot_in, tot_send.at[0]).wait_send()
    sent(run_tot, vtot_send.at[0]).wait_send()
    each(z + 1, NZ, lambda to: log_copy(to, z).wait_send())
    for r in range(1, NH):
        here_copy(r).wait_send()

    @pl.when(jnp.logical_not(stays))
    def _():
        for n in range(3):
            home_copy(n).wait_send()

    for q in range(HALVES):
        sent(st_out.at[q], st_send.at[q]).wait_send()
        for s in range(2):
            run_targets(s, lambda to: run_copy(q, s, to).wait_send())
            pl.when(NZ // 2 * s + z // 2 != z)(pre_copy(q, s).wait_send)
        pl.when(pre_relays)(pre_pass(q).wait_send)
        sent(en_out.at[q], en_send.at[q]).wait_send()


def body(query, keys, values, norm_gain, in_b, out_c, step, log_decay, skip):
    feats = query.shape[2]
    gain = norm_gain.reshape(feats // HDIM, HDIM)
    dma = pltpu.SemaphoreType.DMA
    vm = pltpu.VMEM
    scratch = [
        vm((2, BLK, feats), BF16),
        vm((2, BLK, 256), BF16),
        vm((2, BLK, 256), BF16),
        vm((4 * BLK, 256), BF16),
        vm((4 * BLK, 256), BF16),
        vm((8, HDIM), F32),
        vm((SPAN, STATE), BF16),
        vm((SPAN, STATE), BF16),
        vm((16, SPAN), F32),
        vm((16, SPAN), F32),
        vm((16, 8, SPAN), F32),
        vm((16, 8, SPAN), F32),
        vm((feats, 128), F32),
        vm((16, SPAN, SPAN), BF16),
        vm((SPAN, feats), F32),
        vm((feats, SPAN), BF16),
        vm((2, feats, SPAN), BF16),
        vm((feats, SPAN), BF16),
        vm((8, SPAN), F32),
        vm((2, 8, SPAN), F32),
        vm((NH, 8, SPAN), F32),
        vm((NH, 8, SPAN), F32),
        vm((feats, SPAN), BF16),
        vm((SPAN, feats), F32),
        vm((16, SPAN), BF16),
        vm((16, SPAN), BF16),
        vm((SPAN, STATE), BF16),
        vm((16, 128), F32),
        vm((16, 128), F32),
        vm((8, 8, 128), F32),
        vm((8, 8, 128), F32),
        vm((PLANE, 8, 128), F32),
        vm((PLANE, 8, 128), F32),
        vm((PLANE, 8, 128), F32),
        vm((2, 8, 128), F32),
        vm((NZ, 2, 8, 128), F32),
        vm((HALVES, PLANE, SLICE, STATE), BF16),
        vm((HALVES, PLANE, SLICE, STATE), BF16),
        vm((HALVES, 2, 8, SLICE, STATE), BF16),
        vm((HALVES, 3, 8, SLICE, STATE), BF16),
        vm((HALVES, 2, SLICE, STATE), BF16),
        vm((HALVES, 2 * NZ, SLICE, STATE), BF16),
        vm((HALVES, PLANE, SLICE, STATE), BF16),
        vm((HALVES, PLANE, SLICE, STATE), BF16),
        pltpu.SMEM((16,), F32),
        dma((11,)),
        dma((2, 2, 2)), dma((2, 2, 2)),
        dma((2, 2)), dma((2, 2)),
        dma((2,)), dma((2,)),
        dma((CHUNKS,)), dma((2, CHUNKS)),
        dma((CHUNKS,)),
        dma((CHUNKS,)), dma((CHUNKS,)),
        dma((1,)), dma((2,)), dma((1,)),
        dma((NH,)), dma((NH,)),
        dma((NH,)), dma((NH,)),
        dma((3,)), dma((3,)),
        dma((1,)), dma((1,)),
        dma((HALVES, 2)), dma((HALVES, 3)), dma((HALVES,)),
        dma((1,)), dma((1,)),
        dma((NZ,)), dma((NZ,)),
        dma((HALVES,)), dma((HALVES,)),
        dma((HALVES, 2, NZ)), dma((HALVES, 2 * NZ)),
        dma((HALVES,)), dma((HALVES,)),
        pltpu.SemaphoreType.REGULAR,
        pltpu.SemaphoreType.REGULAR,
        pltpu.SemaphoreType.REGULAR,
        pltpu.SemaphoreType.REGULAR,
    ]
    anywhere = pl.BlockSpec(memory_space=pltpu.HBM)
    pinned = [
        pltpu.with_memory_space_constraint(a, pltpu.HBM)
        for a in (query, keys, values, gain, in_b, out_c, step, log_decay, skip)
    ]
    return pl.pallas_call(
        kernel,
        out_shape=jax.ShapeDtypeStruct((SPAN, feats), BF16),
        in_specs=[anywhere] * 9,
        out_specs=pl.BlockSpec(memory_space=pltpu.VMEM),
        scratch_shapes=scratch,
        compiler_params=pltpu.CompilerParams(
            collective_id=0, has_side_effects=True, vmem_limit_bytes=24 * 1024 * 1024
        ),
    )(*pinned)


def solution(mesh):
    torus = Mesh(mesh.devices.reshape(NZ, NX, NY, NC, NH), AXES)
    return jax.shard_map(
        body,
        mesh=torus,
        in_specs=(
            P(None, SEQ, "head"),
            P(None, SEQ, "head"),
            P(None, SEQ, "head"),
            P("head"),
            P(SEQ, None),
            P(SEQ, None),
            P("head", SEQ),
            P("head", SEQ),
            P("head"),
        ),
        out_specs=P(SEQ, "head"),
        check_vma=False,
    )
```

```python
import math

import jax
import jax.numpy as jnp
from jax import lax
from jax.experimental import pallas as pl
from jax.experimental.pallas import tpu as pltpu
from jax.sharding import Mesh
from jax.sharding import PartitionSpec as P

HDIM = 128
SDIM = 64
STATE = 128
SPAN = 256
BLK = 128
FEATS = 4096
NZ, NX, NY, NC, NH = 8, 4, 2, 2, 4
CHIPS = NZ * NX * NY
PLANE = NX * NY * NC
CHUNKS = 4
WIDE = 256
HALVES = 2
HALF = 512
SLICE = 32
AXES = ("z", "x", "y", "core", "head")
SEQ = ("z", "x", "y", "core")
MESH = pl.DeviceIdType.MESH
F32 = jnp.float32
BF16 = jnp.bfloat16


def chip_coords(chip):
    return chip // (NX * NY), (chip // NY) % NX, chip % NY


def seq_coords(index):
    return index // PLANE, (index // (NY * NC)) % NX, (index // NC) % NY, index % NC


def dot(a, b, dims, **kw):
    return lax.dot_general(a, b, (dims, ((), ())), preferred_element_type=F32, **kw)


def kernel(
    q_hbm, k_hbm, v_hbm, gain_hbm, b_hbm, c_hbm, step_hbm, decay_hbm, skip_hbm,
    out_ref,
    q_span, k_stage, v_stage, k_win, v_win, gain_v, b_v, c_v, step_v, decay_v,
    cum_v, v_v, gcol, mix, ecum, att, z_in, att_in, sq_out, sq_mid, sq_in, sq_here, weighted, local,
    w_low, w_here, b_here, tot_low, tot_row, tot_here, tot_out, tot_in, run_tot, starts, plane_out, plane_in,
    st_out, st_in, pre_out, pre_in, run_out, run_in, en_out, en_in,
    skip_ref, load_sem, halo_send, halo_recv, swap_send, swap_recv, q_send, q_recv, z_send, z_recv,
    relay_send, att_send, att_recv, sqz_send, sqz_recv, sqr_send, sq_send, sq_recv,
    here_send, here_recv, home_send, home_recv, vtot_send, vtot_recv, pre_send, pre_recv, pre_on,
    tot_send, tot_recv, log_send, log_recv, st_send, st_recv, run_send, run_recv,
    en_send, en_recv, ready_sem, later_sem, home_ready, head_sem,
):
    z, x, y, core, hg = (lax.axis_index(a) for a in AXES)
    chip = (z * NX + x) * NY + y
    me = (x * NY + y) * NC + core
    other = 1 - core
    partner = (z, x, y, other, hg)

    after = (chip + 1) % CHIPS
    az, ax, ay = chip_coords(after)
    wraps = (chip == CHIPS - 1).astype(jnp.int32)
    before = (chip + CHIPS - 1) % CHIPS
    bz, bx, by = chip_coords(before)

    span = core * CHIPS + chip
    long_out = z == jnp.where(core == 0, NZ - 1, 0)
    long_out = jnp.where(long_out, 1, 0)
    relays = jnp.where(z == jnp.where(core == 0, 1, NZ - 2), 1, 0)
    long_in = jnp.where(z == jnp.where(core == 0, NZ // 2, NZ // 2 - 1), 1, 0)
    relay_of = jnp.where(core == 0, 1, NZ - 2)
    to_z = jnp.where(long_out == 1, relay_of, NZ // 2 * core + z // 2)
    to_core = jnp.where(long_out == 1, core, z % 2)
    z_to = (to_z, x, y, to_core, hg)
    long_half = jnp.where(z == jnp.where(core == 0, 5, 2), 1, 0)
    helps = z == jnp.where(core == 0, 0, NZ - 1)
    half_to = (
        jnp.where(long_half == 1, jnp.where(core == 0, 0, NZ - 1), to_z), x, y,
        jnp.where(long_half == 1, core, to_core), hg,
    )
    half_out = jnp.maximum(long_out, long_half)
    from_z = jnp.where(long_in == 1, jnp.where(core == 0, NZ - 2, 1), 2 * (z % (NZ // 2)) + core)
    from_core = jnp.where(long_in == 1, other, z // (NZ // 2))
    z_from = (from_z, x, y, from_core, hg)
    relay_from = (jnp.where(core == 0, NZ - 1, 0), x, y, core, hg)
    relay_z = jnp.where(
        helps, jnp.where(core == 0, 2, 5), jnp.where(core == 0, NZ // 2 - 1, NZ // 2)
    )
    relay_to = (relay_z, x, y, other, hg)
    z_stays = jnp.logical_and(to_z == z, to_core == core)
    z_moves = jnp.logical_not(z_stays)
    relaying = relays == 1
    p_to = (z, 2 * core + x // 2, x % 2, y, hg)
    p_from = (z, 2 * (x % 2) + y, core, x // 2, hg)
    p_stays = jnp.logical_and(p_to[1] == x, jnp.logical_and(p_to[2] == y, p_to[3] == core))
    p_moves = jnp.logical_not(p_stays)

    seq = z * PLANE + me
    fz, fx, fy, fc = seq_coords(span)
    home = (fz, fx, fy, fc, hg)
    sz, sx, sy = chip_coords(seq % CHIPS)
    away = (sz, sx, sy, seq // CHIPS, hg)
    stays = span == seq

    barrier = pltpu.get_barrier_semaphore()

    def greet(device):
        pl.semaphore_signal(barrier, inc=1, device_id=device, device_id_type=MESH)

    def plane_device(index):
        return (z, index // (NY * NC), (index // NC) % NY, index % NC, hg)

    def z_device(index):
        return (index, x, y, core, hg)

    def ring(act):
        def visit(r, carry):
            act((me + r) % PLANE)
            return carry

        lax.fori_loop(1, PLANE, visit, 0)

    def each(low, high, act):
        def visit(n, carry):
            act(n)
            return carry

        lax.fori_loop(low, high, visit, 0)

    greet((bz, bx, by, 0, hg))
    greet((bz, bx, by, 1, hg))
    ring(lambda n: greet(plane_device(n)))

    def rank(h):
        return jnp.where(h == 0, 0, jnp.where(h == 2, 2, 1))

    level = rank(hg)
    same = (z, x, y, core)

    def to_heads(position, test, act):
        for r in range(1, NH):
            h = (hg + r) % NH

            @pl.when(test(rank(h)))
            def _():
                act((*position, h))

    to_heads(p_from[:4], lambda n: n >= level, greet)
    to_heads(p_to[:4], lambda n: n > level, greet)
    to_heads(same, lambda n: n >= level, greet)

    @pl.when(jnp.logical_and(z_moves, from_z > z))
    def _():
        greet(z_from)

    @pl.when(jnp.logical_and(z_moves, to_z > z))
    def _():
        greet(z_to)

    @pl.when(jnp.logical_and(relaying, core == 0))
    def _():
        greet(relay_from)

    @pl.when(jnp.logical_and(jnp.logical_or(relaying, helps), core == 0))
    def _():
        greet(relay_to)

    @pl.when(jnp.logical_and(z == 5, core == 0))
    def _():
        greet((NZ - 1, x, y, 1, hg))

    each(z + 1, NZ, lambda n: greet(z_device(n)))
    @pl.when(fz > z)
    def _():
        greet(home)

    @pl.when(sz > z)
    def _():
        greet(away)

    mine = pl.ds(pl.multiple_of((2 + core) * BLK, BLK), BLK)
    theirs = pl.ds(pl.multiple_of((2 + other) * BLK, BLK), BLK)
    prev_row = pl.ds(pl.multiple_of(core * BLK, BLK), BLK)
    loads = [
        (decay_hbm, decay_v), (step_hbm, step_v), (k_hbm, k_stage), (v_hbm, v_stage),
        (k_hbm.at[core], k_win.at[mine]), (v_hbm.at[core], v_win.at[mine]),
        (q_hbm.at[core], q_span.at[core]),
        (b_hbm, b_v), (c_hbm, c_v), (gain_hbm, gain_v), (skip_hbm, skip_ref),
    ]
    loads = [pltpu.make_async_copy(s, d, load_sem.at[i]) for i, (s, d) in enumerate(loads)]
    for copy in loads:
        copy.start()

    loads[0].wait()
    loads[1].wait()
    row = lax.broadcasted_iota(jnp.int32, (SPAN, SPAN), 0)
    col = lax.broadcasted_iota(jnp.int32, (SPAN, SPAN), 1)
    causal = row <= col
    cum = dot(decay_v[...], causal.astype(F32), ((1,), (0,)), precision=lax.Precision.HIGHEST)
    total = cum[:, SPAN - 1:]
    tail_weight = jnp.exp(total - cum) * step_v[...]
    w_low[...] = tail_weight.astype(BF16)
    tot_low[...] = jnp.broadcast_to(total, (16, 128))
    shift = jnp.log(step_v[...]) - cum
    for k in range(16):
        cum_v[k] = jnp.broadcast_to(cum[k:k + 1], (8, SPAN))
        v_v[k] = jnp.broadcast_to(shift[k:k + 1], (8, SPAN))
    for o in range(8):
        lines = [total[8 * (n % 2) + o:8 * (n % 2) + o + 1] for n in range(8)]
        tot_out[o] = jnp.broadcast_to(jnp.concatenate(lines, 0), (8, 128))
    for copy in loads[2:]:
        copy.wait()

    @pl.when(span == 0)
    def _():
        k_win[:2 * BLK] = jnp.zeros((2 * BLK, 256), BF16)
        v_win[:2 * BLK] = jnp.zeros((2 * BLK, 256), BF16)

    def one(condition):
        return jnp.where(condition, 1, 0)

    greeted = (
        z + one(jnp.logical_and(z_moves, to_z < z)) + one(jnp.logical_and(z_moves, from_z < z))
        + 2 * one(jnp.logical_and(relaying, core == 1)) + one(sz < z) + one(fz < z)
        + one(jnp.logical_and(jnp.logical_or(z == 2, z == NZ - 1), core == 1))
    )
    heads = jnp.where(level == 0, 0, jnp.where(level == 1, 5, 9))
    pl.semaphore_wait(barrier, NC + PLANE - 1 + heads + greeted)

    def reply(semaphore, device):
        pl.semaphore_signal(semaphore, inc=1, device_id=device, device_id_type=MESH)

    each(0, z, lambda n: reply(later_sem, z_device(n)))
    to_heads(p_from[:4], lambda n: n < level, lambda d: reply(head_sem, d))
    to_heads(same, lambda n: n < level, lambda d: reply(head_sem, d))

    @pl.when(jnp.logical_and(z_moves, from_z < z))
    def _():
        reply(ready_sem, z_from)

    @pl.when(jnp.logical_and(relaying, core == 1))
    def _():
        reply(ready_sem, relay_from)

    @pl.when(jnp.logical_and(z == 2, core == 1))
    def _():
        reply(ready_sem, (0, x, y, 0, hg))

    @pl.when(fz < z)
    def _():
        reply(home_ready, home)

    def remote(src, dst, send, recv, to):
        return pltpu.make_async_remote_copy(
            src_ref=src, dst_ref=dst, send_sem=send, recv_sem=recv,
            device_id=to, device_id_type=MESH,
        )

    def either(here, keep, leave):
        pl.when(here)(keep)
        pl.when(jnp.logical_not(here))(leave)

    def cols(g, width=HDIM):
        return pl.ds(g * width, width)

    def halo(i, g, slot):
        stage, window = ((k_stage, k_win), (v_stage, v_win))[i]
        to = (az, ax, ay, jnp.where(wraps == 1, 1 - slot, slot), hg)
        return remote(
            stage.at[slot, :, cols(g)], window.at[prev_row, cols(g)],
            halo_send.at[i, g, slot], halo_recv.at[i, g, core], to,
        )

    def halo_arrival(i, g, block):
        part = (k_win, v_win)[i].at[pl.ds(block * BLK, BLK), cols(g)]
        return remote(part, part, halo_send.at[i, g, 0], halo_recv.at[i, g, block], partner)

    def swap(i, g):
        stage, window = ((k_stage, k_win), (v_stage, v_win))[i]
        return remote(
            stage.at[other, :, cols(g)], window.at[mine, cols(g)],
            swap_send.at[i, g], swap_recv.at[i, g], partner,
        )

    def swap_arrival(i, g):
        part = (k_win, v_win)[i].at[theirs, cols(g)]
        return remote(part, part, swap_send.at[i, g], swap_recv.at[i, g], partner)

    def q_swap(g):
        return remote(
            q_hbm.at[other, :, cols(g, 512)], q_span.at[core, :, cols(g, 512)],
            q_send.at[g], q_recv.at[g], partner,
        )

    def q_arrival(g):
        part = q_span.at[other, :, cols(g, 512)]
        return remote(part, part, q_send.at[g], q_recv.at[g], partner)

    last_chip = chip == CHIPS - 1
    home_pairs = ((b_v, b_here), (w_low, w_here), (tot_low, tot_row))

    def home_copy(n):
        return remote(
            home_pairs[n][0], home_pairs[n][1], home_send.at[n], home_recv.at[n], away
        )

    def home_keep(n):
        return pltpu.make_async_copy(home_pairs[n][0], home_pairs[n][1], home_recv.at[n])

    def send_home():
        for n in range(3):
            either(stays, home_keep(n).start, home_copy(n).start)

    def send_halo(g):
        for i in range(2):
            halo(i, g, 0).start()
            pl.when(jnp.logical_not(last_chip))(halo(i, g, 1).start)
        q_swap(g).start()
        for i in range(2):
            swap(i, g).start()

    send_halo(0)
    pl.when(sz <= z)(send_home)
    send_halo(1)

    def tot_copy(to):
        return remote(
            tot_out.at[to // 2], tot_in.at[me], tot_send.at[0], tot_recv.at[0], plane_device(to)
        )

    ring(lambda to: tot_copy(to).start())
    tot_in[me] = tot_out[me // 2]
    for p in range(8):
        line = jnp.broadcast_to(gain_v[p:p + 1, :], (BLK, BLK))
        gcol[p * BLK:(p + 1) * BLK, :] = jnp.transpose(line)

    scale = math.log2(math.e) / math.sqrt(HDIM)
    j = lax.broadcasted_iota(jnp.int32, (BLK, 4 * BLK), 0)
    i = lax.broadcasted_iota(jnp.int32, (BLK, 4 * BLK), 1) % BLK
    first = one(span == 0)
    recent = j > i + first * BLK
    until = j <= i

    def part(q):
        return pl.ds(q * WIDE, WIDE)

    def z_copy(q):
        slot, to = (long_out, z_to) if q < 2 else (half_out, half_to)
        return remote(att.at[part(q)], z_in.at[slot, part(q)], z_send.at[q], z_recv.at[slot, q], to)

    def z_keep(q):
        return pltpu.make_async_copy(att.at[part(q)], z_in.at[0, part(q)], z_recv.at[0, q])

    def relay_copy(q):
        return remote(
            z_in.at[1, part(q)], z_in.at[0, part(q)], relay_send.at[q], z_recv.at[0, q], relay_to
        )

    def z_arrival(at, q):
        return remote(
            z_in.at[at, part(q)], z_in.at[at, part(q)], relay_send.at[q], z_recv.at[at, q], relay_to
        )

    def p_copy(q):
        return remote(z_in.at[0, part(q)], att_in.at[part(q)], att_send.at[q], att_recv.at[q], p_to)

    def p_keep(q):
        return pltpu.make_async_copy(z_in.at[0, part(q)], att_in.at[part(q)], att_recv.at[q])

    def sqz_copy():
        return remote(sq_out, sq_mid.at[long_out], sqz_send.at[0], sqz_recv.at[long_out], z_to)

    def sqz_keep():
        return pltpu.make_async_copy(sq_out, sq_mid.at[0], sqz_recv.at[0])

    def sqr_copy():
        return remote(sq_mid.at[1], sq_mid.at[0], sqr_send.at[0], sqz_recv.at[0], relay_to)

    def sqz_arrival(at):
        return remote(sq_mid.at[at], sq_mid.at[at], sqr_send.at[0], sqz_recv.at[at], relay_to)

    def sq_copy(to, at):
        return remote(
            sq_mid.at[0], sq_in.at[at], sq_send.at[to], sq_recv.at[at],
            (z, p_to[1], p_to[2], p_to[3], to),
        )

    def sq_keep():
        return pltpu.make_async_copy(sq_mid.at[0], sq_in.at[hg], sq_recv.at[hg])

    def here_copy(r):
        return remote(
            sq_out, sq_here.at[hg], here_send.at[r], here_recv.at[hg],
            (z, x, y, core, (hg + r) % NH),
        )

    def here_arrival(r):
        n = (hg + r) % NH
        return remote(sq_here.at[n], sq_here.at[n], here_send.at[r], here_recv.at[n], partner)

    @pl.when(sz > z)
    def _():
        pl.semaphore_wait(home_ready, 1)
        send_home()

    sums = [jnp.zeros((1, BLK), F32) for _ in range(2)]
    for g in range(2):
        @pl.when(span > 0)
        def _():
            for t in range(2):
                for block in range(2):
                    halo_arrival(t, g, block).wait_recv()

        for t in range(2):
            swap_arrival(t, g).wait_recv()
        q_arrival(g).wait_recv()
        lanes = slice(g * HDIM, (g + 1) * HDIM)
        for a in range(2):
            keys = k_win[a * BLK:(a + 3) * BLK, lanes]
            vals = jnp.transpose(v_win[a * BLK:(a + 3) * BLK, lanes])
            heads = [q_span[a, :, (4 * g + h) * HDIM:(4 * g + h + 1) * HDIM] for h in range(4)]
            score = dot(keys, jnp.concatenate(heads, 0), ((1,), (1,)))
            middle = score[BLK:2 * BLK]
            if a == 0:
                middle = jnp.where(first == 1, -jnp.inf, middle)
            score = jnp.concatenate([
                jnp.where(recent, score[:BLK], -jnp.inf), middle,
                jnp.where(until, score[2 * BLK:], -jnp.inf),
            ], 0)
            peak = jnp.max(score, axis=0, keepdims=True)
            terms = jnp.exp2((score - peak) * scale)
            sum_terms = jnp.sum(terms, axis=0, keepdims=True)
            got = dot(vals, terms.astype(BF16), ((1,), (0,)))
            got = (got * (1.0 / sum_terms)).astype(BF16)
            for h in range(4):
                head = got[:, h * BLK:(h + 1) * BLK]
                att[(4 * g + h) * HDIM:(4 * g + h + 1) * HDIM, a * BLK:(a + 1) * BLK] = head
                wide = head.astype(F32)
                sums[a] = sums[a] + jnp.sum(wide * wide, axis=0, keepdims=True)
        if g == 0:
            @pl.when(jnp.logical_and(z_moves, to_z > z))
            def _():
                pl.semaphore_wait(ready_sem, 1)
        else:
            sq_out[...] = jnp.broadcast_to(jnp.concatenate(sums, 1), (8, SPAN))

            @pl.when(level < 2)
            def _():
                pl.semaphore_wait(head_sem, jnp.where(level == 0, 6, 2))

            for r in range(1, NH):
                here_copy(r).start()
            sq_here[hg] = sq_out[...]
            either(z_stays, lambda: sqz_keep().start(), lambda: sqz_copy().start())

            @pl.when(z < NZ - 1)
            def _():
                pl.semaphore_wait(later_sem, NZ - 1 - z)

        for q in (2 * g, 2 * g + 1):
            either(z_stays, z_keep(q).start, z_copy(q).start)
    cross = dot(b_v[...], c_v[...], ((1,), (1,)))

    def make_mix(k, carry):
        ct = cum_v[k, 0:1, :]
        for ub in range(2):
            line = v_v[k, 0:1, ub * BLK:(ub + 1) * BLK]
            colb = jnp.transpose(jnp.broadcast_to(line, (BLK, BLK)))
            arg = ct + jnp.concatenate([colb, colb], 1)
            rows = slice(ub * BLK, (ub + 1) * BLK)
            arg = jnp.where(causal[rows], arg, -jnp.inf)
            mix[k, rows] = (jnp.exp(arg) * cross[rows]).astype(BF16)
        return carry

    lax.fori_loop(0, 16, make_mix, 0)

    def make_ecum(p, carry):
        lanes = pl.ds(pl.multiple_of(p * BLK, BLK), BLK)
        for tb in range(2):
            half = slice(tb * BLK, (tb + 1) * BLK)
            pair = [
                jnp.broadcast_to(jnp.exp(cum_v[2 * p + h, 0:1, half]), (SDIM, BLK))
                for h in range(2)
            ]
            ecum[half, lanes] = jnp.transpose(jnp.concatenate(pair, 0))
        return carry

    lax.fori_loop(0, 8, make_ecum, 0)

    @pl.when(jnp.logical_and(jnp.logical_or(relaying, helps), core == 0))
    def _():
        pl.semaphore_wait(ready_sem, 1)

    def relay(q, here):
        @pl.when(here)
        def _():
            z_arrival(1, q).wait_recv()
            relay_copy(q).start()

    def relay_squares():
        @pl.when(relaying)
        def _():
            sqz_arrival(1).wait_recv()
            sqr_copy().start()

    def arrive(q):
        either(z_stays, z_keep(q).wait, z_arrival(0, q).wait_recv)
        either(p_stays, p_keep(q).start, p_copy(q).start)

    def arrive_squares():
        either(z_stays, lambda: sqz_keep().wait(), lambda: sqz_arrival(0).wait_recv())
        for r in range(1, NH):
            sq_copy((hg + r) % NH, hg).start()
        either(p_stays, lambda: sq_keep().start(), lambda: sq_copy(hg, hg).start())

    def st_copy(q, to):
        return remote(
            st_out.at[q, to], st_in.at[q, me], st_send.at[q], st_recv.at[q], plane_device(to)
        )

    def vtot_copy(to):
        return remote(
            tot_here.at[to // 2], run_tot.at[me], vtot_send.at[0], vtot_recv.at[0],
            plane_device(to),
        )

    after_first = pl.ds(1, 7)

    def pre_copy(q, s):
        far = z == (0 if s else NZ - 1)
        to = jnp.where(far, NZ - 2 if s else 1, NZ // 2 * s + z // 2)
        slot = jnp.where(far, 2, z % 2)
        return remote(
            pre_out.at[q, s, after_first], pre_in.at[q, slot, after_first], pre_send.at[q, s],
            pre_recv.at[q, slot], z_device(to),
        )

    def pre_arrival(q, n):
        part = pre_in.at[q, n, after_first]
        return remote(part, part, pre_send.at[q, 0], pre_recv.at[q, n], partner)

    pre_relays = jnp.logical_or(z == 1, z == NZ - 2)

    def pre_pass(q):
        slot = jnp.where(z == 1, 1, 0)
        return remote(
            pre_in.at[q, 2, after_first], pre_in.at[q, slot, after_first], pre_on.at[q], pre_recv.at[q, slot],
            z_device(jnp.where(z == 1, NZ // 2 - 1, NZ // 2)),
        )

    def pre_relay(q):
        @pl.when(pre_relays)
        def _():
            pre_arrival(q, 2).wait_recv()
            pre_pass(q).start()

    def run_copy(q, s, to):
        return remote(
            run_out.at[q, s], run_in.at[q, NZ * s + z], run_send.at[q, s, to],
            run_recv.at[q, NZ * s + z], z_device(to),
        )

    def run_arrival(q, n):
        return remote(
            run_in.at[q, n], run_in.at[q, n], run_send.at[q, 0, 0], run_recv.at[q, n], partner
        )

    def run_targets(s, act):
        @pl.when(jnp.logical_and(NZ // 2 * s + z // 2 != z, z % 2 == 0))
        def _():
            act(NZ // 2 * s + z // 2)

        def visit(n):
            pl.when(n != z)(lambda: act(n))

        each(NZ // 2 * s + z // 2 + 1, NZ, visit)

    def log_copy(to, at):
        return remote(plane_out, plane_in.at[at], log_send.at[to], log_recv.at[at], z_device(to))

    def en_copy(q, to):
        return remote(
            en_out.at[q, to], en_in.at[q, me], en_send.at[q], en_recv.at[q], plane_device(to)
        )

    def sent(buffer, semaphore):
        rest = buffer.at[pl.ds(0, PLANE - 1)]
        return remote(rest, rest, semaphore, semaphore, partner)

    def states(q):
        square = sq_here[0] + sq_here[1] + sq_here[2] + sq_here[3]
        rate = lax.rsqrt(square[0:1] / FEATS + 1e-06)
        for k in range(8 * q, 8 * q + 8):
            rows = slice(k * SDIM, (k + 1) * SDIM)
            gain = gcol[rows, :]
            value = att[rows, :].astype(F32) * jnp.concatenate([gain, gain], 1) * rate
            value = value.astype(BF16).astype(F32)
            weighted[rows, :] = (value * w_here[k:k + 1, :].astype(F32)).astype(BF16)
        state = dot(weighted[q * HALF:(q + 1) * HALF], b_here[...], ((1,), (0,)))
        st_out[q] = state.astype(BF16).reshape(PLANE, SLICE, STATE)
        ring(lambda to: st_copy(q, to).start())
        st_in[q, me] = st_out[q, me]

    def locals_(q):
        if q == 0:
            for r in range(1, NH):
                sq_copy((hg + r) % NH, (hg + r) % NH).wait_recv()
            either(p_stays, lambda: sq_keep().wait(), lambda: sq_copy(hg, hg).wait_recv())
        for c in (2 * q, 2 * q + 1):
            either(p_stays, p_keep(c).wait, p_copy(c).wait_recv)
        square = sq_in[0] + sq_in[1] + sq_in[2] + sq_in[3]
        rate = lax.rsqrt(square[0:1] / FEATS + 1e-06)

        def make_local(p, carry):
            lanes = pl.ds(pl.multiple_of(p * BLK, BLK), BLK)
            pair = []
            for h in range(2):
                k = 2 * p + h
                rows = pl.ds(pl.multiple_of(k * SDIM, SDIM), SDIM)
                gain = gcol[rows, :]
                value = att_in[rows, :].astype(F32) * jnp.concatenate([gain, gain], 1) * rate
                value = value.astype(BF16)
                pair.append(dot(value, mix[k], ((1,), (0,))) + value.astype(F32) * skip_ref[k])
            both = jnp.concatenate(pair, 0)
            for tb in range(2):
                half = slice(tb * BLK, (tb + 1) * BLK)
                local[half, lanes] = jnp.transpose(both[:, half])
            return carry

        lax.fori_loop(4 * q, 4 * q + 4, make_local, 0)

    def prefix(q):
        sent(st_in.at[q], st_recv.at[q]).wait_recv()
        for s in range(2):
            running = jnp.zeros((SLICE, STATE), F32)
            for n in range(8):
                pre_out[q, s, n] = running.astype(BF16)
                decay = jnp.exp(run_tot[2 * n + s])
                running = decay[q:q + 1] * running + st_in[q, 2 * n + s].astype(F32)
            run_out[q, s] = running.astype(BF16)
        for s in range(2):
            run_targets(s, lambda to: run_copy(q, s, to).start())
            run_in[q, NZ * s + z] = run_out[q, s]
        for s in range(2):
            own = NZ // 2 * s + z // 2 == z
            pl.when(jnp.logical_not(own))(pre_copy(q, s).start)

            @pl.when(own)
            def _():
                pre_in[q, s] = pre_out[q, s]

    def enter(q):
        for n in range(2):
            @pl.when(2 * (z % (NZ // 2)) + n != z)
            def _():
                pre_arrival(q, n).wait_recv()

        if q == 0:
            each(0, z, lambda n: log_copy(n, n).wait_recv())

        def arrived(n):
            pl.when(n % NZ != z)(run_arrival(q, n).wait_recv)

        def gather(p, carried):
            for n in range(2):
                arrived(2 * p + n)
                decay = jnp.exp(plane_in[p, n])
                carried = decay[q:q + 1] * carried + run_in[q, 2 * p + n].astype(F32)
            return carried

        carried = lax.fori_loop(0, z, gather, jnp.zeros((SLICE, STATE), F32))
        en_out[q, 0] = carried.astype(BF16)
        for n in range(1, 8):
            value = pre_in[q, 0, n].astype(F32) + starts[n, q:q + 1] * carried
            en_out[q, n] = value.astype(BF16)
        arrived(2 * z)
        carried = jnp.exp(plane_out[0])[q:q + 1] * carried + run_in[q, 2 * z].astype(F32)
        en_out[q, 8] = carried.astype(BF16)
        for n in range(1, 8):
            value = pre_in[q, 1, n].astype(F32) + starts[8 + n, q:q + 1] * carried
            en_out[q, 8 + n] = value.astype(BF16)
        ring(lambda to: en_copy(q, to).start())
        en_in[q, me] = en_out[q, me]

    def finish(q):
        sent(en_in.at[q], en_recv.at[q]).wait_recv()
        lanes = slice(q * HALF, (q + 1) * HALF)
        entry = dot(c_v[...], en_in[q].reshape(HALF, STATE), ((1,), (1,)))
        out_ref[:, lanes] = (local[:, lanes] + ecum[:, lanes] * entry).astype(BF16)

    relay(0, relaying)
    for n in range(3):
        either(stays, home_keep(n).wait, home_copy(n).wait_recv)
    for o in range(8):
        lines = [tot_row[8 * (n % 2) + o:8 * (n % 2) + o + 1] for n in range(8)]
        tot_here[o] = jnp.concatenate(lines, 0)
    ring(lambda to: vtot_copy(to).start())
    run_tot[me] = tot_here[me // 2]
    for r in range(1, NH):
        here_arrival(r).wait_recv()
    for q in range(HALVES):
        states(q)

    relay(1, relaying)
    relay_squares()
    sent(tot_in, tot_recv.at[0]).wait_recv()
    for r in range(2):
        logs = jnp.zeros((8, 128), F32)
        for n in range(8 * r, 8 * r + 8):
            starts[n] = jnp.exp(logs)
            logs = logs + tot_in[n]
        plane_out[r] = logs

    each(z + 1, NZ, lambda to: log_copy(to, z).start())
    late = jnp.logical_or(
        jnp.logical_and(core == 0, z // 2 == 2), jnp.logical_and(core == 1, z // 2 == 1)
    )
    prompt = jnp.logical_not(late)
    pl.when(prompt)(lambda: arrive(0))
    relay(2, relaying)
    pl.when(prompt)(lambda: arrive(1))
    relay(3, relaying)
    relay(2, jnp.logical_and(helps, z == 0))
    relay(3, jnp.logical_and(helps, z == 0))
    sent(run_tot, vtot_recv.at[0]).wait_recv()
    prefix(0)
    prefix(1)
    relay(2, jnp.logical_and(helps, z > 0))
    relay(3, jnp.logical_and(helps, z > 0))
    for q in range(2):
        pl.when(late)(lambda: arrive(q))
    arrive_squares()
    arrive(2)
    arrive(3)
    pre_relay(0)
    pre_relay(1)
    enter(0)
    enter(1)
    locals_(0)
    finish(0)
    locals_(1)
    finish(1)

    for g in range(2):
        for t in range(2):
            halo(t, g, 0).wait_send()
            pl.when(jnp.logical_not(last_chip))(halo(t, g, 1).wait_send)
            swap(t, g).wait_send()
        q_swap(g).wait_send()
    for r in range(1, NH):
        sq_copy((hg + r) % NH, hg).wait_send()

    @pl.when(z_moves)
    def _():
        sqz_copy().wait_send()
        for q in range(CHUNKS):
            z_copy(q).wait_send()

    @pl.when(relaying)
    def _():
        sqr_copy().wait_send()
        for q in range(2):
            relay_copy(q).wait_send()

    @pl.when(jnp.logical_or(relaying, helps))
    def _():
        for q in range(2, CHUNKS):
            relay_copy(q).wait_send()

    @pl.when(p_moves)
    def _():
        sq_copy(hg, hg).wait_send()
        for q in range(CHUNKS):
            p_copy(q).wait_send()

    sent(tot_in, tot_send.at[0]).wait_send()
    sent(run_tot, vtot_send.at[0]).wait_send()
    each(z + 1, NZ, lambda to: log_copy(to, z).wait_send())
    for r in range(1, NH):
        here_copy(r).wait_send()

    @pl.when(jnp.logical_not(stays))
    def _():
        for n in range(3):
            home_copy(n).wait_send()

    for q in range(HALVES):
        sent(st_out.at[q], st_send.at[q]).wait_send()
        for s in range(2):
            run_targets(s, lambda to: run_copy(q, s, to).wait_send())
            pl.when(NZ // 2 * s + z // 2 != z)(pre_copy(q, s).wait_send)
        pl.when(pre_relays)(pre_pass(q).wait_send)
        sent(en_out.at[q], en_send.at[q]).wait_send()


def body(query, keys, values, norm_gain, in_b, out_c, step, log_decay, skip):
    feats = query.shape[2]
    gain = norm_gain.reshape(feats // HDIM, HDIM)
    dma = pltpu.SemaphoreType.DMA
    vm = pltpu.VMEM
    scratch = [
        vm((2, BLK, feats), BF16),
        vm((2, BLK, 256), BF16),
        vm((2, BLK, 256), BF16),
        vm((4 * BLK, 256), BF16),
        vm((4 * BLK, 256), BF16),
        vm((8, HDIM), F32),
        vm((SPAN, STATE), BF16),
        vm((SPAN, STATE), BF16),
        vm((16, SPAN), F32),
        vm((16, SPAN), F32),
        vm((16, 8, SPAN), F32),
        vm((16, 8, SPAN), F32),
        vm((feats, 128), F32),
        vm((16, SPAN, SPAN), BF16),
        vm((SPAN, feats), F32),
        vm((feats, SPAN), BF16),
        vm((2, feats, SPAN), BF16),
        vm((feats, SPAN), BF16),
        vm((8, SPAN), F32),
        vm((2, 8, SPAN), F32),
        vm((NH, 8, SPAN), F32),
        vm((NH, 8, SPAN), F32),
        vm((feats, SPAN), BF16),
        vm((SPAN, feats), F32),
        vm((16, SPAN), BF16),
        vm((16, SPAN), BF16),
        vm((SPAN, STATE), BF16),
        vm((16, 128), F32),
        vm((16, 128), F32),
        vm((8, 8, 128), F32),
        vm((8, 8, 128), F32),
        vm((PLANE, 8, 128), F32),
        vm((PLANE, 8, 128), F32),
        vm((PLANE, 8, 128), F32),
        vm((2, 8, 128), F32),
        vm((NZ, 2, 8, 128), F32),
        vm((HALVES, PLANE, SLICE, STATE), BF16),
        vm((HALVES, PLANE, SLICE, STATE), BF16),
        vm((HALVES, 2, 8, SLICE, STATE), BF16),
        vm((HALVES, 3, 8, SLICE, STATE), BF16),
        vm((HALVES, 2, SLICE, STATE), BF16),
        vm((HALVES, 2 * NZ, SLICE, STATE), BF16),
        vm((HALVES, PLANE, SLICE, STATE), BF16),
        vm((HALVES, PLANE, SLICE, STATE), BF16),
        pltpu.SMEM((16,), F32),
        dma((11,)),
        dma((2, 2, 2)), dma((2, 2, 2)),
        dma((2, 2)), dma((2, 2)),
        dma((2,)), dma((2,)),
        dma((CHUNKS,)), dma((2, CHUNKS)),
        dma((CHUNKS,)),
        dma((CHUNKS,)), dma((CHUNKS,)),
        dma((1,)), dma((2,)), dma((1,)),
        dma((NH,)), dma((NH,)),
        dma((NH,)), dma((NH,)),
        dma((3,)), dma((3,)),
        dma((1,)), dma((1,)),
        dma((HALVES, 2)), dma((HALVES, 3)), dma((HALVES,)),
        dma((1,)), dma((1,)),
        dma((NZ,)), dma((NZ,)),
        dma((HALVES,)), dma((HALVES,)),
        dma((HALVES, 2, NZ)), dma((HALVES, 2 * NZ)),
        dma((HALVES,)), dma((HALVES,)),
        pltpu.SemaphoreType.REGULAR,
        pltpu.SemaphoreType.REGULAR,
        pltpu.SemaphoreType.REGULAR,
        pltpu.SemaphoreType.REGULAR,
    ]
    anywhere = pl.BlockSpec(memory_space=pltpu.HBM)
    pinned = [
        pltpu.with_memory_space_constraint(a, pltpu.HBM)
        for a in (query, keys, values, gain, in_b, out_c, step, log_decay, skip)
    ]
    return pl.pallas_call(
        kernel,
        out_shape=jax.ShapeDtypeStruct((SPAN, feats), BF16),
        in_specs=[anywhere] * 9,
        out_specs=pl.BlockSpec(memory_space=pltpu.VMEM),
        scratch_shapes=scratch,
        compiler_params=pltpu.CompilerParams(
            collective_id=0, has_side_effects=True, vmem_limit_bytes=24 * 1024 * 1024
        ),
    )(*pinned)


def solution(mesh):
    torus = Mesh(mesh.devices.reshape(NZ, NX, NY, NC, NH), AXES)
    return jax.shard_map(
        body,
        mesh=torus,
        in_specs=(
            P(None, SEQ, "head"),
            P(None, SEQ, "head"),
            P(None, SEQ, "head"),
            P("head"),
            P(SEQ, None),
            P(SEQ, None),
            P("head", SEQ),
            P("head", SEQ),
            P("head"),
        ),
        out_specs=P(SEQ, "head"),
        check_vma=False,
    )
```
